32 devices in a mesh: dp: 8 (over z, y), seq: 4 (over x, core).
Axes of the slice: x: 2, y: 2, z: 4, core: 2. Of those that a mesh axis runs over, the one named last changes fastest.
Arguments:
- tokens: bfloat16 [2, 8192, 2048], P(None, ('dp', 'seq')), may hold values from -6 to 6
- positions: int32 [2, 8192], P(None, 'dp'), may hold values from 0 to 1023, as said below
- cotangent: bfloat16 [2, 8192, 2048], P(None, ('dp', 'seq')), may hold values from -6 to 6
- norm1_gain: bfloat16 [2048], P(('dp', 'seq')), may hold values from 0.099609375 to 1.8984375
- norm1_bias: bfloat16 [2048], P(('dp', 'seq')), may hold values from -2 to 2
- norm2_gain: bfloat16 [2048], P(('dp', 'seq')), may hold values from 0.099609375 to 1.8984375
- norm2_bias: bfloat16 [2048], P(('dp', 'seq')), may hold values from -2 to 2
- qkv_weight: bfloat16 [2048, 6144], P(('dp', 'seq')), may hold values from -1 to 1
- qkv_bias: bfloat16 [6144], P(('dp', 'seq')), may hold values from -2 to 2
- out_weight: bfloat16 [2048, 2048], P(('dp', 'seq')), may hold values from -1 to 1
- out_bias: bfloat16 [2048], P(('dp', 'seq')), may hold values from -3 to 3
- up_weight: bfloat16 [2048, 8192], P(('dp', 'seq')), may hold values from -0.125 to 0.125
- up_bias: bfloat16 [8192], P(('dp', 'seq')), may hold values from -3 to 3
- down_weight: bfloat16 [2048, 8192], P(('dp', 'seq')), may hold values from -0.0625 to 0.0625
- down_bias: bfloat16 [2048], P(('dp', 'seq')), may hold values from -3 to 3
Outputs:
- output: bfloat16 [2, 8192, 2048], P(None, ('dp', 'seq'))
- token_grad: float32 [2, 8192, 2048], P(None, ('dp', 'seq'))
- norm1_gain_grad: float32 [2048], P(('dp', 'seq'))
- norm1_bias_grad: float32 [2048], P(('dp', 'seq'))
- norm2_gain_grad: float32 [2048], P(('dp', 'seq'))
- norm2_bias_grad: float32 [2048], P(('dp', 'seq'))
- qkv_weight_grad: float32 [2048, 6144], P(('dp', 'seq'))
- qkv_bias_grad: float32 [6144], P(('dp', 'seq'))
- out_weight_grad: float32 [2048, 2048], P(('dp', 'seq'))
- out_bias_grad: float32 [2048], P(('dp', 'seq'))
- up_weight_grad: float32 [2048, 8192], P(('dp', 'seq'))
- up_bias_grad: float32 [8192], P(('dp', 'seq'))
- down_weight_grad: float32 [2048, 8192], P(('dp', 'seq'))
- down_bias_grad: float32 [2048], P(('dp', 'seq'))
The draws below stay inside these ranges and needn't reach their ends.
Inputs may be any that keep to these rules, and one draw needn't show every extreme that they name: The 1024 positions of each sequence hold every number of 0 to 1023 once. The positions of one sequence on one index of seq are two runs of 128 consecutive rising numbers, one starting at c * 128 and one at 1024 - (c + 1) * 128 for some c, in either order.
All inputs are finite; a program needn't handle non-finite values.
Results may differ from the reference program's by a relative error of at most 0.0095.
Values may be sent and summed in bfloat16 or wider, within the bound.
A program may use at most 704 MiB of HBM per device.

```python
import math
import jax
import jax.numpy as jnp
from jax import lax

D = 2048
HEADS = 8
HEAD_DIM = 256
FF = 8192
ROTARY = 64
MICRO = 2
SEQ_LEN = 1024
HALF = 128
SEQS = 16
N_DP = 8


def draw_positions(key, part):
    run_len = HALF
    seq_count = SEQS
    pairs = SEQ_LEN // (2 * run_len)
    seq_keys = jax.random.split(jax.random.fold_in(key, 7), seq_count)

    def shuffle(one_key):
        return jax.random.permutation(one_key, pairs).astype(jnp.int32)
    pair_order = jax.vmap(shuffle)(seq_keys)
    flipped = jax.random.randint(jax.random.fold_in(key, 8), (seq_count, pairs), 0, 2)
    mirror = 2 * pairs - 1 - pair_order
    front_block = jnp.where(flipped == 1, mirror, pair_order)
    back_block = jnp.where(flipped == 1, pair_order, mirror)
    block_ids = jnp.stack([front_block, back_block], 2)
    offsets = jnp.arange(run_len, dtype=jnp.int32)
    placed = block_ids[..., None] * run_len + offsets
    return placed.reshape(MICRO, SEQS // MICRO * SEQ_LEN).astype(jnp.int32)


def draw_qkv_weight(key, part):
    scaling = D ** (-0.5)
    whole = jax.random.normal(jax.random.fold_in(key, 1), (D, 3 * D), jnp.float32) * scaling
    return jnp.clip(whole, -1.0, 1.0).astype(jnp.bfloat16)


def spiked(entries, stream_key, source, target, blocks, factor):
    def block_of(axis_at):
        return (jnp.arange(entries.shape[axis_at]) // (entries.shape[axis_at] // blocks)).reshape((-1,) + (1,) * (entries.ndim - 1 - axis_at))

    first = jax.random.permutation(stream_key, blocks)[block_of(target)]
    second = (block_of(target) + blocks // 2) % blocks
    return jnp.where((block_of(source) == first) | (block_of(source) == second), factor * entries, entries)


def block_levels(own_key, dims, shards, least, top_value):
    def one(dim, parts):
        steps = jax.random.uniform(jax.random.fold_in(jax.random.fold_in(own_key, 6), dim), (parts,), jnp.float32, least / len(shards), top_value / len(shards))
        return jnp.repeat(jnp.exp(steps), dims[dim] // parts).reshape((-1,) + (1,) * (len(dims) - dim - 1))

    gain = one(*shards[0])
    for cut in shards[1:]:
        gain = gain * one(*cut)
    return gain


def bell_draw(stream_key, shape, spread, reach, cuts=(), kind=jnp.bfloat16):
    gain = block_levels(stream_key, shape, cuts, -0.22, 0.18) if cuts else 1.0
    values = jax.random.normal(stream_key, shape, jnp.float32) * spread * gain
    return jnp.minimum(jnp.maximum(values, -reach), reach).astype(kind)


def gaussian_with(own_key, shape, scale, reach, cuts, heavy, kind=jnp.bfloat16):
    array = scale * jax.random.normal(own_key, shape, jnp.float32)
    if cuts:
        array = array * block_levels(own_key, shape, cuts, -0.22, 0.18)
    return jnp.clip(spiked(array, jax.random.fold_in(own_key, 3), *heavy), -reach, reach).astype(kind)


def setup_inputs(seed: int = 0) -> dict:
    splits = jax.random.split(jax.random.key(seed), 16)
    return {
        "tokens": bell_draw(splits[0], (MICRO, N_DP * SEQ_LEN, D), 1.0, 6.0, ((1, 32),)),
        "positions": draw_positions(jax.random.fold_in(splits[15], 71), 0),
        "cotangent": gaussian_with(splits[2], (MICRO, N_DP * SEQ_LEN, D), 1.0, 6.0, ((1, 32),), (1, 2, 32, 2.75)),
        "norm1_gain": jnp.clip(1.0 + 0.18 * jax.random.normal(splits[3], (D,), jnp.float32), 0.099609375, 1.8984375).astype(jnp.bfloat16),
        "norm1_bias": bell_draw(splits[4], (D,), 0.3, 2.0, ((0, 32),)),
        "norm2_gain": jnp.clip(1.0 + 0.18 * jax.random.normal(splits[5], (D,), jnp.float32), 0.099609375, 1.8984375).astype(jnp.bfloat16),
        "norm2_bias": bell_draw(splits[6], (D,), 0.3, 2.0, ((0, 32),)),
        "qkv_weight": draw_qkv_weight(jax.random.fold_in(splits[15], 71), 0),
        "qkv_bias": bell_draw(splits[8], (3 * D,), 0.3, 2.0, ((0, 32),)),
        "out_weight": bell_draw(splits[9], (D, D), (D // 64) ** -0.5, 1.0, ((0, 32),)),
        "out_bias": bell_draw(splits[10], (D,), 0.5, 3.0, ((0, 32),)),
        "up_weight": bell_draw(splits[11], (D, FF), D ** -0.5, 0.125, ((0, 32),)),
        "up_bias": bell_draw(splits[12], (FF,), 0.5, 3.0, ((0, 32),)),
        "down_weight": bell_draw(splits[13], (D, FF), FF ** -0.5, 0.0625, ((0, 32),)),
        "down_bias": bell_draw(splits[14], (D,), 0.5, 3.0, ((0, 32),)),
    }


EPSILON = 1e-05
NEGATIVE = -1e+30
HIGHEST = lax.Precision.HIGHEST

@jax.custom_vjp
def low(v):
    return lax.optimization_barrier(v.astype(jnp.bfloat16)).astype(jnp.float32)

@jax.custom_vjp
def low_back(v):
    return v

def low_keep(v):
    return (low(v), None)

def low_pass(kept, grad):
    return (grad,)

def back_keep(v):
    return (v, None)

def back_low(kept, grad):
    return (low(grad),)
low.defvjp(low_keep, low_pass)
low_back.defvjp(back_keep, back_low)

def layer_norm(values, gain_vec, shift_vec):
    center = values - lax.optimization_barrier(jnp.mean(values, -1, keepdims=True))
    spread_sq = lax.optimization_barrier(jnp.mean(center * center, -1, keepdims=True))
    return center * lax.rsqrt(spread_sq + EPSILON) * gain_vec + shift_vec

def matmul(left, right):
    return jnp.dot(left, right, precision=HIGHEST, preferred_element_type=jnp.float32)

def cross_dot(left, right):
    return lax.dot_general(left, right, (((1,), (1,)), ((), ())), precision=HIGHEST, preferred_element_type=jnp.float32)

def angles(places):
    halves = ROTARY // 2
    frequency = jnp.exp(jnp.arange(halves, dtype=jnp.float32) * (-2.0 * math.log(10000.0) / ROTARY))
    phases = places.astype(jnp.float32)[..., None] * frequency
    phases = jnp.concatenate([phases, phases], -1)
    return (jnp.cos(phases), jnp.sin(phases))

def rotate(field_in, cosine, sine_vals):
    halves = ROTARY // 2
    rot_part = field_in[..., :ROTARY]
    front_half = rot_part[..., :halves]
    back_half = rot_part[..., halves:]
    turned = jnp.concatenate([-back_half, front_half], -1)
    rotated = rot_part * cosine + turned * sine_vals
    return jnp.concatenate([rotated, field_in[..., ROTARY:]], -1)

def residual_block(sequence, places, weights):
    gain_one, bias_one, gain_two, bias_two, w_qkv, b_qkv, w_out, b_out, w_up, b_up, w_down, b_down = weights
    length = sequence.shape[0]
    model_width = sequence.shape[1]
    normed_one = low(layer_norm(sequence, gain_one, bias_one))
    normed_two = low(layer_norm(sequence, gain_two, bias_two))
    packed = low_back(matmul(normed_one, w_qkv) + b_qkv)
    shaped = packed.reshape(length, 3, HEADS, HEAD_DIM)
    cosine, sine_vals = angles(places)
    cosine = cosine[:, None, :]
    sine_vals = sine_vals[:, None, :]
    queries = low(rotate(shaped[:, 0], cosine, sine_vals))
    keys_all = low(rotate(shaped[:, 1], cosine, sine_vals))
    values = low(shaped[:, 2])
    scores = low_back(jnp.einsum('qhe,khe->hqk', queries, keys_all, precision=HIGHEST) * HEAD_DIM ** (-0.5))
    allowed = places[None, :] <= places[:, None]
    scores = jnp.where(allowed[None], scores, NEGATIVE)
    row_max = lax.optimization_barrier(jnp.max(scores, -1, keepdims=True))
    exponent = jnp.where(allowed[None], jnp.exp(scores - row_max), 0.0)
    attn_weights = low(exponent / lax.optimization_barrier(jnp.sum(exponent, -1, keepdims=True)))
    context = jnp.einsum('hqk,khe->qhe', attn_weights, values, precision=HIGHEST).reshape(length, model_width)
    context = low_back(low(context))
    attended = cross_dot(context, w_out) + b_out
    hidden = low_back(matmul(normed_two, w_up) + b_up)
    activated = low(jax.nn.gelu(hidden, approximate=False))
    projected = cross_dot(activated, w_down) + b_down
    return sequence + attended + projected

def reference(tokens, positions, cotangent, norm1_gain, norm1_bias, norm2_gain, norm2_bias, qkv_weight, qkv_bias, out_weight, out_bias, up_weight, up_bias, down_weight, down_bias):
    params = tuple((element.astype(jnp.float32) for element in (norm1_gain, norm1_bias, norm2_gain, norm2_bias, qkv_weight, qkv_bias, out_weight, out_bias, up_weight, up_bias, down_weight, down_bias)))
    model_width = tokens.shape[-1]
    inputs = tokens.astype(jnp.float32).reshape(SEQS, SEQ_LEN, model_width)
    places = positions.reshape(SEQS, SEQ_LEN)

    def forward(inputs_all, *weights):

        def single(couple):
            return jax.checkpoint(residual_block)(couple[0], couple[1], weights)
        return lax.map(single, (inputs_all, places))
    result, pullback = jax.vjp(forward, inputs, *params)
    gradients = pullback(cotangent.astype(jnp.float32).reshape(SEQS, SEQ_LEN, model_width))
    output = result.reshape(tokens.shape).astype(jnp.bfloat16)
    token_grad = gradients[0].reshape(tokens.shape)
    return (output, token_grad, gradients[1], gradients[2], gradients[3], gradients[4], gradients[5], gradients[6], gradients[7], gradients[8], gradients[9], gradients[10], gradients[11], gradients[12])
```

```python
import functools
import math

import jax
import jax.numpy as jnp
from jax import lax
from jax.experimental import pallas as pl
from jax.experimental.pallas import tpu as pltpu
from jax.sharding import Mesh, PartitionSpec as P


HEADS = 8
HEAD_DIM = 256
ROTARY = 64
EPSILON = 1e-05
NEGATIVE = -1e30
F32 = jnp.float32
BF16 = jnp.bfloat16
ALL = ("zo", "yi", "seq")
GROUP = ("yi", "seq")
MESH = pl.DeviceIdType.MESH
ANY = pl.BlockSpec(memory_space=pl.ANY)


def dot(left, right, dims):
    return lax.dot_general(left, right, (dims, ((), ())), preferred_element_type=F32)


def split_axes(mesh):
    dp, seq = mesh.shape["dp"], mesh.shape["seq"]
    sub = 1
    while seq * sub * 2 <= HEADS and dp % (sub * 2) == 0:
        sub *= 2
    return dp // sub, sub, seq


def remote(source, target, send, recv, device):
    return pltpu.make_async_remote_copy(
        src_ref=source, dst_ref=target, send_sem=send, recv_sem=recv,
        device_id=device, device_id_type=MESH,
    )


class Layout:
    def __init__(self, outer, sub, seq):
        self.outer, self.sub, self.seq = outer, sub, seq
        self.chips_x = seq // 2
        self.group = sub * seq
        self.count = outer * self.group
        self.heads = HEADS // self.group
        self.offsets = [(ry, rx) for ry in range(sub) for rx in range(self.chips_x)]
        self.far = sorted(self.offsets[1:], key=lambda o: (o[0] > 0) + (o[1] > 0))

    def shift(self, ry, rx):
        pairs = []
        for y in range(self.sub):
            for x in range(self.chips_x):
                for c in range(2):
                    there = ((y + ry) % self.sub, (x + rx) % self.chips_x)
                    pairs.append((y * self.seq + x * 2 + c, there[0] * self.seq + there[1] * 2 + c))
        return pairs

    def flip(self):
        return [(i, i ^ 1) for i in range(self.seq)]


def swap_copies(lay, plan, me, sources, targets, send, recv, back):
    zo = lax.axis_index("zo")
    copies = []
    for k in range(1, lay.group):
        peer = lax.rem(me + k, lay.group)
        device = (zo, peer // lay.seq, lax.rem(peer, lay.seq))
        j = 0
        for (parts, rows, cols), source, target in zip(plan, sources, targets, strict=True):
            for part in range(parts):
                wide = lambda who: pl.ds(pl.multiple_of((part * lay.group + who) * cols, 128), cols)
                thin = pl.ds(part * cols, cols)
                block = lambda who: pl.ds(pl.multiple_of(who * rows, rows), rows)
                if back:
                    copies.append(remote(source.at[block(peer), thin], target.at[:, wide(me)], send.at[k - 1, j], recv.at[k - 1, j], device))
                else:
                    copies.append(remote(source.at[:, wide(peer)], target.at[block(me), thin], send.at[k - 1, j], recv.at[k - 1, j], device))
                j += 1
    return copies


def swap_own(lay, plan, me, sources, targets, sems, back):
    copies = []
    j = 0
    for (parts, rows, cols), source, target in zip(plan, sources, targets, strict=True):
        for part in range(parts):
            wide = pl.ds(pl.multiple_of((part * lay.group + me) * cols, 128), cols)
            thin = pl.ds(part * cols, cols)
            block = pl.ds(pl.multiple_of(me * rows, rows), rows)
            if back:
                copies.append(pltpu.make_async_copy(source.at[block, thin], target.at[:, wide], sems.at[j]))
            else:
                copies.append(pltpu.make_async_copy(source.at[:, wide], target.at[block, thin], sems.at[j]))
            j += 1
    return copies


def group_barrier(lay, me):
    zo = lax.axis_index("zo")
    barrier = pltpu.get_barrier_semaphore()
    for k in range(1, lay.group):
        peer = lax.rem(me + k, lay.group)
        pl.semaphore_signal(
            barrier, inc=1, device_id=(zo, peer // lay.seq, lax.rem(peer, lay.seq)), device_id_type=MESH
        )
    pl.semaphore_wait(barrier, lay.group - 1)


def swap_shapes(lay, plan, back):
    if back:
        return [jax.ShapeDtypeStruct((rows, parts * lay.group * cols), BF16) for parts, rows, cols in plan]
    return [jax.ShapeDtypeStruct((lay.group * rows, parts * cols), BF16) for parts, rows, cols in plan]


def exchange_kernel(lay, plan, back, *refs):
    n = len(plan)
    vec_ref, sources = refs[0], refs[1 : 1 + n]
    all_ref, targets = refs[1 + n], refs[2 + n : 2 + 2 * n]
    send, recv, own, vec_send, vec_recv, vec_own = refs[2 + 2 * n :]
    zo = lax.axis_index("zo")
    me = lax.axis_index("yi") * lay.seq + lax.axis_index("seq")
    rank = zo * lay.group + me

    def device_of(k):
        peer = lax.rem(rank + k, lay.count)
        inner = lax.rem(peer, lay.group)
        return (peer // lay.group, inner // lay.seq, lax.rem(inner, lay.seq))

    barrier = pltpu.get_barrier_semaphore()

    def greet(k, carry):
        pl.semaphore_signal(barrier, inc=1, device_id=device_of(k), device_id_type=MESH)
        return carry

    lax.fori_loop(1, lay.count, greet, 0)
    pl.semaphore_wait(barrier, lay.count - 1)
    copies = swap_copies(lay, plan, me, sources, targets, send, recv, back)
    mine = swap_own(lay, plan, me, sources, targets, own, back)
    mine.append(pltpu.make_async_copy(vec_ref, all_ref.at[rank], vec_own))

    def vec_copy(k):
        return remote(vec_ref, all_ref.at[rank], vec_send.at[k - 1], vec_recv.at[k - 1], device_of(k))

    def start(k, carry):
        vec_copy(k).start()
        return carry

    def finish(k, carry):
        vec_copy(k).wait()
        return carry

    lax.fori_loop(1, lay.count, start, 0)
    for copy in copies + mine:
        copy.start()
    lax.fori_loop(1, lay.count, finish, 0)
    for copy in copies + mine:
        copy.wait()


def busy(microseconds):
    return pl.CostEstimate(flops=int(7e8 * microseconds), bytes_accessed=1 << 20, transcendentals=0)


def exchange(lay, plan, vec, arrays, back, number, time):
    count = sum(parts for parts, _, _ in plan)
    return pl.pallas_call(
        functools.partial(exchange_kernel, lay, plan, back),
        out_shape=[jax.ShapeDtypeStruct((lay.count, *vec.shape), F32), *swap_shapes(lay, plan, back)],
        in_specs=[ANY] * (1 + len(plan)),
        out_specs=[ANY] * (1 + len(plan)),
        scratch_shapes=[
            pltpu.SemaphoreType.DMA((lay.group - 1, count)),
            pltpu.SemaphoreType.DMA((lay.group - 1, count)),
            pltpu.SemaphoreType.DMA((count,)),
            pltpu.SemaphoreType.DMA((lay.count - 1,)),
            pltpu.SemaphoreType.DMA((lay.count - 1,)),
            pltpu.SemaphoreType.DMA,
        ],
        compiler_params=pltpu.CompilerParams(collective_id=number, has_side_effects=True),
        cost_estimate=busy(time),
    )(vec, *arrays)


def norm_kernel(lay, plan, *refs):
    n = len(plan)
    x_ref, gain_ref, sources = refs[0], refs[1], refs[2 : 2 + n]
    one_ref, two_ref, hat_ref, targets = *refs[2 + n : 5 + n], refs[5 + n : 5 + 2 * n]
    held, stage, send, recv, core_send, core_recv, w_send, w_recv, w_own, own_sem, out_sem = refs[5 + 2 * n :]
    batch, length, _ = x_ref.shape
    zo, yi, s = lax.axis_index("zo"), lax.axis_index("yi"), lax.axis_index("seq")
    me = yi * lay.seq + s
    x, core = s // 2, lax.rem(s, 2)
    partner = (zo, yi, x * 2 + 1 - core)

    def chip(ry, rx):
        return (zo, lax.rem(yi + ry, lay.sub), lax.rem(x + rx, lay.chips_x) * 2 + core)

    group_barrier(lay, me)
    slot = {offset: i for i, offset in enumerate(lay.offsets)}
    own_copy = pltpu.make_async_copy(x_ref, held.at[0, 0], own_sem)
    own_copy.start()
    straight = [o for o in lay.far if not (o[0] and o[1])]
    diagonal = [o for o in lay.far if o[0] and o[1]]
    copies = {}
    for o in straight:
        copies[o] = [remote(x_ref, held.at[0, slot[o]], send.at[slot[o], 0], recv.at[slot[o], 0], chip(*o))]
    half = batch // 2
    for ry, rx in diagonal:
        j = slot[(ry, rx)]
        copies[(ry, rx)] = [
            remote(held.at[0, slot[(0, rx)], :half], held.at[0, j, :half], send.at[j, 0], recv.at[j, 0], chip(ry, 0)),
            remote(held.at[0, slot[(ry, 0)], half:], held.at[0, j, half:], send.at[j, 1], recv.at[j, 1], chip(0, rx)),
        ]
    to_partner = {
        o: remote(x_ref if o == (0, 0) else held.at[0, slot[o]], held.at[1, slot[o]],
                  core_send.at[slot[o]], core_recv.at[slot[o]], partner)
        for o in lay.offsets
    }
    for o in straight:
        copies[o][0].start()
    to_partner[(0, 0)].start()
    swaps = swap_copies(lay, plan, me, sources, targets, w_send, w_recv, False)
    mine = swap_own(lay, plan, me, sources, targets, w_own, False)
    for copy in swaps + mine:
        copy.start()

    gains = [gain_ref[i : i + 1, :] for i in range(4)]
    rows = 16
    pending = [[], []]
    turn = [0]

    def norm(c, j):
        for m in range(batch):
            k = turn[0] % 2
            turn[0] += 1
            for copy in pending[k]:
                copy.wait()

            def chunk(i, carry):
                at = pl.ds(pl.multiple_of(i * rows, rows), rows)
                value = held[c, j, m, at, :].astype(F32)
                center = value - jnp.mean(value, -1, keepdims=True)
                hat = center * lax.rsqrt(jnp.mean(center * center, -1, keepdims=True) + EPSILON)
                stage[k, 0, at, :] = (hat * gains[0] + gains[1]).astype(BF16)
                stage[k, 1, at, :] = (hat * gains[2] + gains[3]).astype(BF16)
                stage[k, 2, at, :] = hat.astype(BF16)
                return carry

            lax.fori_loop(0, length // rows, chunk, 0)
            pending[k] = [
                pltpu.make_async_copy(stage.at[k, i], ref.at[c, j, m], out_sem.at[k, i])
                for i, ref in enumerate((one_ref, two_ref, hat_ref))
            ]
            for copy in pending[k]:
                copy.start()

    own_copy.wait()
    norm(0, 0)
    to_partner[(0, 0)].wait_recv()
    norm(1, 0)
    for o in straight:
        copies[o][0].wait_recv()
        to_partner[o].start()
        for ry, rx in diagonal:
            if o == (0, rx):
                copies[(ry, rx)][0].start()
            if o == (ry, 0):
                copies[(ry, rx)][1].start()
        norm(0, slot[o])
    for o in straight:
        to_partner[o].wait_recv()
        norm(1, slot[o])
    for o in diagonal:
        for copy in copies[o]:
            copy.wait_recv()
        to_partner[o].start()
        norm(0, slot[o])
    for o in diagonal:
        to_partner[o].wait_recv()
        norm(1, slot[o])
    for side in pending:
        for copy in side:
            copy.wait()
    for o in lay.far:
        for copy in copies[o]:
            copy.wait_send()
    for o in lay.offsets:
        to_partner[o].wait_send()
    for copy in swaps + mine:
        copy.wait()


def norm_exchange(lay, plan, tokens, gains, weights):
    count = sum(parts for parts, _, _ in plan)
    chips = lay.group // 2
    whole = jax.ShapeDtypeStruct((2, chips, *tokens.shape), BF16)
    return pl.pallas_call(
        functools.partial(norm_kernel, lay, plan),
        out_shape=[whole] * 3 + swap_shapes(lay, plan, False),
        in_specs=[ANY, pl.BlockSpec(memory_space=pltpu.VMEM)] + [ANY] * len(plan),
        out_specs=[ANY] * (3 + len(plan)),
        scratch_shapes=[
            pltpu.VMEM((2, chips, *tokens.shape), BF16),
            pltpu.VMEM((2, 3, *tokens.shape[1:]), BF16),
            pltpu.SemaphoreType.DMA((chips, 2)),
            pltpu.SemaphoreType.DMA((chips, 2)),
            pltpu.SemaphoreType.DMA((chips,)),
            pltpu.SemaphoreType.DMA((chips,)),
            pltpu.SemaphoreType.DMA((lay.group - 1, count)),
            pltpu.SemaphoreType.DMA((lay.group - 1, count)),
            pltpu.SemaphoreType.DMA((count,)),
            pltpu.SemaphoreType.DMA,
            pltpu.SemaphoreType.DMA((2, 3)),
        ],
        compiler_params=pltpu.CompilerParams(
            collective_id=1, has_side_effects=True, vmem_limit_bytes=48 << 20
        ),
        cost_estimate=busy(100),
        name="norm_exchange",
    )(tokens, gains, *weights)


def deal_kernel(lay, plan, *refs):
    n = len(plan)
    sources, targets = refs[:n], refs[n : 2 * n]
    send, recv, own = refs[2 * n :]
    me = lax.axis_index("yi") * lay.seq + lax.axis_index("seq")
    group_barrier(lay, me)
    copies = swap_copies(lay, plan, me, sources, targets, send, recv, True)
    copies += swap_own(lay, plan, me, sources, targets, own, True)
    for copy in copies:
        copy.start()
    for copy in copies:
        copy.wait()


def deal_exchange(lay, plan, sums, number):
    count = sum(parts for parts, _, _ in plan)
    return pl.pallas_call(
        functools.partial(deal_kernel, lay, plan),
        out_shape=swap_shapes(lay, plan, True),
        in_specs=[ANY] * len(plan),
        out_specs=[ANY] * len(plan),
        scratch_shapes=[
            pltpu.SemaphoreType.DMA((lay.group - 1, count)),
            pltpu.SemaphoreType.DMA((lay.group - 1, count)),
            pltpu.SemaphoreType.DMA((count,)),
        ],
        compiler_params=pltpu.CompilerParams(collective_id=number, has_side_effects=True),
        cost_estimate=busy(17),
    )(*sums)


def turn_pairs(field, cosine, sine):
    halves = ROTARY // 2
    front = field[:, :128]
    lane = lax.broadcasted_iota(jnp.int32, front.shape, 1)
    other = jnp.where(lane < halves, pltpu.roll(front, 128 - halves, 1), pltpu.roll(front, halves, 1))
    return jnp.concatenate([front * cosine + other * sine, field[:, 128:]], -1)


QUERY_BLOCK = 256


def attend_kernel(scaling, packed_ref, cos_ref, sin_ref, col_ref, row_ref, q_ref, k_ref, v_ref, ctx_ref, lse_ref,
                  q_buf, k_buf, v_buf):
    cores, _, chips, _, length, _ = packed_ref.shape
    for c in range(cores):
        for i in range(chips):
            at = pl.ds((c * chips + i) * length, length)
            block = packed_ref[c, 0, i, 0]
            cosine, sine = cos_ref[0, at, :], sin_ref[0, at, :]
            q_buf[at, :] = turn_pairs(block[:, :HEAD_DIM], cosine, sine).astype(BF16)
            k_buf[at, :] = turn_pairs(block[:, HEAD_DIM : 2 * HEAD_DIM], cosine, sine).astype(BF16)
            v_buf[at, :] = block[:, 2 * HEAD_DIM :].astype(BF16)
    q_ref[0] = q_buf[...]
    k_ref[0] = k_buf[...]
    v_ref[0] = v_buf[...]
    total = cores * chips * length

    def one(j, carry):
        at = pl.ds(pl.multiple_of(j * QUERY_BLOCK, QUERY_BLOCK), QUERY_BLOCK)
        scores = dot(k_buf[...], q_buf[at, :], ((1,), (1,))) * scaling
        allowed = col_ref[0] <= row_ref[0, :, at]
        scores = jnp.where(allowed, scores, NEGATIVE)
        top = jnp.max(scores, 0, keepdims=True)
        weights = jnp.where(allowed, jnp.exp(scores - top), 0.0)
        total_row = jnp.sum(weights, 0, keepdims=True)
        probs = (weights * (1.0 / total_row)).astype(BF16)
        ctx_ref[0, at, :] = dot(probs, v_buf[...], ((0,), (0,))).astype(BF16)
        lse_ref[0, :, at] = top + jnp.log(total_row)
        return carry

    lax.fori_loop(0, total // QUERY_BLOCK, one, 0)


def attend_back_kernel(scaling, q_ref, k_ref, v_ref, g_ref, cos_ref, sin_ref, col_ref, row_ref, lse_ref, out_ref,
                       dq_buf, dk_buf, dv_buf):
    cores, _, chips, _, length, _ = out_ref.shape
    total = q_ref.shape[1]
    dk_buf[...] = jnp.zeros_like(dk_buf)
    dv_buf[...] = jnp.zeros_like(dv_buf)

    def one(j, carry):
        at = pl.ds(pl.multiple_of(j * QUERY_BLOCK, QUERY_BLOCK), QUERY_BLOCK)
        queries = q_ref[0, at, :]
        grads = g_ref[0, at, :]
        scores = dot(k_ref[0], queries, ((1,), (1,))) * scaling
        allowed = col_ref[0] <= row_ref[0, :, at]
        scores = jnp.where(allowed, scores, NEGATIVE)
        probs = jnp.where(allowed, jnp.exp(scores - lse_ref[0, :, at]), 0.0)
        grad_probs = dot(v_ref[0], grads, ((1,), (1,)))
        delta = jnp.sum(probs * grad_probs, 0, keepdims=True)
        grad_scores = (probs * (grad_probs - delta)).astype(BF16)
        dv_buf[...] += dot(probs.astype(BF16), grads, ((1,), (0,)))
        dk_buf[...] += dot(grad_scores, queries, ((1,), (0,)))
        dq_buf[at, :] = dot(grad_scores, k_ref[0], ((0,), (0,)))
        return carry

    lax.fori_loop(0, total // QUERY_BLOCK, one, 0)
    for c in range(cores):
        for i in range(chips):
            at = pl.ds((c * chips + i) * length, length)
            cosine, sine = cos_ref[0, at, :], sin_ref[0, at, :]
            out_ref[c, 0, i, 0, :, :HEAD_DIM] = turn_pairs(dq_buf[at, :] * scaling, cosine, -sine).astype(BF16)
            out_ref[c, 0, i, 0, :, HEAD_DIM : 2 * HEAD_DIM] = turn_pairs(dk_buf[at, :] * scaling, cosine, -sine).astype(BF16)
            out_ref[c, 0, i, 0, :, 2 * HEAD_DIM :] = dv_buf[at, :].astype(BF16)


def make_body(lay):
    sub, seq, group, chips_x = lay.sub, lay.seq, lay.group, lay.chips_x

    def gather_near(value):
        return [value if o == (0, 0) else lax.ppermute(value, GROUP, lay.shift(*o)) for o in lay.offsets]

    def gather_partner(near):
        partner = [lax.ppermute(piece, "seq", lay.flip()) for piece in near]
        return jnp.concatenate([piece[None] for piece in near + partner], 0)

    def reduce_near(kept, given):
        came = lax.ppermute(given, "seq", lay.flip())
        came, kept = lax.optimization_barrier((came, kept))
        return [
            (kept[i].astype(F32) + came[i].astype(F32)).astype(BF16) if o != (0, 0) else kept[i].astype(F32) + came[i].astype(F32)
            for i, o in enumerate(lay.offsets)
        ]

    def reduce_far(pieces):
        total = pieces[0]
        for o, piece in zip(lay.offsets[1:], pieces[1:], strict=True):
            back = ((-o[0]) % sub, (-o[1]) % chips_x)
            came = lax.ppermute(piece, GROUP, lay.shift(*back))
            total = total + came.astype(F32)
        return total

    def after(value, *tokens):
        return lax.optimization_barrier((value, *tokens))[0]

    def step(
        tokens, positions, cotangent, gain1, bias1, gain2, bias2,
        w_qkv, b_qkv, w_out, b_out, w_up, b_up, w_down, b_down,
    ):
        batch, length, width = tokens.shape
        rows = w_qkv.shape[0]
        ff = w_up.shape[1]
        count = seq * length
        total = group * batch * length
        my_seq = lax.axis_index("seq")
        me = lax.axis_index("yi") * seq + my_seq
        scaling = HEAD_DIM ** (-0.5)
        cols = lay.heads * HEAD_DIM
        ff_cols = ff // group
        out_cols = width // group
        plans = {"up": (1, rows, ff_cols), "down": (1, rows, ff_cols), "qkv": (3, rows, cols), "out": (1, rows, out_cols)}

        def gather_rows(mine):
            return lax.all_gather(mine, "zo", axis=0, tiled=True)

        names = (bias1, bias2, gain1, gain2, b_qkv, b_up, b_out, b_down)
        vec = jnp.concatenate([v.astype(F32) for v in names])
        size = -(-vec.shape[0] // 1024) * 1024
        vec = jnp.pad(vec, (0, size - vec.shape[0])).reshape(-1, 128)
        vectors, up_own, qkv_own = exchange(lay, [plans["up"], plans["qkv"]], vec, [w_up, w_qkv], False, 0, 30)
        up_w = gather_rows(up_own)
        qkv_w = gather_rows(qkv_own)
        vectors = vectors.reshape(lay.count, -1)
        cuts = []
        at = 0
        for piece in names:
            cuts.append(vectors[:, at : at + piece.shape[0]].reshape(-1))
            at += piece.shape[0]
        bias1_all, bias2_all, gain1_all, gain2_all, b_qkv_all, b_up_all, b_out_all, b_down_all = cuts
        b_qkv_mine = lax.dynamic_index_in_dim(b_qkv_all.reshape(3, group, cols), me, 1, keepdims=False).reshape(-1)
        b_up_mine = lax.dynamic_index_in_dim(b_up_all.reshape(group, ff_cols), me, 0, keepdims=False)
        zeros = jnp.zeros_like(bias1_all)
        gains = jnp.stack([gain1_all, bias1_all, gain2_all, bias2_all, zeros, zeros, zeros, zeros])
        one, two, hat, out_own, down_own = norm_exchange(lay, [plans["out"], plans["down"]], tokens, gains, [w_out, w_down])
        out_w = gather_rows(out_own)
        down_w = gather_rows(down_own)
        one, two, hat = [v.reshape(total, width) for v in (one, two, hat)]
        cotangent, hat = lax.optimization_barrier((cotangent, hat))
        near_dy = gather_near(cotangent)

        x, core = my_seq // 2, my_seq % 2
        places = []
        for ry in range(sub):
            from_there = positions
            if ry:
                from_there = lax.ppermute(positions, "yi", [(i, (i + ry) % sub) for i in range(sub)])
            blocks = from_there.reshape(batch, seq, length)
            order = [((x - rx) % chips_x) * 2 + (core + rc) % 2 for rc in range(2) for rx in range(chips_x)]
            places.append(jnp.concatenate([lax.dynamic_slice_in_dim(blocks, o, 1, 1) for o in order], 1))
        places = jnp.stack(places).reshape(sub * batch, count)
        halves = ROTARY // 2
        frequency = jnp.exp(jnp.arange(halves, dtype=F32) * (-2.0 * math.log(10000.0) / ROTARY))
        phases = places.astype(F32)[..., None] * frequency
        cosine, sine = jnp.cos(phases), jnp.sin(phases)
        rest = (sub * batch, count, 128 - ROTARY)
        cosine = jnp.concatenate([cosine, cosine, jnp.ones(rest, F32)], -1)
        sine = jnp.concatenate([-sine, sine, jnp.zeros(rest, F32)], -1)
        place_col = places[:, :, None]
        place_row = places[:, None, :]

        hidden = dot(two, up_w, ((1,), (0,))) + b_up_mine
        phi_cdf = 0.5 * (1.0 + lax.erf(hidden * math.sqrt(0.5)))
        density = jnp.exp(-0.5 * hidden * hidden) * (1.0 / math.sqrt(2.0 * math.pi))
        activated = (hidden * phi_cdf).astype(BF16)
        slope = (phi_cdf + hidden * density).astype(BF16)
        activated, slope = lax.optimization_barrier((activated, slope))

        seqs = sub * batch
        one = after(one, activated)
        packed = dot(one, qkv_w, ((1,), (0,))) + b_qkv_mine
        wide = (2, 1, chips_x, 1, length, 3 * cols)
        wide_spec = pl.BlockSpec(wide, lambda i: (0, i // batch, 0, i % batch, 0, 0))
        full = (2, sub, chips_x, batch, length, 3 * cols)
        head_spec = pl.BlockSpec((1, count, HEAD_DIM), lambda i: (i, 0, 0))
        turn_spec = pl.BlockSpec((1, count, 128), lambda i: (i, 0, 0))
        col_spec = pl.BlockSpec((1, count, 1), lambda i: (i, 0, 0))
        row_spec = pl.BlockSpec((1, 1, count), lambda i: (i, 0, 0))
        head_shape = jax.ShapeDtypeStruct((seqs, count, HEAD_DIM), BF16)
        work = 2 * seqs * count * count * HEAD_DIM
        params = pltpu.CompilerParams(vmem_limit_bytes=56 << 20)
        queries, keys, values, context, lse = pl.pallas_call(
            functools.partial(attend_kernel, scaling),
            grid=(seqs,),
            in_specs=[wide_spec, turn_spec, turn_spec, col_spec, row_spec],
            out_specs=[head_spec] * 4 + [row_spec],
            out_shape=[head_shape] * 4 + [jax.ShapeDtypeStruct((seqs, 1, count), F32)],
            scratch_shapes=[pltpu.VMEM((count, HEAD_DIM), BF16)] * 3,
            compiler_params=params,
            cost_estimate=pl.CostEstimate(flops=2 * work, bytes_accessed=30 << 20, transcendentals=seqs * count * count),
            name="attend",
        )(packed.reshape(full), cosine, sine, place_col, place_row)

        def to_tokens(v):
            v = v.reshape(sub, batch, 2, chips_x, length, cols)
            return jnp.transpose(v, (2, 0, 3, 1, 4, 5)).reshape(total, cols)

        def to_heads(v):
            v = v.reshape(2, sub, chips_x, batch, length, cols)
            return jnp.transpose(v, (1, 3, 0, 2, 4, 5)).reshape(seqs, count, cols)

        context = to_tokens(context)

        def scatter(grad):
            return lax.psum_scatter(grad, "zo", scatter_dimension=0, tiled=True)

        def outer_dot(left, right):
            return dot(left, right, ((0,), (0,))).astype(BF16)

        near_dy = lax.optimization_barrier((*near_dy, context))[:-1]
        upstream = gather_partner(list(near_dy)).reshape(total, width)
        down_part = outer_dot(upstream, activated)
        upstream = after(upstream, down_part)
        down_sum = scatter(down_part)
        grad_context = dot(upstream, out_w, ((1,), (0,))).astype(BF16)
        upstream = after(upstream, grad_context)
        out_part = outer_dot(upstream, context)
        out_w_sum = scatter(out_part)

        def two_dots(half, first, first_w, second, second_w):
            size = total // 2
            cut = slice(half * size, (half + 1) * size)
            sums = dot(first[cut], first_w, ((1,), (1,))) + dot(second[cut], second_w, ((1,), (1,)))
            return sums.astype(BF16).reshape(group // 2, batch, length, first_w.shape[0])

        def chain(values, *tokens):
            return lax.optimization_barrier((*values, *tokens))[: len(values)]

        pair = chain((context, activated), out_part)
        given = two_dots(1, pair[0], out_w, pair[1], down_w)
        pair = chain(pair, given)
        kept = two_dots(0, pair[0], out_w, pair[1], down_w)
        out_near = reduce_near(kept, given)
        grad_context, *out_near = chain((grad_context, *out_near))
        out_sum = reduce_far(out_near)
        output = (tokens.astype(F32) + out_sum + b_out_all + b_down_all).astype(BF16)

        grad_packed = pl.pallas_call(
            functools.partial(attend_back_kernel, scaling),
            grid=(seqs,),
            in_specs=[head_spec] * 4 + [turn_spec, turn_spec, col_spec, row_spec, row_spec],
            out_specs=wide_spec,
            out_shape=jax.ShapeDtypeStruct(full, BF16),
            scratch_shapes=[pltpu.VMEM((count, HEAD_DIM), F32)] * 3,
            compiler_params=params,
            cost_estimate=pl.CostEstimate(flops=5 * work, bytes_accessed=24 << 20, transcendentals=seqs * count * count),
            name="attend_back",
        )(queries, keys, values, to_heads(grad_context), cosine, sine, place_col, place_row, lse)
        grad_packed = grad_packed.reshape(total, 3 * cols)

        qkv_part = outer_dot(hat, grad_packed)
        qkv_sum = scatter(qkv_part)
        (upstream,) = chain((upstream,), qkv_part)
        grad_hidden = (dot(upstream, down_w, ((1,), (0,))) * slope.astype(F32)).astype(BF16)
        hat, grad_hidden = chain((hat, grad_hidden))
        up_part = outer_dot(hat, grad_hidden)
        up_sum = scatter(up_part)

        down_sum, out_w_sum = chain((down_sum, out_w_sum), up_part)
        down_raw, out_raw = deal_exchange(lay, [plans["down"], plans["out"]], [down_sum, out_w_sum], 2)

        fold_qkv = (gain1_all[:, None] * qkv_w.astype(F32)).astype(BF16)
        fold_up = (gain2_all[:, None] * up_w.astype(F32)).astype(BF16)
        pair = chain((grad_packed, grad_hidden, fold_qkv, fold_up), down_raw, out_raw)
        normal_sums = []
        chunk = width // 2
        for k in range(2):
            cut = slice(k * chunk, (k + 1) * chunk)
            given = two_dots(1, pair[0], pair[2][cut], pair[1], pair[3][cut])
            pair = chain(pair, given)
            kept = two_dots(0, pair[0], pair[2][cut], pair[1], pair[3][cut])
            near = reduce_near(kept, given)
            both = chain((*pair, *near))
            pair, near = both[:4], both[4:]
            normal_sums.append(reduce_far(near))
        inputs = tokens.astype(F32)
        center = inputs - jnp.mean(inputs, -1, keepdims=True)
        inv_std = lax.rsqrt(jnp.mean(center * center, -1, keepdims=True) + EPSILON)
        normal = center * inv_std
        grad_normal = jnp.concatenate(normal_sums, -1)
        token_grad = cotangent.astype(F32) + inv_std * (
            grad_normal
            - jnp.mean(grad_normal, -1, keepdims=True)
            - normal * jnp.mean(grad_normal * normal, -1, keepdims=True)
        )

        own_sums = [
            jnp.sum(grad_packed.astype(F32), 0),
            jnp.sum(grad_hidden.astype(F32), 0),
            jnp.sum(cotangent.astype(F32), (0, 1)),
        ]
        vec = jnp.concatenate(own_sums)
        size = -(-vec.shape[0] // 1024) * 1024
        vec = jnp.pad(vec, (0, size - vec.shape[0])).reshape(-1, 128)
        rank = lax.axis_index("zo") * group + me
        everyone, up_raw, qkv_raw = exchange(lay, [plans["up"], plans["qkv"]], vec, [up_sum, qkv_sum], True, 3, 25)
        sums = jnp.sum(everyone.reshape(lay.outer, group, -1), 0)
        sum_qkv = jnp.transpose(sums[:, : 3 * cols].reshape(group, 3, cols), (1, 0, 2)).reshape(-1)
        sum_up = sums[:, 3 * cols : 3 * cols + ff_cols].reshape(-1)
        sum_dy = jnp.sum(sums[:, 3 * cols + ff_cols : 3 * cols + ff_cols + width], 0)

        def own_part(vector):
            return lax.dynamic_index_in_dim(vector.reshape(lay.count, -1), rank, 0, keepdims=False)

        up_raw, qkv_raw = up_raw.astype(F32), qkv_raw.astype(F32)
        column = lambda v: v.astype(F32)[:, None]
        return (
            output,
            token_grad,
            jnp.sum(w_qkv.astype(F32) * qkv_raw, 1),
            jnp.sum(w_qkv.astype(F32) * sum_qkv, 1),
            jnp.sum(w_up.astype(F32) * up_raw, 1),
            jnp.sum(w_up.astype(F32) * sum_up, 1),
            column(gain1) * qkv_raw + column(bias1) * sum_qkv,
            own_part(sum_qkv),
            out_raw.astype(F32),
            own_part(sum_dy),
            column(gain2) * up_raw + column(bias2) * sum_up,
            own_part(sum_up),
            down_raw.astype(F32),
            own_part(sum_dy),
        )

    return step


def solution(mesh):
    outer, sub, seq = split_axes(mesh)
    inner = Mesh(mesh.devices.reshape(outer, sub, seq), ALL)
    act = P(None, ALL, None)
    vec = P(ALL)
    mat = P(ALL, None)
    return jax.shard_map(
        make_body(Layout(outer, sub, seq)),
        mesh=inner,
        in_specs=(
            act, P(None, ("zo", "yi")), act, vec, vec, vec, vec,
            mat, vec, mat, vec, mat, vec, mat, vec,
        ),
        out_specs=(act, act, vec, vec, vec, vec, mat, vec, mat, vec, mat, vec, mat, vec),
        check_vma=False,
    )
```

```python
import functools
import math

import jax
import jax.numpy as jnp
from jax import lax
from jax.experimental import pallas as pl
from jax.experimental.pallas import tpu as pltpu
from jax.sharding import Mesh, PartitionSpec as P


HEADS = 8
HEAD_DIM = 256
ROTARY = 64
EPSILON = 1e-05
NEGATIVE = -1e30
F32 = jnp.float32
BF16 = jnp.bfloat16
ALL = ("zo", "yi", "seq")
GROUP = ("yi", "seq")
MESH = pl.DeviceIdType.MESH
ANY = pl.BlockSpec(memory_space=pl.ANY)


def dot(left, right, dims):
    return lax.dot_general(left, right, (dims, ((), ())), preferred_element_type=F32)


def split_axes(mesh):
    dp, seq = mesh.shape["dp"], mesh.shape["seq"]
    sub = 1
    while seq * sub * 2 <= HEADS and dp % (sub * 2) == 0:
        sub *= 2
    return dp // sub, sub, seq


def remote(source, target, send, recv, device):
    return pltpu.make_async_remote_copy(
        src_ref=source, dst_ref=target, send_sem=send, recv_sem=recv,
        device_id=device, device_id_type=MESH,
    )


class Layout:
    def __init__(self, outer, sub, seq):
        self.outer, self.sub, self.seq = outer, sub, seq
        self.chips_x = seq // 2
        self.group = sub * seq
        self.count = outer * self.group
        self.heads = HEADS // self.group
        self.offsets = [(ry, rx) for ry in range(sub) for rx in range(self.chips_x)]
        self.far = sorted(self.offsets[1:], key=lambda o: (o[0] > 0) + (o[1] > 0))

    def shift(self, ry, rx):
        pairs = []
        for y in range(self.sub):
            for x in range(self.chips_x):
                for c in range(2):
                    there = ((y + ry) % self.sub, (x + rx) % self.chips_x)
                    pairs.append((y * self.seq + x * 2 + c, there[0] * self.seq + there[1] * 2 + c))
        return pairs

    def flip(self):
        return [(i, i ^ 1) for i in range(self.seq)]


def swap_copies(lay, plan, me, sources, targets, send, recv, back):
    zo = lax.axis_index("zo")
    copies = []
    for k in range(1, lay.group):
        peer = lax.rem(me + k, lay.group)
        device = (zo, peer // lay.seq, lax.rem(peer, lay.seq))
        j = 0
        for (parts, rows, cols), source, target in zip(plan, sources, targets, strict=True):
            for part in range(parts):
                wide = lambda who: pl.ds(pl.multiple_of((part * lay.group + who) * cols, 128), cols)
                thin = pl.ds(part * cols, cols)
                block = lambda who: pl.ds(pl.multiple_of(who * rows, rows), rows)
                if back:
                    copies.append(remote(source.at[block(peer), thin], target.at[:, wide(me)], send.at[k - 1, j], recv.at[k - 1, j], device))
                else:
                    copies.append(remote(source.at[:, wide(peer)], target.at[block(me), thin], send.at[k - 1, j], recv.at[k - 1, j], device))
                j += 1
    return copies


def swap_own(lay, plan, me, sources, targets, sems, back):
    copies = []
    j = 0
    for (parts, rows, cols), source, target in zip(plan, sources, targets, strict=True):
        for part in range(parts):
            wide = pl.ds(pl.multiple_of((part * lay.group + me) * cols, 128), cols)
            thin = pl.ds(part * cols, cols)
            block = pl.ds(pl.multiple_of(me * rows, rows), rows)
            if back:
                copies.append(pltpu.make_async_copy(source.at[block, thin], target.at[:, wide], sems.at[j]))
            else:
                copies.append(pltpu.make_async_copy(source.at[:, wide], target.at[block, thin], sems.at[j]))
            j += 1
    return copies


def group_barrier(lay, me):
    zo = lax.axis_index("zo")
    barrier = pltpu.get_barrier_semaphore()
    for k in range(1, lay.group):
        peer = lax.rem(me + k, lay.group)
        pl.semaphore_signal(
            barrier, inc=1, device_id=(zo, peer // lay.seq, lax.rem(peer, lay.seq)), device_id_type=MESH
        )
    pl.semaphore_wait(barrier, lay.group - 1)


def swap_shapes(lay, plan, back):
    if back:
        return [jax.ShapeDtypeStruct((rows, parts * lay.group * cols), BF16) for parts, rows, cols in plan]
    return [jax.ShapeDtypeStruct((lay.group * rows, parts * cols), BF16) for parts, rows, cols in plan]


def exchange_kernel(lay, plan, back, *refs):
    n = len(plan)
    vec_ref, sources = refs[0], refs[1 : 1 + n]
    all_ref, targets = refs[1 + n], refs[2 + n : 2 + 2 * n]
    send, recv, own, vec_send, vec_recv, vec_own = refs[2 + 2 * n :]
    zo = lax.axis_index("zo")
    me = lax.axis_index("yi") * lay.seq + lax.axis_index("seq")
    rank = zo * lay.group + me

    def device_of(k):
        peer = lax.rem(rank + k, lay.count)
        inner = lax.rem(peer, lay.group)
        return (peer // lay.group, inner // lay.seq, lax.rem(inner, lay.seq))

    barrier = pltpu.get_barrier_semaphore()

    def greet(k, carry):
        pl.semaphore_signal(barrier, inc=1, device_id=device_of(k), device_id_type=MESH)
        return carry

    lax.fori_loop(1, lay.count, greet, 0)
    pl.semaphore_wait(barrier, lay.count - 1)
    copies = swap_copies(lay, plan, me, sources, targets, send, recv, back)
    mine = swap_own(lay, plan, me, sources, targets, own, back)
    mine.append(pltpu.make_async_copy(vec_ref, all_ref.at[rank], vec_own))

    def vec_copy(k):
        return remote(vec_ref, all_ref.at[rank], vec_send.at[k - 1], vec_recv.at[k - 1], device_of(k))

    def start(k, carry):
        vec_copy(k).start()
        return carry

    def finish(k, carry):
        vec_copy(k).wait()
        return carry

    lax.fori_loop(1, lay.count, start, 0)
    for copy in copies + mine:
        copy.start()
    lax.fori_loop(1, lay.count, finish, 0)
    for copy in copies + mine:
        copy.wait()


def busy(microseconds):
    return pl.CostEstimate(flops=int(7e8 * microseconds), bytes_accessed=1 << 20, transcendentals=0)


def exchange(lay, plan, vec, arrays, back, number, time):
    count = sum(parts for parts, _, _ in plan)
    return pl.pallas_call(
        functools.partial(exchange_kernel, lay, plan, back),
        out_shape=[jax.ShapeDtypeStruct((lay.count, *vec.shape), F32), *swap_shapes(lay, plan, back)],
        in_specs=[ANY] * (1 + len(plan)),
        out_specs=[ANY] * (1 + len(plan)),
        scratch_shapes=[
            pltpu.SemaphoreType.DMA((lay.group - 1, count)),
            pltpu.SemaphoreType.DMA((lay.group - 1, count)),
            pltpu.SemaphoreType.DMA((count,)),
            pltpu.SemaphoreType.DMA((lay.count - 1,)),
            pltpu.SemaphoreType.DMA((lay.count - 1,)),
            pltpu.SemaphoreType.DMA,
        ],
        compiler_params=pltpu.CompilerParams(collective_id=number, has_side_effects=True),
        cost_estimate=busy(time),
    )(vec, *arrays)


def norm_kernel(lay, plan, *refs):
    n = len(plan)
    x_ref, gain_ref, sources = refs[0], refs[1], refs[2 : 2 + n]
    one_ref, two_ref, hat_ref, targets = *refs[2 + n : 5 + n], refs[5 + n : 5 + 2 * n]
    held, stage, send, recv, core_send, core_recv, w_send, w_recv, w_own, own_sem, out_sem = refs[5 + 2 * n :]
    batch, length, _ = x_ref.shape
    zo, yi, s = lax.axis_index("zo"), lax.axis_index("yi"), lax.axis_index("seq")
    me = yi * lay.seq + s
    x, core = s // 2, lax.rem(s, 2)
    partner = (zo, yi, x * 2 + 1 - core)

    def chip(ry, rx):
        return (zo, lax.rem(yi + ry, lay.sub), lax.rem(x + rx, lay.chips_x) * 2 + core)

    group_barrier(lay, me)
    slot = {offset: i for i, offset in enumerate(lay.offsets)}
    own_copy = pltpu.make_async_copy(x_ref, held.at[0, 0], own_sem)
    own_copy.start()
    straight = [o for o in lay.far if not (o[0] and o[1])]
    diagonal = [o for o in lay.far if o[0] and o[1]]
    copies = {}
    for o in straight:
        copies[o] = [remote(x_ref, held.at[0, slot[o]], send.at[slot[o], 0], recv.at[slot[o], 0], chip(*o))]
    half = batch // 2
    for ry, rx in diagonal:
        j = slot[(ry, rx)]
        copies[(ry, rx)] = [
            remote(held.at[0, slot[(0, rx)], :half], held.at[0, j, :half], send.at[j, 0], recv.at[j, 0], chip(ry, 0)),
            remote(held.at[0, slot[(ry, 0)], half:], held.at[0, j, half:], send.at[j, 1], recv.at[j, 1], chip(0, rx)),
        ]
    to_partner = {
        o: remote(x_ref if o == (0, 0) else held.at[0, slot[o]], held.at[1, slot[o]],
                  core_send.at[slot[o]], core_recv.at[slot[o]], partner)
        for o in lay.offsets
    }
    for o in straight:
        copies[o][0].start()
    to_partner[(0, 0)].start()
    swaps = swap_copies(lay, plan, me, sources, targets, w_send, w_recv, False)
    mine = swap_own(lay, plan, me, sources, targets, w_own, False)
    for copy in swaps + mine:
        copy.start()

    gains = [gain_ref[i : i + 1, :] for i in range(4)]
    rows = 16
    pending = [[], []]
    turn = [0]

    def norm(c, j):
        for m in range(batch):
            k = turn[0] % 2
            turn[0] += 1
            for copy in pending[k]:
                copy.wait()

            def chunk(i, carry):
                at = pl.ds(pl.multiple_of(i * rows, rows), rows)
                value = held[c, j, m, at, :].astype(F32)
                center = value - jnp.mean(value, -1, keepdims=True)
                hat = center * lax.rsqrt(jnp.mean(center * center, -1, keepdims=True) + EPSILON)
                stage[k, 0, at, :] = (hat * gains[0] + gains[1]).astype(BF16)
                stage[k, 1, at, :] = (hat * gains[2] + gains[3]).astype(BF16)
                stage[k, 2, at, :] = hat.astype(BF16)
                return carry

            lax.fori_loop(0, length // rows, chunk, 0)
            pending[k] = [
                pltpu.make_async_copy(stage.at[k, i], ref.at[c, j, m], out_sem.at[k, i])
                for i, ref in enumerate((one_ref, two_ref, hat_ref))
            ]
            for copy in pending[k]:
                copy.start()

    own_copy.wait()
    norm(0, 0)
    to_partner[(0, 0)].wait_recv()
    norm(1, 0)
    for o in straight:
        copies[o][0].wait_recv()
        to_partner[o].start()
        for ry, rx in diagonal:
            if o == (0, rx):
                copies[(ry, rx)][0].start()
            if o == (ry, 0):
                copies[(ry, rx)][1].start()
        norm(0, slot[o])
    for o in straight:
        to_partner[o].wait_recv()
        norm(1, slot[o])
    for o in diagonal:
        for copy in copies[o]:
            copy.wait_recv()
        to_partner[o].start()
        norm(0, slot[o])
    for o in diagonal:
        to_partner[o].wait_recv()
        norm(1, slot[o])
    for side in pending:
        for copy in side:
            copy.wait()
    for o in lay.far:
        for copy in copies[o]:
            copy.wait_send()
    for o in lay.offsets:
        to_partner[o].wait_send()
    for copy in swaps + mine:
        copy.wait()


def norm_exchange(lay, plan, tokens, gains, weights):
    count = sum(parts for parts, _, _ in plan)
    chips = lay.group // 2
    whole = jax.ShapeDtypeStruct((2, chips, *tokens.shape), BF16)
    return pl.pallas_call(
        functools.partial(norm_kernel, lay, plan),
        out_shape=[whole] * 3 + swap_shapes(lay, plan, False),
        in_specs=[ANY, pl.BlockSpec(memory_space=pltpu.VMEM)] + [ANY] * len(plan),
        out_specs=[ANY] * (3 + len(plan)),
        scratch_shapes=[
            pltpu.VMEM((2, chips, *tokens.shape), BF16),
            pltpu.VMEM((2, 3, *tokens.shape[1:]), BF16),
            pltpu.SemaphoreType.DMA((chips, 2)),
            pltpu.SemaphoreType.DMA((chips, 2)),
            pltpu.SemaphoreType.DMA((chips,)),
            pltpu.SemaphoreType.DMA((chips,)),
            pltpu.SemaphoreType.DMA((lay.group - 1, count)),
            pltpu.SemaphoreType.DMA((lay.group - 1, count)),
            pltpu.SemaphoreType.DMA((count,)),
            pltpu.SemaphoreType.DMA,
            pltpu.SemaphoreType.DMA((2, 3)),
        ],
        compiler_params=pltpu.CompilerParams(
            collective_id=1, has_side_effects=True, vmem_limit_bytes=48 << 20
        ),
        cost_estimate=busy(100),
        name="norm_exchange",
    )(tokens, gains, *weights)


def deal_kernel(lay, plan, *refs):
    n = len(plan)
    sources, targets = refs[:n], refs[n : 2 * n]
    send, recv, own = refs[2 * n :]
    me = lax.axis_index("yi") * lay.seq + lax.axis_index("seq")
    group_barrier(lay, me)
    copies = swap_copies(lay, plan, me, sources, targets, send, recv, True)
    copies += swap_own(lay, plan, me, sources, targets, own, True)
    for copy in copies:
        copy.start()
    for copy in copies:
        copy.wait()


def deal_exchange(lay, plan, sums, number):
    count = sum(parts for parts, _, _ in plan)
    return pl.pallas_call(
        functools.partial(deal_kernel, lay, plan),
        out_shape=swap_shapes(lay, plan, True),
        in_specs=[ANY] * len(plan),
        out_specs=[ANY] * len(plan),
        scratch_shapes=[
            pltpu.SemaphoreType.DMA((lay.group - 1, count)),
            pltpu.SemaphoreType.DMA((lay.group - 1, count)),
            pltpu.SemaphoreType.DMA((count,)),
        ],
        compiler_params=pltpu.CompilerParams(collective_id=number, has_side_effects=True),
        cost_estimate=busy(17),
    )(*sums)


def pair_kernel(lay, first_ref, first_w, second_ref, second_w, *refs):
    step = pl.program_id(0)
    chips = lay.group // 2
    outs, (given, came, send, recv, out_sem) = refs[:chips], refs[chips:]
    zo, yi, s = lax.axis_index("zo"), lax.axis_index("yi"), lax.axis_index("seq")
    partner = (zo, yi, (s // 2) * 2 + 1 - lax.rem(s, 2))

    def copy(j):
        return remote(given.at[j], came.at[j], send.at[j], recv.at[j], partner)

    def store(j):
        return pltpu.make_async_copy(came.at[j], outs[(j + 1) % chips], out_sem.at[j])

    @pl.when(step == 0)
    def _():
        barrier = pltpu.get_barrier_semaphore()
        pl.semaphore_signal(barrier, inc=1, device_id=partner, device_id_type=MESH)
        pl.semaphore_wait(barrier, 1)

    for j in range(chips):

        @pl.when(step == j + 1)
        def _():
            copy(j).start()

    total = dot(first_ref[0, 0], first_w[...], ((1,), (1,))) + dot(second_ref[0, 0], second_w[...], ((1,), (1,)))
    for j in range(chips):

        @pl.when(step == j)
        def _():
            given[j] = total.astype(BF16)

        @pl.when(step == chips + j)
        def _():
            copy(j).wait_recv()
            came[j] = (total + came[j].astype(F32)).astype(BF16)

    for j in range(chips - 1):

        @pl.when(step == chips + j + 1)
        def _():
            store(j).start()

    @pl.when(step == 2 * chips - 1)
    def _():
        store(chips - 1).start()
        for j in range(chips):
            copy(j).wait_send()
            store(j).wait()


def pair_matmul(lay, first, first_w, second, second_w, cut, number):
    chips = lay.group // 2
    rows = first.shape[0] // lay.group
    width = first_w.shape[0] // cut[1]
    depth1, depth2 = first.shape[1], second.shape[1]

    def act(depth):
        return pl.BlockSpec((1, 1, rows, depth), lambda i: (1 - i // chips, (i + 1) % chips, 0, 0))

    def weight(depth):
        return pl.BlockSpec((width, depth), lambda i: (cut[0], 0), pipeline_mode=pl.Buffered(1))

    shape = lambda v: v.reshape(2, chips, rows, v.shape[1])
    return pl.pallas_call(
        functools.partial(pair_kernel, lay),
        grid=(2 * chips,),
        in_specs=[act(depth1), weight(depth1), act(depth2), weight(depth2)],
        out_specs=[ANY] * chips,
        out_shape=[jax.ShapeDtypeStruct((rows, width), BF16)] * chips,
        scratch_shapes=[
            pltpu.VMEM((chips, rows, width), BF16),
            pltpu.VMEM((chips, rows, width), BF16),
            pltpu.SemaphoreType.DMA((chips,)),
            pltpu.SemaphoreType.DMA((chips,)),
            pltpu.SemaphoreType.DMA((chips,)),
        ],
        compiler_params=pltpu.CompilerParams(
            collective_id=number, has_side_effects=True, vmem_limit_bytes=60 << 20
        ),
        cost_estimate=pl.CostEstimate(
            flops=2 * first.shape[0] * (depth1 + depth2) * width, bytes_accessed=32 << 20, transcendentals=0
        ),
    )(shape(first), first_w, shape(second), second_w)


def turn_pairs(field, cosine, sine):
    halves = ROTARY // 2
    front = field[:, :128]
    lane = lax.broadcasted_iota(jnp.int32, front.shape, 1)
    other = jnp.where(lane < halves, pltpu.roll(front, 128 - halves, 1), pltpu.roll(front, halves, 1))
    return jnp.concatenate([front * cosine + other * sine, field[:, 128:]], -1)


QUERY_BLOCK = 256


def attend_kernel(scaling, packed_ref, cos_ref, sin_ref, col_ref, row_ref, q_ref, k_ref, v_ref, ctx_ref, lse_ref,
                  q_buf, k_buf, v_buf):
    cores, _, chips, _, length, _ = packed_ref.shape
    for c in range(cores):
        for i in range(chips):
            at = pl.ds((c * chips + i) * length, length)
            block = packed_ref[c, 0, i, 0]
            cosine, sine = cos_ref[0, at, :], sin_ref[0, at, :]
            q_buf[at, :] = turn_pairs(block[:, :HEAD_DIM], cosine, sine).astype(BF16)
            k_buf[at, :] = turn_pairs(block[:, HEAD_DIM : 2 * HEAD_DIM], cosine, sine).astype(BF16)
            v_buf[at, :] = block[:, 2 * HEAD_DIM :].astype(BF16)
    q_ref[0] = q_buf[...]
    k_ref[0] = k_buf[...]
    v_ref[0] = v_buf[...]
    total = cores * chips * length

    def one(j, carry):
        at = pl.ds(pl.multiple_of(j * QUERY_BLOCK, QUERY_BLOCK), QUERY_BLOCK)
        scores = dot(k_buf[...], q_buf[at, :], ((1,), (1,))) * scaling
        allowed = col_ref[0] <= row_ref[0, :, at]
        scores = jnp.where(allowed, scores, NEGATIVE)
        top = jnp.max(scores, 0, keepdims=True)
        weights = jnp.where(allowed, jnp.exp(scores - top), 0.0)
        total_row = jnp.sum(weights, 0, keepdims=True)
        probs = (weights * (1.0 / total_row)).astype(BF16)
        ctx_ref[0, at, :] = dot(probs, v_buf[...], ((0,), (0,))).astype(BF16)
        lse_ref[0, :, at] = top + jnp.log(total_row)
        return carry

    lax.fori_loop(0, total // QUERY_BLOCK, one, 0)


def attend_back_kernel(scaling, q_ref, k_ref, v_ref, g_ref, cos_ref, sin_ref, col_ref, row_ref, lse_ref, out_ref,
                       dq_buf, dk_buf, dv_buf):
    cores, _, chips, _, length, _ = out_ref.shape
    total = q_ref.shape[1]
    dk_buf[...] = jnp.zeros_like(dk_buf)
    dv_buf[...] = jnp.zeros_like(dv_buf)

    def one(j, carry):
        at = pl.ds(pl.multiple_of(j * QUERY_BLOCK, QUERY_BLOCK), QUERY_BLOCK)
        queries = q_ref[0, at, :]
        grads = g_ref[0, at, :]
        scores = dot(k_ref[0], queries, ((1,), (1,))) * scaling
        allowed = col_ref[0] <= row_ref[0, :, at]
        scores = jnp.where(allowed, scores, NEGATIVE)
        probs = jnp.where(allowed, jnp.exp(scores - lse_ref[0, :, at]), 0.0)
        grad_probs = dot(v_ref[0], grads, ((1,), (1,)))
        delta = jnp.sum(probs * grad_probs, 0, keepdims=True)
        grad_scores = (probs * (grad_probs - delta)).astype(BF16)
        dv_buf[...] += dot(probs.astype(BF16), grads, ((1,), (0,)))
        dk_buf[...] += dot(grad_scores, queries, ((1,), (0,)))
        dq_buf[at, :] = dot(grad_scores, k_ref[0], ((0,), (0,)))
        return carry

    lax.fori_loop(0, total // QUERY_BLOCK, one, 0)
    for c in range(cores):
        for i in range(chips):
            at = pl.ds((c * chips + i) * length, length)
            cosine, sine = cos_ref[0, at, :], sin_ref[0, at, :]
            out_ref[c, 0, i, 0, :, :HEAD_DIM] = turn_pairs(dq_buf[at, :] * scaling, cosine, -sine).astype(BF16)
            out_ref[c, 0, i, 0, :, HEAD_DIM : 2 * HEAD_DIM] = turn_pairs(dk_buf[at, :] * scaling, cosine, -sine).astype(BF16)
            out_ref[c, 0, i, 0, :, 2 * HEAD_DIM :] = dv_buf[at, :].astype(BF16)


def make_body(lay):
    sub, seq, group, chips_x = lay.sub, lay.seq, lay.group, lay.chips_x

    def gather_near(value):
        return [value if o == (0, 0) else lax.ppermute(value, GROUP, lay.shift(*o)) for o in lay.offsets]

    def gather_partner(near):
        partner = [lax.ppermute(piece, "seq", lay.flip()) for piece in near]
        return jnp.concatenate([piece[None] for piece in near + partner], 0)

    def send_far(pieces):
        came = [pieces[0]]
        for o, piece in zip(lay.offsets[1:], pieces[1:], strict=True):
            back = ((-o[0]) % sub, (-o[1]) % chips_x)
            came.append(lax.ppermute(piece, GROUP, lay.shift(*back)))
        return came

    def add_all(pieces):
        total = pieces[0].astype(F32)
        for piece in pieces[1:]:
            total = total + piece.astype(F32)
        return total

    def after(value, *tokens):
        return lax.optimization_barrier((value, *tokens))[0]

    def step(
        tokens, positions, cotangent, gain1, bias1, gain2, bias2,
        w_qkv, b_qkv, w_out, b_out, w_up, b_up, w_down, b_down,
    ):
        batch, length, width = tokens.shape
        rows = w_qkv.shape[0]
        ff = w_up.shape[1]
        count = seq * length
        total = group * batch * length
        my_seq = lax.axis_index("seq")
        me = lax.axis_index("yi") * seq + my_seq
        scaling = HEAD_DIM ** (-0.5)
        cols = lay.heads * HEAD_DIM
        ff_cols = ff // group
        out_cols = width // group
        plans = {"up": (1, rows, ff_cols), "down": (1, rows, ff_cols), "qkv": (3, rows, cols), "out": (1, rows, out_cols)}

        def gather_rows(mine):
            return lax.all_gather(mine, "zo", axis=0, tiled=True)

        x, core = my_seq // 2, my_seq % 2
        places = []
        for ry in range(sub):
            from_there = positions
            if ry:
                from_there = lax.ppermute(positions, "yi", [(i, (i + ry) % sub) for i in range(sub)])
            blocks = from_there.reshape(batch, seq, length)
            order = [((x - rx) % chips_x) * 2 + (core + rc) % 2 for rc in range(2) for rx in range(chips_x)]
            places.append(jnp.concatenate([lax.dynamic_slice_in_dim(blocks, o, 1, 1) for o in order], 1))
        places = jnp.stack(places).reshape(sub * batch, count)
        names = (bias1, bias2, gain1, gain2, b_qkv, b_up, b_out, b_down)
        vec = jnp.concatenate([v.astype(F32) for v in names])
        size = -(-vec.shape[0] // 1024) * 1024
        vec = jnp.pad(vec, (0, size - vec.shape[0])).reshape(-1, 128)
        vec, places = lax.optimization_barrier((vec, places))
        vectors, up_own, qkv_own = exchange(lay, [plans["up"], plans["qkv"]], vec, [w_up, w_qkv], False, 0, 30)
        up_w = gather_rows(up_own)
        qkv_w = gather_rows(qkv_own)
        vectors = vectors.reshape(lay.count, -1)
        cuts = []
        at = 0
        for piece in names:
            cuts.append(vectors[:, at : at + piece.shape[0]].reshape(-1))
            at += piece.shape[0]
        bias1_all, bias2_all, gain1_all, gain2_all, b_qkv_all, b_up_all, b_out_all, b_down_all = cuts
        b_qkv_mine = lax.dynamic_index_in_dim(b_qkv_all.reshape(3, group, cols), me, 1, keepdims=False).reshape(-1)
        b_up_mine = lax.dynamic_index_in_dim(b_up_all.reshape(group, ff_cols), me, 0, keepdims=False)
        zeros = jnp.zeros_like(bias1_all)
        gains = jnp.stack([gain1_all, bias1_all, gain2_all, bias2_all, zeros, zeros, zeros, zeros])
        one, two, hat, out_own, down_own = norm_exchange(lay, [plans["out"], plans["down"]], tokens, gains, [w_out, w_down])
        out_w = gather_rows(out_own)
        down_w = gather_rows(down_own)
        one, two, hat = [v.reshape(total, width) for v in (one, two, hat)]
        cotangent, hat = lax.optimization_barrier((cotangent, hat))
        near_dy = gather_near(cotangent)

        hidden = dot(two, up_w, ((1,), (0,))) + b_up_mine
        phi_cdf = 0.5 * (1.0 + lax.erf(hidden * math.sqrt(0.5)))
        density = jnp.exp(-0.5 * hidden * hidden) * (1.0 / math.sqrt(2.0 * math.pi))
        activated = (hidden * phi_cdf).astype(BF16)
        slope = (phi_cdf + hidden * density).astype(BF16)
        activated, slope = lax.optimization_barrier((activated, slope))

        halves = ROTARY // 2
        frequency = jnp.exp(jnp.arange(halves, dtype=F32) * (-2.0 * math.log(10000.0) / ROTARY))
        places = after(places, activated)
        phases = places.astype(F32)[..., None] * frequency
        cosine, sine = jnp.cos(phases), jnp.sin(phases)
        rest = (sub * batch, count, 128 - ROTARY)
        cosine = jnp.concatenate([cosine, cosine, jnp.ones(rest, F32)], -1)
        sine = jnp.concatenate([-sine, sine, jnp.zeros(rest, F32)], -1)
        place_col = places[:, :, None]
        place_row = places[:, None, :]

        seqs = sub * batch
        one = after(one, cosine, sine)
        packed = dot(one, qkv_w, ((1,), (0,))) + b_qkv_mine
        wide = (2, 1, chips_x, 1, length, 3 * cols)
        wide_spec = pl.BlockSpec(wide, lambda i: (0, i // batch, 0, i % batch, 0, 0))
        full = (2, sub, chips_x, batch, length, 3 * cols)
        head_spec = pl.BlockSpec((1, count, HEAD_DIM), lambda i: (i, 0, 0))
        turn_spec = pl.BlockSpec((1, count, 128), lambda i: (i, 0, 0))
        col_spec = pl.BlockSpec((1, count, 1), lambda i: (i, 0, 0))
        row_spec = pl.BlockSpec((1, 1, count), lambda i: (i, 0, 0))
        head_shape = jax.ShapeDtypeStruct((seqs, count, HEAD_DIM), BF16)
        work = 2 * seqs * count * count * HEAD_DIM
        params = pltpu.CompilerParams(vmem_limit_bytes=56 << 20)
        queries, keys, values, context, lse = pl.pallas_call(
            functools.partial(attend_kernel, scaling),
            grid=(seqs,),
            in_specs=[wide_spec, turn_spec, turn_spec, col_spec, row_spec],
            out_specs=[head_spec] * 4 + [row_spec],
            out_shape=[head_shape] * 4 + [jax.ShapeDtypeStruct((seqs, 1, count), F32)],
            scratch_shapes=[pltpu.VMEM((count, HEAD_DIM), BF16)] * 3,
            compiler_params=params,
            cost_estimate=pl.CostEstimate(flops=2 * work, bytes_accessed=30 << 20, transcendentals=seqs * count * count),
            name="attend",
        )(packed.reshape(full), cosine, sine, place_col, place_row)

        def to_tokens(v):
            v = v.reshape(sub, batch, 2, chips_x, length, cols)
            return jnp.transpose(v, (2, 0, 3, 1, 4, 5)).reshape(total, cols)

        def to_heads(v):
            v = v.reshape(2, sub, chips_x, batch, length, cols)
            return jnp.transpose(v, (1, 3, 0, 2, 4, 5)).reshape(seqs, count, cols)

        context = to_tokens(context)

        def scatter(grad):
            return lax.psum_scatter(grad, "zo", scatter_dimension=0, tiled=True)

        def outer_dot(left, right):
            return dot(left, right, ((0,), (0,))).astype(BF16)

        near_dy = lax.optimization_barrier((*near_dy, context))[:-1]
        upstream = gather_partner(list(near_dy)).reshape(total, width)
        down_part = outer_dot(upstream, activated)
        upstream = after(upstream, down_part)
        down_sum = scatter(down_part)
        grad_context = dot(upstream, out_w, ((1,), (0,))).astype(BF16)
        upstream = after(upstream, grad_context)
        out_part = outer_dot(upstream, context)
        out_w_sum = scatter(out_part)

        def chain(values, *tokens):
            return lax.optimization_barrier((*values, *tokens))[: len(values)]

        def tokens_of(pieces):
            return [piece.reshape(batch, length, -1) for piece in pieces]

        pair = chain((context, activated), out_part)
        out_near = pair_matmul(lay, pair[0], out_w, pair[1], down_w, (0, 1), 4)
        grad_context, *out_near = chain((grad_context, *out_near))
        out_near = tokens_of(out_near)
        out_sum = add_all(send_far(out_near))
        output = (tokens.astype(F32) + out_sum + b_out_all + b_down_all).astype(BF16)

        grad_packed = pl.pallas_call(
            functools.partial(attend_back_kernel, scaling),
            grid=(seqs,),
            in_specs=[head_spec] * 4 + [turn_spec, turn_spec, col_spec, row_spec, row_spec],
            out_specs=wide_spec,
            out_shape=jax.ShapeDtypeStruct(full, BF16),
            scratch_shapes=[pltpu.VMEM((count, HEAD_DIM), F32)] * 3,
            compiler_params=params,
            cost_estimate=pl.CostEstimate(flops=5 * work, bytes_accessed=24 << 20, transcendentals=seqs * count * count),
            name="attend_back",
        )(queries, keys, values, to_heads(grad_context), cosine, sine, place_col, place_row, lse)
        grad_packed = grad_packed.reshape(total, 3 * cols)

        qkv_part = outer_dot(hat, grad_packed)
        qkv_sum = scatter(qkv_part)
        (upstream,) = chain((upstream,), qkv_part)
        grad_hidden = (dot(upstream, down_w, ((1,), (0,))) * slope.astype(F32)).astype(BF16)

        fold_qkv = (gain1_all[:, None] * qkv_w.astype(F32)).astype(BF16)
        fold_up = (gain2_all[:, None] * up_w.astype(F32)).astype(BF16)
        left = grad_packed
        came = []
        for k in range(2):
            near = pair_matmul(lay, left, fold_qkv, grad_hidden, fold_up, (k, 2), 5 + k)
            left, *near = chain((left, *near))
            came.append(send_far(tokens_of(near)))

        hat, grad_hidden = chain((hat, grad_hidden), left)
        up_part = outer_dot(hat, grad_hidden)
        up_sum = scatter(up_part)
        down_sum, out_w_sum = chain((down_sum, out_w_sum), up_part)
        down_raw, out_raw = deal_exchange(lay, [plans["down"], plans["out"]], [down_sum, out_w_sum], 2)

        inputs = tokens.astype(F32)
        center = inputs - jnp.mean(inputs, -1, keepdims=True)
        inv_std = lax.rsqrt(jnp.mean(center * center, -1, keepdims=True) + EPSILON)
        normal = center * inv_std
        came[1] = chain(came[1], down_raw, out_raw)
        grad_normal = jnp.concatenate([add_all(pieces) for pieces in came], -1)
        token_grad = cotangent.astype(F32) + inv_std * (
            grad_normal
            - jnp.mean(grad_normal, -1, keepdims=True)
            - normal * jnp.mean(grad_normal * normal, -1, keepdims=True)
        )

        own_sums = [
            jnp.sum(grad_packed.astype(F32), 0),
            jnp.sum(grad_hidden.astype(F32), 0),
            jnp.sum(cotangent.astype(F32), (0, 1)),
        ]
        vec = jnp.concatenate(own_sums)
        size = -(-vec.shape[0] // 1024) * 1024
        vec = jnp.pad(vec, (0, size - vec.shape[0])).reshape(-1, 128)
        rank = lax.axis_index("zo") * group + me
        everyone, up_raw, qkv_raw = exchange(lay, [plans["up"], plans["qkv"]], vec, [up_sum, qkv_sum], True, 3, 25)
        sums = jnp.sum(everyone.reshape(lay.outer, group, -1), 0)
        sum_qkv = jnp.transpose(sums[:, : 3 * cols].reshape(group, 3, cols), (1, 0, 2)).reshape(-1)
        sum_up = sums[:, 3 * cols : 3 * cols + ff_cols].reshape(-1)
        sum_dy = jnp.sum(sums[:, 3 * cols + ff_cols : 3 * cols + ff_cols + width], 0)

        def own_part(vector):
            return lax.dynamic_index_in_dim(vector.reshape(lay.count, -1), rank, 0, keepdims=False)

        up_raw, qkv_raw = up_raw.astype(F32), qkv_raw.astype(F32)
        column = lambda v: v.astype(F32)[:, None]
        return (
            output,
            token_grad,
            jnp.sum(w_qkv.astype(F32) * qkv_raw, 1),
            jnp.sum(w_qkv.astype(F32) * sum_qkv, 1),
            jnp.sum(w_up.astype(F32) * up_raw, 1),
            jnp.sum(w_up.astype(F32) * sum_up, 1),
            column(gain1) * qkv_raw + column(bias1) * sum_qkv,
            own_part(sum_qkv),
            out_raw.astype(F32),
            own_part(sum_dy),
            column(gain2) * up_raw + column(bias2) * sum_up,
            own_part(sum_up),
            down_raw.astype(F32),
            own_part(sum_dy),
        )

    return step


def solution(mesh):
    outer, sub, seq = split_axes(mesh)
    inner = Mesh(mesh.devices.reshape(outer, sub, seq), ALL)
    act = P(None, ALL, None)
    vec = P(ALL)
    mat = P(ALL, None)
    return jax.shard_map(
        make_body(Layout(outer, sub, seq)),
        mesh=inner,
        in_specs=(
            act, P(None, ("zo", "yi")), act, vec, vec, vec, vec,
            mat, vec, mat, vec, mat, vec, mat, vec,
        ),
        out_specs=(act, act, vec, vec, vec, vec, mat, vec, mat, vec, mat, vec, mat, vec),
        check_vma=False,
    )
```

```python
import functools
import math

import jax
import jax.numpy as jnp
from jax import lax
from jax.experimental import pallas as pl
from jax.experimental.pallas import tpu as pltpu
from jax.sharding import Mesh, PartitionSpec as P


HEADS = 8
HEAD_DIM = 256
ROTARY = 64
EPSILON = 1e-05
NEGATIVE = -1e30
F32 = jnp.float32
BF16 = jnp.bfloat16
ALL = ("zo", "yi", "seq")
GROUP = ("yi", "seq")
MESH = pl.DeviceIdType.MESH
ANY = pl.BlockSpec(memory_space=pl.ANY)


def dot(left, right, dims):
    return lax.dot_general(left, right, (dims, ((), ())), preferred_element_type=F32)


def split_axes(mesh):
    dp, seq = mesh.shape["dp"], mesh.shape["seq"]
    sub = 1
    while seq * sub * 2 <= HEADS and dp % (sub * 2) == 0:
        sub *= 2
    return dp // sub, sub, seq


def remote(source, target, send, recv, device):
    return pltpu.make_async_remote_copy(
        src_ref=source, dst_ref=target, send_sem=send, recv_sem=recv,
        device_id=device, device_id_type=MESH,
    )


class Layout:
    def __init__(self, outer, sub, seq):
        self.outer, self.sub, self.seq = outer, sub, seq
        self.chips_x = seq // 2
        self.group = sub * seq
        self.count = outer * self.group
        self.heads = HEADS // self.group
        self.offsets = [(ry, rx) for ry in range(sub) for rx in range(self.chips_x)]
        self.far = sorted(self.offsets[1:], key=lambda o: (o[0] > 0) + (o[1] > 0))

    def shift(self, ry, rx):
        pairs = []
        for y in range(self.sub):
            for x in range(self.chips_x):
                for c in range(2):
                    there = ((y + ry) % self.sub, (x + rx) % self.chips_x)
                    pairs.append((y * self.seq + x * 2 + c, there[0] * self.seq + there[1] * 2 + c))
        return pairs

    def flip(self):
        return [(i, i ^ 1) for i in range(self.seq)]


def swap_copies(lay, plan, me, sources, targets, send, recv, back):
    zo = lax.axis_index("zo")
    copies = []
    for k in range(1, lay.group):
        peer = lax.rem(me + k, lay.group)
        device = (zo, peer // lay.seq, lax.rem(peer, lay.seq))
        j = 0
        for (parts, rows, cols), source, target in zip(plan, sources, targets, strict=True):
            for part in range(parts):
                wide = lambda who: pl.ds(pl.multiple_of((part * lay.group + who) * cols, 128), cols)
                thin = pl.ds(part * cols, cols)
                block = lambda who: pl.ds(pl.multiple_of(who * rows, rows), rows)
                if back:
                    copies.append(remote(source.at[block(peer), thin], target.at[:, wide(me)], send.at[k - 1, j], recv.at[k - 1, j], device))
                else:
                    copies.append(remote(source.at[:, wide(peer)], target.at[block(me), thin], send.at[k - 1, j], recv.at[k - 1, j], device))
                j += 1
    return copies


def swap_own(lay, plan, me, sources, targets, sems, back):
    copies = []
    j = 0
    for (parts, rows, cols), source, target in zip(plan, sources, targets, strict=True):
        for part in range(parts):
            wide = pl.ds(pl.multiple_of((part * lay.group + me) * cols, 128), cols)
            thin = pl.ds(part * cols, cols)
            block = pl.ds(pl.multiple_of(me * rows, rows), rows)
            if back:
                copies.append(pltpu.make_async_copy(source.at[block, thin], target.at[:, wide], sems.at[j]))
            else:
                copies.append(pltpu.make_async_copy(source.at[:, wide], target.at[block, thin], sems.at[j]))
            j += 1
    return copies


def group_barrier(lay, me):
    zo = lax.axis_index("zo")
    barrier = pltpu.get_barrier_semaphore()
    for k in range(1, lay.group):
        peer = lax.rem(me + k, lay.group)
        pl.semaphore_signal(
            barrier, inc=1, device_id=(zo, peer // lay.seq, lax.rem(peer, lay.seq)), device_id_type=MESH
        )
    pl.semaphore_wait(barrier, lay.group - 1)


def swap_shapes(lay, plan, back):
    if back:
        return [jax.ShapeDtypeStruct((rows, parts * lay.group * cols), BF16) for parts, rows, cols in plan]
    return [jax.ShapeDtypeStruct((lay.group * rows, parts * cols), BF16) for parts, rows, cols in plan]


def exchange_kernel(lay, plan, back, *refs):
    n = len(plan)
    vec_ref, sources = refs[0], refs[1 : 1 + n]
    all_ref, targets = refs[1 + n], refs[2 + n : 2 + 2 * n]
    send, recv, own, vec_send, vec_recv, vec_own = refs[2 + 2 * n :]
    zo = lax.axis_index("zo")
    me = lax.axis_index("yi") * lay.seq + lax.axis_index("seq")
    rank = zo * lay.group + me

    def device_of(k):
        peer = lax.rem(rank + k, lay.count)
        inner = lax.rem(peer, lay.group)
        return (peer // lay.group, inner // lay.seq, lax.rem(inner, lay.seq))

    barrier = pltpu.get_barrier_semaphore()

    def greet(k, carry):
        pl.semaphore_signal(barrier, inc=1, device_id=device_of(k), device_id_type=MESH)
        return carry

    lax.fori_loop(1, lay.count, greet, 0)
    pl.semaphore_wait(barrier, lay.count - 1)
    copies = swap_copies(lay, plan, me, sources, targets, send, recv, back)
    mine = swap_own(lay, plan, me, sources, targets, own, back)
    mine.append(pltpu.make_async_copy(vec_ref, all_ref.at[rank], vec_own))

    def vec_copy(k):
        return remote(vec_ref, all_ref.at[rank], vec_send.at[k - 1], vec_recv.at[k - 1], device_of(k))

    def start(k, carry):
        vec_copy(k).start()
        return carry

    def finish(k, carry):
        vec_copy(k).wait()
        return carry

    lax.fori_loop(1, lay.count, start, 0)
    for copy in copies + mine:
        copy.start()
    lax.fori_loop(1, lay.count, finish, 0)
    for copy in copies + mine:
        copy.wait()


def busy(microseconds):
    return pl.CostEstimate(flops=int(7e8 * microseconds), bytes_accessed=1 << 20, transcendentals=0)


def exchange(lay, plan, vec, arrays, back, number, time):
    count = sum(parts for parts, _, _ in plan)
    return pl.pallas_call(
        functools.partial(exchange_kernel, lay, plan, back),
        out_shape=[jax.ShapeDtypeStruct((lay.count, *vec.shape), F32), *swap_shapes(lay, plan, back)],
        in_specs=[ANY] * (1 + len(plan)),
        out_specs=[ANY] * (1 + len(plan)),
        scratch_shapes=[
            pltpu.SemaphoreType.DMA((lay.group - 1, count)),
            pltpu.SemaphoreType.DMA((lay.group - 1, count)),
            pltpu.SemaphoreType.DMA((count,)),
            pltpu.SemaphoreType.DMA((lay.count - 1,)),
            pltpu.SemaphoreType.DMA((lay.count - 1,)),
            pltpu.SemaphoreType.DMA,
        ],
        compiler_params=pltpu.CompilerParams(collective_id=number, has_side_effects=True),
        cost_estimate=busy(time),
    )(vec, *arrays)


def norm_kernel(lay, plan, *refs):
    n = len(plan)
    x_ref, gain_ref, sources = refs[0], refs[1], refs[2 : 2 + n]
    one_ref, two_ref, hat_ref, targets = *refs[2 + n : 5 + n], refs[5 + n : 5 + 2 * n]
    held, stage, send, recv, core_send, core_recv, w_send, w_recv, w_own, own_sem, out_sem = refs[5 + 2 * n :]
    batch, length, _ = x_ref.shape
    zo, yi, s = lax.axis_index("zo"), lax.axis_index("yi"), lax.axis_index("seq")
    me = yi * lay.seq + s
    x, core = s // 2, lax.rem(s, 2)
    partner = (zo, yi, x * 2 + 1 - core)

    def chip(ry, rx):
        return (zo, lax.rem(yi + ry, lay.sub), lax.rem(x + rx, lay.chips_x) * 2 + core)

    group_barrier(lay, me)
    slot = {offset: i for i, offset in enumerate(lay.offsets)}
    own_copy = pltpu.make_async_copy(x_ref, held.at[0, 0], own_sem)
    own_copy.start()
    straight = [o for o in lay.far if not (o[0] and o[1])]
    diagonal = [o for o in lay.far if o[0] and o[1]]
    copies = {}
    for o in straight:
        copies[o] = [remote(x_ref, held.at[0, slot[o]], send.at[slot[o], 0], recv.at[slot[o], 0], chip(*o))]
    half = batch // 2
    for ry, rx in diagonal:
        j = slot[(ry, rx)]
        copies[(ry, rx)] = [
            remote(held.at[0, slot[(0, rx)], :half], held.at[0, j, :half], send.at[j, 0], recv.at[j, 0], chip(ry, 0)),
            remote(held.at[0, slot[(ry, 0)], half:], held.at[0, j, half:], send.at[j, 1], recv.at[j, 1], chip(0, rx)),
        ]
    to_partner = {
        o: remote(x_ref if o == (0, 0) else held.at[0, slot[o]], held.at[1, slot[o]],
                  core_send.at[slot[o]], core_recv.at[slot[o]], partner)
        for o in lay.offsets
    }
    for o in straight:
        copies[o][0].start()
    to_partner[(0, 0)].start()
    swaps = swap_copies(lay, plan, me, sources, targets, w_send, w_recv, False)
    swaps += swap_own(lay, plan, me, sources, targets, w_own, False)
    gains = [gain_ref[i : i + 1, :] for i in range(4)]
    rows = 16
    pending = [[], []]
    turn = [0]

    def norm(c, j):
        for m in range(batch):
            k = turn[0] % 2
            turn[0] += 1
            for copy in pending[k]:
                copy.wait()

            def chunk(i, carry):
                at = pl.ds(pl.multiple_of(i * rows, rows), rows)
                value = held[c, j, m, at, :].astype(F32)
                center = value - jnp.mean(value, -1, keepdims=True)
                hat = center * lax.rsqrt(jnp.mean(center * center, -1, keepdims=True) + EPSILON)
                stage[k, 0, at, :] = (hat * gains[0] + gains[1]).astype(BF16)
                stage[k, 1, at, :] = (hat * gains[2] + gains[3]).astype(BF16)
                stage[k, 2, at, :] = hat.astype(BF16)
                return carry

            lax.fori_loop(0, length // rows, chunk, 0)
            pending[k] = [
                pltpu.make_async_copy(stage.at[k, i], ref.at[c, j, m], out_sem.at[k, i])
                for i, ref in enumerate((one_ref, two_ref, hat_ref))
            ]
            for copy in pending[k]:
                copy.start()

    own_copy.wait()
    norm(0, 0)
    to_partner[(0, 0)].wait_recv()
    norm(1, 0)
    for o in straight:
        copies[o][0].wait_recv()
        to_partner[o].start()
        for ry, rx in diagonal:
            if o == (0, rx):
                copies[(ry, rx)][0].start()
            if o == (ry, 0):
                copies[(ry, rx)][1].start()
        if o == straight[-1]:
            for copy in swaps:
                copy.start()
        norm(0, slot[o])
    for o in straight:
        to_partner[o].wait_recv()
        norm(1, slot[o])
    for o in diagonal:
        for copy in copies[o]:
            copy.wait_recv()
        to_partner[o].start()
        norm(0, slot[o])
    for o in diagonal:
        to_partner[o].wait_recv()
        norm(1, slot[o])
    for side in pending:
        for copy in side:
            copy.wait()
    for o in lay.far:
        for copy in copies[o]:
            copy.wait_send()
    for o in lay.offsets:
        to_partner[o].wait_send()
    for copy in swaps:
        copy.wait()


def norm_exchange(lay, plan, tokens, gains, weights):
    count = sum(parts for parts, _, _ in plan)
    chips = lay.group // 2
    whole = jax.ShapeDtypeStruct((2, chips, *tokens.shape), BF16)
    return pl.pallas_call(
        functools.partial(norm_kernel, lay, plan),
        out_shape=[whole] * 3 + swap_shapes(lay, plan, False),
        in_specs=[ANY, pl.BlockSpec(memory_space=pltpu.VMEM)] + [ANY] * len(plan),
        out_specs=[ANY] * (3 + len(plan)),
        scratch_shapes=[
            pltpu.VMEM((2, chips, *tokens.shape), BF16),
            pltpu.VMEM((2, 3, *tokens.shape[1:]), BF16),
            pltpu.SemaphoreType.DMA((chips, 2)),
            pltpu.SemaphoreType.DMA((chips, 2)),
            pltpu.SemaphoreType.DMA((chips,)),
            pltpu.SemaphoreType.DMA((chips,)),
            pltpu.SemaphoreType.DMA((lay.group - 1, count)),
            pltpu.SemaphoreType.DMA((lay.group - 1, count)),
            pltpu.SemaphoreType.DMA((count,)),
            pltpu.SemaphoreType.DMA,
            pltpu.SemaphoreType.DMA((2, 3)),
        ],
        compiler_params=pltpu.CompilerParams(
            collective_id=1, has_side_effects=True, vmem_limit_bytes=48 << 20
        ),
        cost_estimate=busy(100),
        name="norm_exchange",
    )(tokens, gains, *weights)


def deal_kernel(lay, plan, *refs):
    n = len(plan)
    sources, targets = refs[:n], refs[n : 2 * n]
    send, recv, own = refs[2 * n :]
    me = lax.axis_index("yi") * lay.seq + lax.axis_index("seq")
    group_barrier(lay, me)
    copies = swap_copies(lay, plan, me, sources, targets, send, recv, True)
    copies += swap_own(lay, plan, me, sources, targets, own, True)
    for copy in copies:
        copy.start()
    for copy in copies:
        copy.wait()


def deal_exchange(lay, plan, sums, number):
    count = sum(parts for parts, _, _ in plan)
    return pl.pallas_call(
        functools.partial(deal_kernel, lay, plan),
        out_shape=swap_shapes(lay, plan, True),
        in_specs=[ANY] * len(plan),
        out_specs=[ANY] * len(plan),
        scratch_shapes=[
            pltpu.SemaphoreType.DMA((lay.group - 1, count)),
            pltpu.SemaphoreType.DMA((lay.group - 1, count)),
            pltpu.SemaphoreType.DMA((count,)),
        ],
        compiler_params=pltpu.CompilerParams(collective_id=number, has_side_effects=True),
        cost_estimate=busy(17),
    )(*sums)


def pair_kernel(lay, first_ref, first_w, second_ref, second_w, *refs):
    step = pl.program_id(0)
    chips = lay.group // 2
    outs, (given, came, send, recv, out_sem) = refs[:chips], refs[chips:]
    zo, yi, s = lax.axis_index("zo"), lax.axis_index("yi"), lax.axis_index("seq")
    partner = (zo, yi, (s // 2) * 2 + 1 - lax.rem(s, 2))

    def copy(j):
        return remote(given.at[j], came.at[j], send.at[j], recv.at[j], partner)

    def store(j):
        return pltpu.make_async_copy(came.at[j], outs[(j + 1) % chips], out_sem.at[j])

    @pl.when(step == 0)
    def _():
        barrier = pltpu.get_barrier_semaphore()
        pl.semaphore_signal(barrier, inc=1, device_id=partner, device_id_type=MESH)
        pl.semaphore_wait(barrier, 1)

    for j in range(chips):

        @pl.when(step == j + 1)
        def _():
            copy(j).start()

    total = dot(first_ref[0, 0], first_w[...], ((1,), (1,))) + dot(second_ref[0, 0], second_w[...], ((1,), (1,)))
    for j in range(chips):

        @pl.when(step == j)
        def _():
            given[j] = total.astype(BF16)

        @pl.when(step == chips + j)
        def _():
            copy(j).wait_recv()
            came[j] = (total + came[j].astype(F32)).astype(BF16)

    for j in range(chips - 1):

        @pl.when(step == chips + j + 1)
        def _():
            store(j).start()

    @pl.when(step == 2 * chips - 1)
    def _():
        store(chips - 1).start()
        for j in range(chips):
            copy(j).wait_send()
            store(j).wait()


def pair_matmul(lay, first, first_w, second, second_w, cut, number):
    chips = lay.group // 2
    rows = first.shape[0] // lay.group
    width = first_w.shape[0] // cut[1]
    depth1, depth2 = first.shape[1], second.shape[1]

    def act(depth):
        return pl.BlockSpec((1, 1, rows, depth), lambda i: (1 - i // chips, (i + 1) % chips, 0, 0))

    def weight(depth):
        return pl.BlockSpec((width, depth), lambda i: (cut[0], 0), pipeline_mode=pl.Buffered(1))

    shape = lambda v: v.reshape(2, chips, rows, v.shape[1])
    return pl.pallas_call(
        functools.partial(pair_kernel, lay),
        grid=(2 * chips,),
        in_specs=[act(depth1), weight(depth1), act(depth2), weight(depth2)],
        out_specs=[ANY] * chips,
        out_shape=[jax.ShapeDtypeStruct((rows, width), BF16)] * chips,
        scratch_shapes=[
            pltpu.VMEM((chips, rows, width), BF16),
            pltpu.VMEM((chips, rows, width), BF16),
            pltpu.SemaphoreType.DMA((chips,)),
            pltpu.SemaphoreType.DMA((chips,)),
            pltpu.SemaphoreType.DMA((chips,)),
        ],
        compiler_params=pltpu.CompilerParams(
            collective_id=number, has_side_effects=True, vmem_limit_bytes=60 << 20
        ),
        cost_estimate=pl.CostEstimate(
            flops=2 * first.shape[0] * (depth1 + depth2) * width, bytes_accessed=32 << 20, transcendentals=0
        ),
    )(shape(first), first_w, shape(second), second_w)


def turn_pairs(field, cosine, sine):
    halves = ROTARY // 2
    front = field[:, :128]
    lane = lax.broadcasted_iota(jnp.int32, front.shape, 1)
    other = jnp.where(lane < halves, pltpu.roll(front, 128 - halves, 1), pltpu.roll(front, halves, 1))
    return jnp.concatenate([front * cosine + other * sine, field[:, 128:]], -1)


QUERY_BLOCK = 256


def wide_angles(ref):
    part = ref[0]
    return jnp.transpose(jnp.concatenate([part, part, part, part], 0), (1, 0))


def wide_pair(cos_ref, sin_ref):
    cosine, sine = wide_angles(cos_ref), wide_angles(sin_ref)
    lane = lax.broadcasted_iota(jnp.int32, cosine.shape, 1)
    cosine = jnp.where(lane < ROTARY, cosine, 1.0)
    sine = jnp.where(lane < ROTARY // 2, -sine, jnp.where(lane < ROTARY, sine, 0.0))
    return cosine, sine


def attend_kernel(scaling, packed_ref, cos_ref, sin_ref, col_ref, row_ref, q_ref, k_ref, v_ref, ctx_ref, lse_ref,
                  q_buf, k_buf, v_buf, ctx_buf, cos_buf, sin_buf):
    cores, _, chips, _, length, _ = packed_ref.shape
    cos_all, sin_all = wide_pair(cos_ref, sin_ref)
    cos_buf[...] = cos_all
    sin_buf[...] = sin_all
    for c in range(cores):
        for i in range(chips):
            at = pl.ds((c * chips + i) * length, length)
            block = packed_ref[c, 0, i, 0]
            cosine, sine = cos_buf[at, :], sin_buf[at, :]
            q_buf[at, :] = turn_pairs(block[:, :HEAD_DIM], cosine, sine).astype(BF16)
            k_buf[at, :] = turn_pairs(block[:, HEAD_DIM : 2 * HEAD_DIM], cosine, sine).astype(BF16)
            v_buf[at, :] = block[:, 2 * HEAD_DIM :].astype(BF16)
    q_ref[0] = q_buf[...]
    k_ref[0] = k_buf[...]
    v_ref[0] = v_buf[...]
    total = cores * chips * length

    def one(j, carry):
        at = pl.ds(pl.multiple_of(j * QUERY_BLOCK, QUERY_BLOCK), QUERY_BLOCK)
        scores = dot(k_buf[...], q_buf[at, :], ((1,), (1,))) * scaling
        allowed = col_ref[0] <= row_ref[0, :, at]
        scores = jnp.where(allowed, scores, NEGATIVE)
        top = jnp.max(scores, 0, keepdims=True)
        weights = jnp.where(allowed, jnp.exp(scores - top), 0.0)
        total_row = jnp.sum(weights, 0, keepdims=True)
        probs = (weights * (1.0 / total_row)).astype(BF16)
        ctx_buf[at, :] = dot(probs, v_buf[...], ((0,), (0,))).astype(BF16)
        lse_ref[0, :, at] = top + jnp.log(total_row)
        return carry

    lax.fori_loop(0, total // QUERY_BLOCK, one, 0)
    for c in range(cores):
        for i in range(chips):
            ctx_ref[c, 0, i, 0] = ctx_buf[pl.ds((c * chips + i) * length, length), :]


def attend_back_kernel(scaling, q_ref, k_ref, v_ref, g_ref, cos_ref, sin_ref, col_ref, row_ref, lse_ref, out_ref,
                       g_buf, dq_buf, dk_buf, dv_buf, cos_buf, sin_buf):
    cores, _, chips, _, length, _ = out_ref.shape
    total = q_ref.shape[1]
    cos_all, sin_all = wide_pair(cos_ref, sin_ref)
    cos_buf[...] = cos_all
    sin_buf[...] = sin_all
    for c in range(cores):
        for i in range(chips):
            g_buf[pl.ds((c * chips + i) * length, length), :] = g_ref[c, 0, i, 0]
    dk_buf[...] = jnp.zeros_like(dk_buf)
    dv_buf[...] = jnp.zeros_like(dv_buf)

    def one(j, carry):
        at = pl.ds(pl.multiple_of(j * QUERY_BLOCK, QUERY_BLOCK), QUERY_BLOCK)
        queries = q_ref[0, at, :]
        grads = g_buf[at, :]
        scores = dot(k_ref[0], queries, ((1,), (1,))) * scaling
        allowed = col_ref[0] <= row_ref[0, :, at]
        scores = jnp.where(allowed, scores, NEGATIVE)
        probs = jnp.where(allowed, jnp.exp(scores - lse_ref[0, :, at]), 0.0)
        grad_probs = dot(v_ref[0], grads, ((1,), (1,)))
        delta = jnp.sum(probs * grad_probs, 0, keepdims=True)
        grad_scores = (probs * (grad_probs - delta)).astype(BF16)
        dv_buf[...] += dot(probs.astype(BF16), grads, ((1,), (0,)))
        dk_buf[...] += dot(grad_scores, queries, ((1,), (0,)))
        dq_buf[at, :] = dot(grad_scores, k_ref[0], ((0,), (0,)))
        return carry

    lax.fori_loop(0, total // QUERY_BLOCK, one, 0)
    for c in range(cores):
        for i in range(chips):
            at = pl.ds((c * chips + i) * length, length)
            cosine, sine = cos_buf[at, :], sin_buf[at, :]
            out_ref[c, 0, i, 0, :, :HEAD_DIM] = turn_pairs(dq_buf[at, :] * scaling, cosine, -sine).astype(BF16)
            out_ref[c, 0, i, 0, :, HEAD_DIM : 2 * HEAD_DIM] = turn_pairs(dk_buf[at, :] * scaling, cosine, -sine).astype(BF16)
            out_ref[c, 0, i, 0, :, 2 * HEAD_DIM :] = dv_buf[at, :].astype(BF16)


def make_body(lay):
    sub, seq, group, chips_x = lay.sub, lay.seq, lay.group, lay.chips_x

    def gather_near(value):
        return [value if o == (0, 0) else lax.ppermute(value, GROUP, lay.shift(*o)) for o in lay.offsets]

    def gather_partner(near):
        partner = [lax.ppermute(piece, "seq", lay.flip()) for piece in near]
        return jnp.concatenate([piece[None] for piece in near + partner], 0)

    def send_far(pieces):
        came = [pieces[0]]
        for o, piece in zip(lay.offsets[1:], pieces[1:], strict=True):
            back = ((-o[0]) % sub, (-o[1]) % chips_x)
            came.append(lax.ppermute(piece, GROUP, lay.shift(*back)))
        return came

    def add_all(pieces):
        total = pieces[0].astype(F32)
        for piece in pieces[1:]:
            total = total + piece.astype(F32)
        return total

    def after(value, *tokens):
        return lax.optimization_barrier((value, *tokens))[0]

    def step(
        tokens, positions, cotangent, gain1, bias1, gain2, bias2,
        w_qkv, b_qkv, w_out, b_out, w_up, b_up, w_down, b_down,
    ):
        batch, length, width = tokens.shape
        rows = w_qkv.shape[0]
        ff = w_up.shape[1]
        count = seq * length
        total = group * batch * length
        my_seq = lax.axis_index("seq")
        me = lax.axis_index("yi") * seq + my_seq
        scaling = HEAD_DIM ** (-0.5)
        cols = lay.heads * HEAD_DIM
        ff_cols = ff // group
        out_cols = width // group
        plans = {"up": (1, rows, ff_cols), "down": (1, rows, ff_cols), "qkv": (3, rows, cols), "out": (1, rows, out_cols)}

        def gather_rows(mine):
            return lax.all_gather(mine, "zo", axis=0, tiled=True)

        x, core = my_seq // 2, my_seq % 2
        places = []
        for ry in range(sub):
            from_there = positions
            if ry:
                from_there = lax.ppermute(positions, "yi", [(i, (i + ry) % sub) for i in range(sub)])
            blocks = from_there.reshape(batch, seq, length)
            order = [((x - rx) % chips_x) * 2 + (core + rc) % 2 for rc in range(2) for rx in range(chips_x)]
            places.append(jnp.concatenate([lax.dynamic_slice_in_dim(blocks, o, 1, 1) for o in order], 1))
        places = jnp.stack(places).reshape(sub * batch, count)
        names = (bias1, bias2, gain1, gain2, b_qkv, b_up, b_out, b_down)
        vec = jnp.concatenate([v.astype(F32) for v in names])
        size = -(-vec.shape[0] // 1024) * 1024
        vec = jnp.pad(vec, (0, size - vec.shape[0])).reshape(-1, 128)
        vectors, up_own, qkv_own = exchange(lay, [plans["up"], plans["qkv"]], vec, [w_up, w_qkv], False, 0, 30)
        up_w = gather_rows(up_own)
        qkv_w = gather_rows(qkv_own)
        vectors = vectors.reshape(lay.count, -1)
        cuts = []
        at = 0
        for piece in names:
            cuts.append(vectors[:, at : at + piece.shape[0]].reshape(-1))
            at += piece.shape[0]
        bias1_all, bias2_all, gain1_all, gain2_all, b_qkv_all, b_up_all, b_out_all, b_down_all = cuts
        b_qkv_mine = lax.dynamic_index_in_dim(b_qkv_all.reshape(3, group, cols), me, 1, keepdims=False).reshape(-1)
        b_up_mine = lax.dynamic_index_in_dim(b_up_all.reshape(group, ff_cols), me, 0, keepdims=False)
        zeros = jnp.zeros_like(bias1_all)
        gains = jnp.stack([gain1_all, bias1_all, gain2_all, bias2_all, zeros, zeros, zeros, zeros])
        one, two, hat, out_own, down_own = norm_exchange(lay, [plans["out"], plans["down"]], tokens, gains, [w_out, w_down])
        out_w = gather_rows(out_own)
        down_w = gather_rows(down_own)
        one, two, hat = [v.reshape(total, width) for v in (one, two, hat)]
        cotangent, hat, places = lax.optimization_barrier((cotangent, hat, places))
        near_dy = gather_near(cotangent)

        hidden = dot(two, up_w, ((1,), (0,))) + b_up_mine
        phi_cdf = 0.5 * (1.0 + lax.erf(hidden * math.sqrt(0.5)))
        density = jnp.exp(-0.5 * hidden * hidden) * (1.0 / math.sqrt(2.0 * math.pi))
        activated = (hidden * phi_cdf).astype(BF16)
        slope = (phi_cdf + hidden * density).astype(BF16)
        activated, slope = lax.optimization_barrier((activated, slope))

        halves = ROTARY // 2
        frequency = jnp.exp(jnp.arange(halves, dtype=F32) * (-2.0 * math.log(10000.0) / ROTARY))
        places = after(places, activated)
        phases = places.astype(F32)[:, None, :] * frequency[None, :, None]
        cosine, sine = jnp.cos(phases), jnp.sin(phases)
        place_col = places[:, :, None]
        place_row = places[:, None, :]

        seqs = sub * batch
        one = after(one, cosine, sine)
        packed = dot(one, qkv_w, ((1,), (0,))) + b_qkv_mine
        wide = (2, 1, chips_x, 1, length, 3 * cols)
        wide_spec = pl.BlockSpec(wide, lambda i: (0, i // batch, 0, i % batch, 0, 0))
        full = (2, sub, chips_x, batch, length, 3 * cols)
        head_spec = pl.BlockSpec((1, count, HEAD_DIM), lambda i: (i, 0, 0))
        turn_spec = pl.BlockSpec((1, ROTARY // 2, count), lambda i: (i, 0, 0))
        tokens_spec = pl.BlockSpec((2, 1, chips_x, 1, length, cols), lambda i: (0, i // batch, 0, i % batch, 0, 0))
        by_token = (2, sub, chips_x, batch, length, cols)
        turn_bufs = [pltpu.VMEM((count, 128), F32)] * 2
        col_spec = pl.BlockSpec((1, count, 1), lambda i: (i, 0, 0))
        row_spec = pl.BlockSpec((1, 1, count), lambda i: (i, 0, 0))
        head_shape = jax.ShapeDtypeStruct((seqs, count, HEAD_DIM), BF16)
        work = 2 * seqs * count * count * HEAD_DIM
        params = pltpu.CompilerParams(vmem_limit_bytes=56 << 20)
        queries, keys, values, context, lse = pl.pallas_call(
            functools.partial(attend_kernel, scaling),
            grid=(seqs,),
            in_specs=[wide_spec, turn_spec, turn_spec, col_spec, row_spec],
            out_specs=[head_spec] * 3 + [tokens_spec, row_spec],
            out_shape=[head_shape] * 3 + [jax.ShapeDtypeStruct(by_token, BF16), jax.ShapeDtypeStruct((seqs, 1, count), F32)],
            scratch_shapes=[pltpu.VMEM((count, HEAD_DIM), BF16)] * 4 + turn_bufs,
            compiler_params=params,
            cost_estimate=pl.CostEstimate(flops=2 * work, bytes_accessed=30 << 20, transcendentals=seqs * count * count),
            name="attend",
        )(packed.reshape(full), cosine, sine, place_col, place_row)

        context = context.reshape(total, cols)

        def scatter(grad):
            return lax.psum_scatter(grad, "zo", scatter_dimension=0, tiled=True)

        def outer_dot(left, right):
            return dot(left, right, ((0,), (0,))).astype(BF16)

        qkv_late, up_late = lax.optimization_barrier((qkv_w, up_w, context))[:-1]
        fold_qkv = (gain1_all[:, None] * qkv_late.astype(F32)).astype(BF16)
        fold_up = (gain2_all[:, None] * up_late.astype(F32)).astype(BF16)
        near_dy = lax.optimization_barrier((*near_dy, fold_qkv, fold_up))[:-2]
        upstream = gather_partner(list(near_dy)).reshape(total, width)
        down_part = outer_dot(upstream, activated)
        upstream = after(upstream, down_part)
        down_sum = scatter(down_part)
        grad_context = dot(upstream, out_w, ((1,), (0,))).astype(BF16)
        upstream = after(upstream, grad_context)
        out_part = outer_dot(upstream, context)
        out_w_sum = scatter(out_part)

        def chain(values, *tokens):
            return lax.optimization_barrier((*values, *tokens))[: len(values)]

        def tokens_of(pieces):
            return [piece.reshape(batch, length, -1) for piece in pieces]

        pair = chain((context, activated), out_part)
        out_near = pair_matmul(lay, pair[0], out_w, pair[1], down_w, (0, 1), 4)
        grad_context, *out_near = chain((grad_context, *out_near))
        out_near = tokens_of(out_near)
        out_near = send_far(out_near)

        grad_packed = pl.pallas_call(
            functools.partial(attend_back_kernel, scaling),
            grid=(seqs,),
            in_specs=[head_spec] * 3 + [tokens_spec, turn_spec, turn_spec, col_spec, row_spec, row_spec],
            out_specs=wide_spec,
            out_shape=jax.ShapeDtypeStruct(full, BF16),
            scratch_shapes=[pltpu.VMEM((count, HEAD_DIM), BF16)] + [pltpu.VMEM((count, HEAD_DIM), F32)] * 3 + turn_bufs,
            compiler_params=params,
            cost_estimate=pl.CostEstimate(flops=5 * work, bytes_accessed=24 << 20, transcendentals=seqs * count * count),
            name="attend_back",
        )(queries, keys, values, grad_context.reshape(by_token), cosine, sine, place_col, place_row, lse)
        grad_packed = grad_packed.reshape(total, 3 * cols)

        qkv_part = outer_dot(hat, grad_packed)
        qkv_sum = scatter(qkv_part)
        (upstream,) = chain((upstream,), qkv_part)
        grad_hidden = (dot(upstream, down_w, ((1,), (0,))) * slope.astype(F32)).astype(BF16)

        near = pair_matmul(lay, grad_packed, fold_qkv, grad_hidden, fold_up, (0, 2), 5)
        hat, *near = chain((hat, *near))
        came = [send_far(tokens_of(near))]
        up_part = outer_dot(hat, grad_hidden)
        up_sum = scatter(up_part)
        (left,) = chain((grad_packed,), up_part)
        near = pair_matmul(lay, left, fold_qkv, grad_hidden, fold_up, (1, 2), 6)
        came.append(send_far(tokens_of(near)))

        own_sums = [
            jnp.sum(grad_packed.astype(F32), 0),
            jnp.sum(grad_hidden.astype(F32), 0),
            jnp.sum(cotangent.astype(F32), (0, 1)),
        ]
        vec = jnp.concatenate(own_sums)
        size = -(-vec.shape[0] // 1024) * 1024
        vec = jnp.pad(vec, (0, size - vec.shape[0])).reshape(-1, 128)
        out_near, vec, down_sum, out_w_sum = chain((out_near, vec, down_sum, out_w_sum), *near)
        output = (tokens.astype(F32) + add_all(out_near) + b_out_all + b_down_all).astype(BF16)
        vec, output = chain((vec, output))
        everyone, down_raw, out_raw, qkv_raw = exchange(
            lay, [plans["down"], plans["out"], plans["qkv"]], vec, [down_sum, out_w_sum, qkv_sum], True, 2, 40
        )
        came[1] = chain(came[1], everyone)

        inputs = tokens.astype(F32)
        center = inputs - jnp.mean(inputs, -1, keepdims=True)
        inv_std = lax.rsqrt(jnp.mean(center * center, -1, keepdims=True) + EPSILON)
        normal = center * inv_std
        grad_normal = jnp.concatenate([add_all(pieces) for pieces in came], -1)
        token_grad = cotangent.astype(F32) + inv_std * (
            grad_normal
            - jnp.mean(grad_normal, -1, keepdims=True)
            - normal * jnp.mean(grad_normal * normal, -1, keepdims=True)
        )

        rank = lax.axis_index("zo") * group + me
        (up_raw,) = deal_exchange(lay, [plans["up"]], [up_sum], 3)
        sums = jnp.sum(everyone.reshape(lay.outer, group, -1), 0)
        sum_qkv = jnp.transpose(sums[:, : 3 * cols].reshape(group, 3, cols), (1, 0, 2)).reshape(-1)
        sum_up = sums[:, 3 * cols : 3 * cols + ff_cols].reshape(-1)
        sum_dy = jnp.sum(sums[:, 3 * cols + ff_cols : 3 * cols + ff_cols + width], 0)

        def own_part(vector):
            return lax.dynamic_index_in_dim(vector.reshape(lay.count, -1), rank, 0, keepdims=False)

        up_raw, qkv_raw = up_raw.astype(F32), qkv_raw.astype(F32)
        column = lambda v: v.astype(F32)[:, None]
        return (
            output,
            token_grad,
            jnp.sum(w_qkv.astype(F32) * qkv_raw, 1),
            jnp.sum(w_qkv.astype(F32) * sum_qkv, 1),
            jnp.sum(w_up.astype(F32) * up_raw, 1),
            jnp.sum(w_up.astype(F32) * sum_up, 1),
            column(gain1) * qkv_raw + column(bias1) * sum_qkv,
            own_part(sum_qkv),
            out_raw.astype(F32),
            own_part(sum_dy),
            column(gain2) * up_raw + column(bias2) * sum_up,
            own_part(sum_up),
            down_raw.astype(F32),
            own_part(sum_dy),
        )

    return step


def solution(mesh):
    outer, sub, seq = split_axes(mesh)
    inner = Mesh(mesh.devices.reshape(outer, sub, seq), ALL)
    act = P(None, ALL, None)
    vec = P(ALL)
    mat = P(ALL, None)
    return jax.shard_map(
        make_body(Layout(outer, sub, seq)),
        mesh=inner,
        in_specs=(
            act, P(None, ("zo", "yi")), act, vec, vec, vec, vec,
            mat, vec, mat, vec, mat, vec, mat, vec,
        ),
        out_specs=(act, act, vec, vec, vec, vec, mat, vec, mat, vec, mat, vec, mat, vec),
        check_vma=False,
    )
```

```python
import functools
import math

import jax
import jax.numpy as jnp
from jax import lax
from jax.experimental import pallas as pl
from jax.experimental.pallas import tpu as pltpu
from jax.sharding import Mesh, PartitionSpec as P


HEADS = 8
HEAD_DIM = 256
ROTARY = 64
EPSILON = 1e-05
NEGATIVE = -1e30
F32 = jnp.float32
BF16 = jnp.bfloat16
ALL = ("zo", "yi", "seq")
GROUP = ("yi", "seq")
MESH = pl.DeviceIdType.MESH
ANY = pl.BlockSpec(memory_space=pl.ANY)


def dot(left, right, dims):
    return lax.dot_general(left, right, (dims, ((), ())), preferred_element_type=F32)


def split_axes(mesh):
    dp, seq = mesh.shape["dp"], mesh.shape["seq"]
    sub = 1
    while seq * sub * 2 <= HEADS and dp % (sub * 2) == 0:
        sub *= 2
    return dp // sub, sub, seq


def remote(source, target, send, recv, device):
    return pltpu.make_async_remote_copy(
        src_ref=source, dst_ref=target, send_sem=send, recv_sem=recv,
        device_id=device, device_id_type=MESH,
    )


class Layout:
    def __init__(self, outer, sub, seq):
        self.outer, self.sub, self.seq = outer, sub, seq
        self.chips_x = seq // 2
        self.group = sub * seq
        self.count = outer * self.group
        self.heads = HEADS // self.group
        self.offsets = [(ry, rx) for ry in range(sub) for rx in range(self.chips_x)]
        self.far = sorted(self.offsets[1:], key=lambda o: (o[0] > 0) + (o[1] > 0))

    def shift(self, ry, rx):
        pairs = []
        for y in range(self.sub):
            for x in range(self.chips_x):
                for c in range(2):
                    there = ((y + ry) % self.sub, (x + rx) % self.chips_x)
                    pairs.append((y * self.seq + x * 2 + c, there[0] * self.seq + there[1] * 2 + c))
        return pairs

    def flip(self):
        return [(i, i ^ 1) for i in range(self.seq)]


def swap_copies(lay, plan, me, sources, targets, send, recv, back):
    zo = lax.axis_index("zo")
    copies = []
    for k in range(1, lay.group):
        peer = lax.rem(me + k, lay.group)
        device = (zo, peer // lay.seq, lax.rem(peer, lay.seq))
        j = 0
        for (parts, rows, cols), source, target in zip(plan, sources, targets, strict=True):
            for part in range(parts):
                wide = lambda who: pl.ds(pl.multiple_of((part * lay.group + who) * cols, 128), cols)
                thin = pl.ds(part * cols, cols)
                block = lambda who: pl.ds(pl.multiple_of(who * rows, rows), rows)
                if back:
                    copies.append(remote(source.at[block(peer), thin], target.at[:, wide(me)], send.at[k - 1, j], recv.at[k - 1, j], device))
                else:
                    copies.append(remote(source.at[:, wide(peer)], target.at[block(me), thin], send.at[k - 1, j], recv.at[k - 1, j], device))
                j += 1
    return copies


def swap_own(lay, plan, me, sources, targets, sems, back):
    copies = []
    j = 0
    for (parts, rows, cols), source, target in zip(plan, sources, targets, strict=True):
        for part in range(parts):
            wide = pl.ds(pl.multiple_of((part * lay.group + me) * cols, 128), cols)
            thin = pl.ds(part * cols, cols)
            block = pl.ds(pl.multiple_of(me * rows, rows), rows)
            if back:
                copies.append(pltpu.make_async_copy(source.at[block, thin], target.at[:, wide], sems.at[j]))
            else:
                copies.append(pltpu.make_async_copy(source.at[:, wide], target.at[block, thin], sems.at[j]))
            j += 1
    return copies


def group_barrier(lay, me):
    zo = lax.axis_index("zo")
    barrier = pltpu.get_barrier_semaphore()
    for k in range(1, lay.group):
        peer = lax.rem(me + k, lay.group)
        pl.semaphore_signal(
            barrier, inc=1, device_id=(zo, peer // lay.seq, lax.rem(peer, lay.seq)), device_id_type=MESH
        )
    pl.semaphore_wait(barrier, lay.group - 1)


def swap_shapes(lay, plan, back):
    if back:
        return [jax.ShapeDtypeStruct((rows, parts * lay.group * cols), BF16) for parts, rows, cols in plan]
    return [jax.ShapeDtypeStruct((lay.group * rows, parts * cols), BF16) for parts, rows, cols in plan]


def device_after(lay, rank, k):
    peer = lax.rem(rank + k, lay.count)
    inner = lax.rem(peer, lay.group)
    return (peer // lay.group, inner // lay.seq, lax.rem(inner, lay.seq))


def barrier_all(lay, device_of):
    barrier = pltpu.get_barrier_semaphore()

    def greet(k, carry):
        pl.semaphore_signal(barrier, inc=1, device_id=device_of(k), device_id_type=MESH)
        return carry

    lax.fori_loop(1, lay.count, greet, 0)
    pl.semaphore_wait(barrier, lay.count - 1)


def exchange_kernel(lay, plan, *refs):
    n = len(plan)
    vec_ref, sources = refs[0], refs[1 : 1 + n]
    all_ref, targets = refs[1 + n], refs[2 + n : 2 + 2 * n]
    send, recv, own, vec_send, vec_recv, vec_own = refs[2 + 2 * n :]
    zo = lax.axis_index("zo")
    me = lax.axis_index("yi") * lay.seq + lax.axis_index("seq")
    rank = zo * lay.group + me

    device_of = functools.partial(device_after, lay, rank)
    barrier_all(lay, device_of)
    copies = swap_copies(lay, plan, me, sources, targets, send, recv, True)
    mine = swap_own(lay, plan, me, sources, targets, own, True)
    mine.append(pltpu.make_async_copy(vec_ref, all_ref.at[rank], vec_own))

    def vec_copy(k):
        return remote(vec_ref, all_ref.at[rank], vec_send.at[k - 1], vec_recv.at[k - 1], device_of(k))

    def start(k, carry):
        vec_copy(k).start()
        return carry

    def finish(k, carry):
        vec_copy(k).wait()
        return carry

    lax.fori_loop(1, lay.count, start, 0)
    for copy in copies + mine:
        copy.start()
    lax.fori_loop(1, lay.count, finish, 0)
    for copy in copies + mine:
        copy.wait()


def busy(microseconds):
    return pl.CostEstimate(flops=int(7e8 * microseconds), bytes_accessed=1 << 20, transcendentals=0)


def exchange(lay, plan, vec, arrays, number, time):
    count = sum(parts for parts, _, _ in plan)
    return pl.pallas_call(
        functools.partial(exchange_kernel, lay, plan),
        out_shape=[jax.ShapeDtypeStruct((lay.count, *vec.shape), F32), *swap_shapes(lay, plan, True)],
        in_specs=[ANY] * (1 + len(plan)),
        out_specs=[ANY] * (1 + len(plan)),
        scratch_shapes=[
            pltpu.SemaphoreType.DMA((lay.group - 1, count)),
            pltpu.SemaphoreType.DMA((lay.group - 1, count)),
            pltpu.SemaphoreType.DMA((count,)),
            pltpu.SemaphoreType.DMA((lay.count - 1,)),
            pltpu.SemaphoreType.DMA((lay.count - 1,)),
            pltpu.SemaphoreType.DMA,
        ],
        compiler_params=pltpu.CompilerParams(collective_id=number, has_side_effects=True),
        cost_estimate=busy(time),
    )(vec, *arrays)


def norm_kernel(lay, plan, *refs):
    n = len(plan)
    x_ref, vec_ref, sources = refs[0], refs[1], refs[2 : 2 + n]
    one_ref, two_ref, hat_ref, all_ref, targets = *refs[2 + n : 6 + n], refs[6 + n : 6 + 2 * n]
    (held, stage, vectors, gain_buf, send, recv, core_send, core_recv, w_send, w_recv, w_own, own_sem, out_sem,
     vec_send, vec_recv, vec_own) = refs[6 + 2 * n :]
    batch, length, width = x_ref.shape
    zo, yi, s = lax.axis_index("zo"), lax.axis_index("yi"), lax.axis_index("seq")
    me = yi * lay.seq + s
    x, core = s // 2, lax.rem(s, 2)
    partner = (zo, yi, x * 2 + 1 - core)

    def chip(ry, rx):
        return (zo, lax.rem(yi + ry, lay.sub), lax.rem(x + rx, lay.chips_x) * 2 + core)

    rank = zo * lay.group + me
    device_of = functools.partial(device_after, lay, rank)
    barrier_all(lay, device_of)

    def vec_copy(k):
        return remote(vec_ref, vectors.at[rank], vec_send.at[k - 1], vec_recv.at[k - 1], device_of(k))

    def vec_start(k, carry):
        vec_copy(k).start()
        return carry

    def vec_finish(k, carry):
        vec_copy(k).wait()
        return carry

    lax.fori_loop(1, lay.count, vec_start, 0)
    vec_mine = pltpu.make_async_copy(vec_ref, vectors.at[rank], vec_own.at[0])
    vec_mine.start()
    slot = {offset: i for i, offset in enumerate(lay.offsets)}
    own_copy = pltpu.make_async_copy(x_ref, held.at[0, 0], own_sem)
    own_copy.start()
    straight = [o for o in lay.far if not (o[0] and o[1])]
    diagonal = [o for o in lay.far if o[0] and o[1]]
    copies = {}
    for o in straight:
        copies[o] = [remote(x_ref, held.at[0, slot[o]], send.at[slot[o], 0], recv.at[slot[o], 0], chip(*o))]
    half = batch // 2
    for ry, rx in diagonal:
        j = slot[(ry, rx)]
        copies[(ry, rx)] = [
            remote(held.at[0, slot[(0, rx)], :half], held.at[0, j, :half], send.at[j, 0], recv.at[j, 0], chip(ry, 0)),
            remote(held.at[0, slot[(ry, 0)], half:], held.at[0, j, half:], send.at[j, 1], recv.at[j, 1], chip(0, rx)),
        ]
    to_partner = {
        o: remote(x_ref if o == (0, 0) else held.at[0, slot[o]], held.at[1, slot[o]],
                  core_send.at[slot[o]], core_recv.at[slot[o]], partner)
        for o in lay.offsets
    }
    for o in straight:
        copies[o][0].start()
    to_partner[(0, 0)].start()
    swaps = swap_copies(lay, plan, me, sources, targets, w_send, w_recv, False)
    swaps += swap_own(lay, plan, me, sources, targets, w_own, False)
    lax.fori_loop(1, lay.count, vec_finish, 0)
    vec_mine.wait()
    vec_out = pltpu.make_async_copy(vectors, all_ref, vec_own.at[1])
    vec_out.start()
    size = width // lay.count
    lane = lax.broadcasted_iota(jnp.int32, (1, 128), 1)
    for v in range(4):
        row, low = (v * size) // 128, (v * size) % 128
        for k in range(width // 128):
            line = None
            for j in range(128 // size):
                piece = vectors[k * (128 // size) + j, row : row + 1, :]
                turn = (j * size - low) % 128
                piece = pltpu.roll(piece, turn, 1) if turn else piece
                line = piece if line is None else jnp.where(lane >= j * size, piece, line)
            gain_buf[v : v + 1, k * 128 : (k + 1) * 128] = line
    gains = [gain_buf[i : i + 1, :] for i in range(4)]
    rows = 16
    pending = [[], []]
    turn = [0]

    def norm(c, j):
        for m in range(batch):
            k = turn[0] % 2
            turn[0] += 1
            for copy in pending[k]:
                copy.wait()

            def chunk(i, carry):
                at = pl.ds(pl.multiple_of(i * rows, rows), rows)
                value = held[c, j, m, at, :].astype(F32)
                center = value - jnp.mean(value, -1, keepdims=True)
                hat = center * lax.rsqrt(jnp.mean(center * center, -1, keepdims=True) + EPSILON)
                stage[k, 0, at, :] = (hat * gains[2] + gains[0]).astype(BF16)
                stage[k, 1, at, :] = (hat * gains[3] + gains[1]).astype(BF16)
                stage[k, 2, at, :] = hat.astype(BF16)
                return carry

            lax.fori_loop(0, length // rows, chunk, 0)
            pending[k] = [
                pltpu.make_async_copy(stage.at[k, i], ref.at[c, j, m], out_sem.at[k, i])
                for i, ref in enumerate((one_ref, two_ref, hat_ref))
            ]
            for copy in pending[k]:
                copy.start()

    own_copy.wait()
    norm(0, 0)
    to_partner[(0, 0)].wait_recv()
    norm(1, 0)
    for o in straight:
        copies[o][0].wait_recv()
        to_partner[o].start()
        for ry, rx in diagonal:
            if o == (0, rx):
                copies[(ry, rx)][0].start()
            if o == (ry, 0):
                copies[(ry, rx)][1].start()
        if o == straight[-1]:
            for copy in swaps:
                copy.start()
        norm(0, slot[o])
    for o in straight:
        to_partner[o].wait_recv()
        norm(1, slot[o])
    for o in diagonal:
        for copy in copies[o]:
            copy.wait_recv()
        to_partner[o].start()
        norm(0, slot[o])
    for o in diagonal:
        to_partner[o].wait_recv()
        norm(1, slot[o])
    for side in pending:
        for copy in side:
            copy.wait()
    for o in lay.far:
        for copy in copies[o]:
            copy.wait_send()
    for o in lay.offsets:
        to_partner[o].wait_send()
    for copy in swaps:
        copy.wait()
    vec_out.wait()


def norm_exchange(lay, plan, tokens, vec, weights):
    count = sum(parts for parts, _, _ in plan)
    chips = lay.group // 2
    whole = jax.ShapeDtypeStruct((2, chips, *tokens.shape), BF16)
    return pl.pallas_call(
        functools.partial(norm_kernel, lay, plan),
        out_shape=[whole] * 3 + [jax.ShapeDtypeStruct((lay.count, *vec.shape), F32)] + swap_shapes(lay, plan, False),
        in_specs=[ANY] * (2 + len(plan)),
        out_specs=[ANY] * (4 + len(plan)),
        scratch_shapes=[
            pltpu.VMEM((2, chips, *tokens.shape), BF16),
            pltpu.VMEM((2, 3, *tokens.shape[1:]), BF16),
            pltpu.VMEM((lay.count, *vec.shape), F32),
            pltpu.VMEM((4, tokens.shape[2]), F32),
            pltpu.SemaphoreType.DMA((chips, 2)),
            pltpu.SemaphoreType.DMA((chips, 2)),
            pltpu.SemaphoreType.DMA((chips,)),
            pltpu.SemaphoreType.DMA((chips,)),
            pltpu.SemaphoreType.DMA((lay.group - 1, count)),
            pltpu.SemaphoreType.DMA((lay.group - 1, count)),
            pltpu.SemaphoreType.DMA((count,)),
            pltpu.SemaphoreType.DMA,
            pltpu.SemaphoreType.DMA((2, 3)),
            pltpu.SemaphoreType.DMA((lay.count - 1,)),
            pltpu.SemaphoreType.DMA((lay.count - 1,)),
            pltpu.SemaphoreType.DMA((2,)),
        ],
        compiler_params=pltpu.CompilerParams(
            collective_id=1, has_side_effects=True, vmem_limit_bytes=48 << 20
        ),
        cost_estimate=busy(100),
        name="norm_exchange",
    )(tokens, vec, *weights)


def deal_kernel(lay, plan, back, *refs):
    n = len(plan)
    sources, targets = refs[:n], refs[n : 2 * n]
    send, recv, own = refs[2 * n :]
    me = lax.axis_index("yi") * lay.seq + lax.axis_index("seq")
    group_barrier(lay, me)
    copies = swap_copies(lay, plan, me, sources, targets, send, recv, back)
    copies += swap_own(lay, plan, me, sources, targets, own, back)
    for copy in copies:
        copy.start()
    for copy in copies:
        copy.wait()


def deal_exchange(lay, plan, arrays, back, number):
    count = sum(parts for parts, _, _ in plan)
    return pl.pallas_call(
        functools.partial(deal_kernel, lay, plan, back),
        out_shape=swap_shapes(lay, plan, back),
        in_specs=[ANY] * len(plan),
        out_specs=[ANY] * len(plan),
        scratch_shapes=[
            pltpu.SemaphoreType.DMA((lay.group - 1, count)),
            pltpu.SemaphoreType.DMA((lay.group - 1, count)),
            pltpu.SemaphoreType.DMA((count,)),
        ],
        compiler_params=pltpu.CompilerParams(collective_id=number, has_side_effects=True),
        cost_estimate=busy(17),
    )(*arrays)


def pair_kernel(lay, first_ref, first_w, second_ref, second_w, *refs):
    step = pl.program_id(0)
    chips = lay.group // 2
    (given, came, send, recv, out_sem), outs = refs[-5:], refs[:-5]
    batch = len(outs) // chips
    zo, yi, s = lax.axis_index("zo"), lax.axis_index("yi"), lax.axis_index("seq")
    partner = (zo, yi, (s // 2) * 2 + 1 - lax.rem(s, 2))

    def copy(j):
        return remote(given.at[j], came.at[j], send.at[j], recv.at[j], partner)

    def stores(j):
        length = came.shape[1] // batch
        return [
            pltpu.make_async_copy(
                came.at[j, pl.ds(m * length, length)], outs[(j + 1) % chips * batch + m], out_sem.at[j, m]
            )
            for m in range(batch)
        ]

    @pl.when(step == 0)
    def _():
        barrier = pltpu.get_barrier_semaphore()
        pl.semaphore_signal(barrier, inc=1, device_id=partner, device_id_type=MESH)
        pl.semaphore_wait(barrier, 1)

    for j in range(chips):

        @pl.when(step == j + 1)
        def _():
            copy(j).start()

    total = dot(first_ref[0, 0], first_w[...], ((1,), (1,))) + dot(second_ref[0, 0], second_w[...], ((1,), (1,)))
    for j in range(chips):

        @pl.when(step == j)
        def _():
            given[j] = total.astype(BF16)

        @pl.when(step == chips + j)
        def _():
            copy(j).wait_recv()
            came[j] = (total + came[j].astype(F32)).astype(BF16)

    for j in range(chips - 1):

        @pl.when(step == chips + j + 1)
        def _():
            for piece in stores(j):
                piece.start()

    @pl.when(step == 2 * chips - 1)
    def _():
        for piece in stores(chips - 1):
            piece.start()
        for j in range(chips):
            copy(j).wait_send()
            for piece in stores(j):
                piece.wait()


def pair_matmul(lay, first, first_w, second, second_w, batch, cut, number):
    chips = lay.group // 2
    rows = first.shape[0] // lay.group
    width = first_w.shape[0] // cut[1]
    depth1, depth2 = first.shape[1], second.shape[1]

    def act(depth):
        return pl.BlockSpec((1, 1, rows, depth), lambda i: (1 - i // chips, (i + 1) % chips, 0, 0))

    def weight(depth):
        return pl.BlockSpec((width, depth), lambda i: (cut[0], 0), pipeline_mode=pl.Buffered(1))

    shape = lambda v: v.reshape(2, chips, rows, v.shape[1])
    return pl.pallas_call(
        functools.partial(pair_kernel, lay),
        grid=(2 * chips,),
        in_specs=[act(depth1), weight(depth1), act(depth2), weight(depth2)],
        out_specs=[ANY] * (chips * batch),
        out_shape=[jax.ShapeDtypeStruct((rows // batch, width), BF16)] * (chips * batch),
        scratch_shapes=[
            pltpu.VMEM((chips, rows, width), BF16),
            pltpu.VMEM((chips, rows, width), BF16),
            pltpu.SemaphoreType.DMA((chips,)),
            pltpu.SemaphoreType.DMA((chips,)),
            pltpu.SemaphoreType.DMA((chips, batch)),
        ],
        compiler_params=pltpu.CompilerParams(
            collective_id=number, has_side_effects=True, vmem_limit_bytes=60 << 20
        ),
        cost_estimate=pl.CostEstimate(
            flops=2 * first.shape[0] * (depth1 + depth2) * width, bytes_accessed=32 << 20, transcendentals=0
        ),
    )(shape(first), first_w, shape(second), second_w)


def turn_pairs(field, cosine, sine):
    halves = ROTARY // 2
    front = field[:, :128]
    lane = lax.broadcasted_iota(jnp.int32, front.shape, 1)
    other = jnp.where(lane < halves, pltpu.roll(front, 128 - halves, 1), pltpu.roll(front, halves, 1))
    return jnp.concatenate([front * cosine + other * sine, field[:, 128:]], -1)


QUERY_BLOCK = 256


def wide_angles(ref):
    part = ref[0]
    return jnp.transpose(jnp.concatenate([part, part, part, part], 0), (1, 0))


def wide_pair(cos_ref, sin_ref):
    cosine, sine = wide_angles(cos_ref), wide_angles(sin_ref)
    lane = lax.broadcasted_iota(jnp.int32, cosine.shape, 1)
    cosine = jnp.where(lane < ROTARY, cosine, 1.0)
    sine = jnp.where(lane < ROTARY // 2, -sine, jnp.where(lane < ROTARY, sine, 0.0))
    return cosine, sine


def attend_kernel(scaling, packed_ref, cos_ref, sin_ref, col_ref, row_ref, q_ref, k_ref, v_ref, ctx_ref, lse_ref,
                  q_buf, k_buf, v_buf, ctx_buf, cos_buf, sin_buf):
    cores, _, chips, _, length, _ = packed_ref.shape
    cos_all, sin_all = wide_pair(cos_ref, sin_ref)
    cos_buf[...] = cos_all
    sin_buf[...] = sin_all
    for c in range(cores):
        for i in range(chips):
            at = pl.ds((c * chips + i) * length, length)
            block = packed_ref[c, 0, i, 0]
            cosine, sine = cos_buf[at, :], sin_buf[at, :]
            q_buf[at, :] = turn_pairs(block[:, :HEAD_DIM], cosine, sine).astype(BF16)
            k_buf[at, :] = turn_pairs(block[:, HEAD_DIM : 2 * HEAD_DIM], cosine, sine).astype(BF16)
            v_buf[at, :] = block[:, 2 * HEAD_DIM :].astype(BF16)
    q_ref[0] = q_buf[...]
    k_ref[0] = k_buf[...]
    v_ref[0] = v_buf[...]
    total = cores * chips * length

    def one(j, carry):
        at = pl.ds(pl.multiple_of(j * QUERY_BLOCK, QUERY_BLOCK), QUERY_BLOCK)
        scores = dot(k_buf[...], q_buf[at, :], ((1,), (1,))) * scaling
        allowed = col_ref[0] <= row_ref[0, :, at]
        scores = jnp.where(allowed, scores, NEGATIVE)
        top = jnp.max(scores, 0, keepdims=True)
        weights = jnp.where(allowed, jnp.exp(scores - top), 0.0)
        total_row = jnp.sum(weights, 0, keepdims=True)
        probs = (weights * (1.0 / total_row)).astype(BF16)
        ctx_buf[at, :] = dot(probs, v_buf[...], ((0,), (0,))).astype(BF16)
        lse_ref[0, :, at] = top + jnp.log(total_row)
        return carry

    lax.fori_loop(0, total // QUERY_BLOCK, one, 0)
    for c in range(cores):
        for i in range(chips):
            ctx_ref[c, 0, i, 0] = ctx_buf[pl.ds((c * chips + i) * length, length), :]


def attend_back_kernel(scaling, q_ref, k_ref, v_ref, g_ref, cos_ref, sin_ref, col_ref, row_ref, lse_ref, out_ref,
                       g_buf, dq_buf, dk_buf, dv_buf, cos_buf, sin_buf):
    cores, _, chips, _, length, _ = out_ref.shape
    total = q_ref.shape[1]
    cos_all, sin_all = wide_pair(cos_ref, sin_ref)
    cos_buf[...] = cos_all
    sin_buf[...] = sin_all
    for c in range(cores):
        for i in range(chips):
            g_buf[pl.ds((c * chips + i) * length, length), :] = g_ref[c, 0, i, 0]
    dk_buf[...] = jnp.zeros_like(dk_buf)
    dv_buf[...] = jnp.zeros_like(dv_buf)

    def one(j, carry):
        at = pl.ds(pl.multiple_of(j * QUERY_BLOCK, QUERY_BLOCK), QUERY_BLOCK)
        queries = q_ref[0, at, :]
        grads = g_buf[at, :]
        scores = dot(k_ref[0], queries, ((1,), (1,))) * scaling
        allowed = col_ref[0] <= row_ref[0, :, at]
        scores = jnp.where(allowed, scores, NEGATIVE)
        probs = jnp.where(allowed, jnp.exp(scores - lse_ref[0, :, at]), 0.0)
        grad_probs = dot(v_ref[0], grads, ((1,), (1,)))
        delta = jnp.sum(probs * grad_probs, 0, keepdims=True)
        grad_scores = (probs * (grad_probs - delta)).astype(BF16)
        dv_buf[...] += dot(probs.astype(BF16), grads, ((1,), (0,)))
        dk_buf[...] += dot(grad_scores, queries, ((1,), (0,)))
        dq_buf[at, :] = dot(grad_scores, k_ref[0], ((0,), (0,)))
        return carry

    lax.fori_loop(0, total // QUERY_BLOCK, one, 0)
    for c in range(cores):
        for i in range(chips):
            at = pl.ds((c * chips + i) * length, length)
            cosine, sine = cos_buf[at, :], sin_buf[at, :]
            out_ref[c, 0, i, 0, :, :HEAD_DIM] = turn_pairs(dq_buf[at, :] * scaling, cosine, -sine).astype(BF16)
            out_ref[c, 0, i, 0, :, HEAD_DIM : 2 * HEAD_DIM] = turn_pairs(dk_buf[at, :] * scaling, cosine, -sine).astype(BF16)
            out_ref[c, 0, i, 0, :, 2 * HEAD_DIM :] = dv_buf[at, :].astype(BF16)


def make_body(lay):
    sub, seq, group, chips_x = lay.sub, lay.seq, lay.group, lay.chips_x

    square = sub == 2 and chips_x == 2

    def across(value, o):
        return lax.ppermute(value, GROUP, lay.shift(*o))

    def partners(pieces):
        return [lax.ppermute(piece, "seq", lay.flip()) for piece in pieces]

    def add(*pieces):
        total = pieces[0].astype(F32)
        for piece in pieces[1:]:
            total = total + piece.astype(F32)
        return total

    def far_first(pieces):
        if square:
            return [
                [across(pieces[2][0], (1, 0)), across(pieces[3][0], (1, 0))],
                [across(pieces[1][1], (0, 1)), across(pieces[3][1], (0, 1))],
            ]
        batch = len(pieces[0])
        return [
            [across(pieces[i][m], ((-o[0]) % sub, (-o[1]) % chips_x)) for i, o in enumerate(lay.offsets) if i]
            for m in range(batch)
        ]

    def far_onward(pieces, came):
        if square:
            return [add(pieces[1][0], came[0][1]).astype(BF16), add(pieces[2][1], came[1][1]).astype(BF16)]
        return []

    def far_second(pieces, came, onward):
        if square:
            last = [across(onward[0], (0, 1)), across(onward[1], (1, 0))]
            return [[pieces[0][m], came[m][0], last[m]] for m in range(2)]
        return [[pieces[0][m], *came[m]] for m in range(len(came))]

    def add_all(parts):
        return jnp.stack([add(*pieces) for pieces in parts])

    def after(value, *tokens):
        return lax.optimization_barrier((value, *tokens))[0]

    def step(
        tokens, positions, cotangent, gain1, bias1, gain2, bias2,
        w_qkv, b_qkv, w_out, b_out, w_up, b_up, w_down, b_down,
    ):
        batch, length, width = tokens.shape
        rows = w_qkv.shape[0]
        ff = w_up.shape[1]
        count = seq * length
        total = group * batch * length
        my_seq = lax.axis_index("seq")
        me = lax.axis_index("yi") * seq + my_seq
        scaling = HEAD_DIM ** (-0.5)
        cols = lay.heads * HEAD_DIM
        ff_cols = ff // group
        out_cols = width // group
        plans = {"up": (1, rows, ff_cols), "down": (1, rows, ff_cols), "qkv": (3, rows, cols), "out": (1, rows, out_cols)}

        def gather_rows(mine):
            return lax.all_gather(mine, "zo", axis=0, tiled=True)

        x, core = my_seq // 2, my_seq % 2
        places = []
        for ry in range(sub):
            from_there = positions
            if ry:
                from_there = lax.ppermute(positions, "yi", [(i, (i + ry) % sub) for i in range(sub)])
            blocks = from_there.reshape(batch, seq, length)
            order = [((x - rx) % chips_x) * 2 + (core + rc) % 2 for rc in range(2) for rx in range(chips_x)]
            places.append(jnp.concatenate([lax.dynamic_slice_in_dim(blocks, o, 1, 1) for o in order], 1))
        places = jnp.stack(places).reshape(sub * batch, count)

        def laid(values):
            size = -(-sum(v.size for v in values) // 1024) * 1024
            whole, at = 0.0, 0
            for v in values:
                whole = whole + jnp.pad(v.astype(F32), (at, size - at - v.size))
                at += v.size
            return whole.reshape(-1, 128)

        names = (bias1, bias2, gain1, gain2, b_qkv, b_up, b_out, b_down)
        (qkv_own,) = deal_exchange(lay, [plans["qkv"]], [w_qkv], False, 0)
        qkv_w = gather_rows(qkv_own)
        w_up_late, _ = lax.optimization_barrier((w_up, qkv_own))
        (up_own,) = deal_exchange(lay, [plans["up"]], [w_up_late], False, 7)
        up_w = gather_rows(up_own)
        tokens_late, _ = lax.optimization_barrier((tokens, up_own))
        one, two, hat, vectors, out_own, down_own = norm_exchange(
            lay, [plans["out"], plans["down"]], tokens_late, laid(names), [w_out, w_down]
        )
        out_w = gather_rows(out_own)
        down_w = gather_rows(down_own)
        vectors = vectors.reshape(lay.count, -1)
        cuts = []
        at = 0
        for piece in names:
            cuts.append(vectors[:, at : at + piece.shape[0]].reshape(-1))
            at += piece.shape[0]
        _, _, gain1_all, gain2_all, b_qkv_all, b_up_all, b_out_all, b_down_all = cuts
        b_qkv_mine = lax.dynamic_index_in_dim(b_qkv_all.reshape(3, group, cols), me, 1, keepdims=False).reshape(-1)
        b_up_mine = lax.dynamic_index_in_dim(b_up_all.reshape(group, ff_cols), me, 0, keepdims=False)
        one, two, hat = [v.reshape(total, width) for v in (one, two, hat)]
        cotangent, hat, places = lax.optimization_barrier((cotangent, hat, places))
        near_dy = [across(cotangent, o) for o in lay.offsets[1:] if not (square and o == (1, 1))]

        halves = ROTARY // 2
        frequency = jnp.exp(jnp.arange(halves, dtype=F32) * (-2.0 * math.log(10000.0) / ROTARY))
        phases = places.astype(F32)[:, None, :] * frequency[None, :, None]
        cosine, sine = jnp.cos(phases), jnp.sin(phases)
        place_col = places[:, :, None]
        place_row = places[:, None, :]

        seqs = sub * batch
        one = after(one, cosine, sine)
        packed = dot(one, qkv_w, ((1,), (0,))) + b_qkv_mine
        wide = (2, 1, chips_x, 1, length, 3 * cols)
        wide_spec = pl.BlockSpec(wide, lambda i: (0, i // batch, 0, i % batch, 0, 0))
        full = (2, sub, chips_x, batch, length, 3 * cols)
        head_spec = pl.BlockSpec((1, count, HEAD_DIM), lambda i: (i, 0, 0))
        turn_spec = pl.BlockSpec((1, ROTARY // 2, count), lambda i: (i, 0, 0))
        tokens_spec = pl.BlockSpec((2, 1, chips_x, 1, length, cols), lambda i: (0, i // batch, 0, i % batch, 0, 0))
        by_token = (2, sub, chips_x, batch, length, cols)
        turn_bufs = [pltpu.VMEM((count, 128), F32)] * 2
        col_spec = pl.BlockSpec((1, count, 1), lambda i: (i, 0, 0))
        row_spec = pl.BlockSpec((1, 1, count), lambda i: (i, 0, 0))
        head_shape = jax.ShapeDtypeStruct((seqs, count, HEAD_DIM), BF16)
        work = 2 * seqs * count * count * HEAD_DIM
        params = pltpu.CompilerParams(vmem_limit_bytes=56 << 20)
        queries, keys, values, context, lse = pl.pallas_call(
            functools.partial(attend_kernel, scaling),
            grid=(seqs,),
            in_specs=[wide_spec, turn_spec, turn_spec, col_spec, row_spec],
            out_specs=[head_spec] * 3 + [tokens_spec, row_spec],
            out_shape=[head_shape] * 3 + [jax.ShapeDtypeStruct(by_token, BF16), jax.ShapeDtypeStruct((seqs, 1, count), F32)],
            scratch_shapes=[pltpu.VMEM((count, HEAD_DIM), BF16)] * 4 + turn_bufs,
            compiler_params=params,
            cost_estimate=pl.CostEstimate(flops=2 * work, bytes_accessed=30 << 20, transcendentals=seqs * count * count),
            name="attend",
        )(packed.reshape(full), cosine, sine, place_col, place_row)

        context = context.reshape(total, cols)
        two, *near_dy = lax.optimization_barrier((two, *near_dy, context))[:-1]
        pieces = [cotangent, *near_dy]
        early = partners(pieces)
        if square:
            halves_dy = [across(pieces[1][0], (1, 0)), across(pieces[2][1], (0, 1))]

        hidden = dot(two, up_w, ((1,), (0,))) + b_up_mine
        phi_cdf = 0.5 * (1.0 + lax.erf(hidden * math.sqrt(0.5)))
        density = jnp.exp(-0.5 * hidden * hidden) * (1.0 / math.sqrt(2.0 * math.pi))
        activated = (hidden * phi_cdf).astype(BF16)
        slope = (phi_cdf + hidden * density).astype(BF16)
        activated, slope = lax.optimization_barrier((activated, slope))

        def scatter(grad):
            return lax.psum_scatter(grad, "zo", scatter_dimension=0, tiled=True)

        def outer_dot(left, right):
            return dot(left, right, ((0,), (0,))).astype(BF16)

        qkv_late, up_late = lax.optimization_barrier((qkv_w, up_w, activated))[:-1]
        fold_qkv = (gain1_all[:, None] * qkv_late.astype(F32)).astype(BF16)
        fold_up = (gain2_all[:, None] * up_late.astype(F32)).astype(BF16)
        flat = lambda values: [v.reshape(-1, width) for v in values]
        if square:
            halves_dy = lax.optimization_barrier((*halves_dy, fold_qkv, fold_up))[:2]
            rows_dy = flat(pieces) + flat(halves_dy) + flat(early) + flat(partners(halves_dy))
        else:
            rows_dy = flat(pieces) + flat(early)
        upstream = jnp.concatenate(rows_dy, 0)
        down_part = outer_dot(upstream, activated)
        upstream = after(upstream, down_part)
        down_sum = scatter(down_part)
        grad_context = dot(upstream, out_w, ((1,), (0,))).astype(BF16)
        upstream = after(upstream, grad_context)
        out_part = outer_dot(upstream, context)
        out_w_sum = scatter(out_part)

        def chain(values, *tokens):
            return lax.optimization_barrier((*values, *tokens))[: len(values)]

        def tokens_of(pieces):
            return [pieces[i * batch : (i + 1) * batch] for i in range(group // 2)]

        pair = chain((context, activated), out_part)
        out_near = pair_matmul(lay, pair[0], out_w, pair[1], down_w, batch, (0, 1), 4)
        grad_context, *out_near = chain((grad_context, *out_near))
        out_near = tokens_of(out_near)
        out_came = far_first(out_near)

        grad_packed = pl.pallas_call(
            functools.partial(attend_back_kernel, scaling),
            grid=(seqs,),
            in_specs=[head_spec] * 3 + [tokens_spec, turn_spec, turn_spec, col_spec, row_spec, row_spec],
            out_specs=wide_spec,
            out_shape=jax.ShapeDtypeStruct(full, BF16),
            scratch_shapes=[pltpu.VMEM((count, HEAD_DIM), BF16)] + [pltpu.VMEM((count, HEAD_DIM), F32)] * 3 + turn_bufs,
            compiler_params=params,
            cost_estimate=pl.CostEstimate(flops=5 * work, bytes_accessed=24 << 20, transcendentals=seqs * count * count),
            name="attend_back",
        )(queries, keys, values, grad_context.reshape(by_token), cosine, sine, place_col, place_row, lse)
        grad_packed = grad_packed.reshape(total, 3 * cols)

        qkv_part = outer_dot(hat, grad_packed)
        qkv_sum = scatter(qkv_part)
        out_came, upstream = chain((out_came, upstream), qkv_part)
        onward, upstream = chain((far_onward(out_near, out_came), upstream))
        out_parts = far_second(out_near, out_came, onward)
        grad_hidden = (dot(upstream, down_w, ((1,), (0,))) * slope.astype(F32)).astype(BF16)

        near0 = pair_matmul(lay, grad_packed, fold_qkv, grad_hidden, fold_up, batch, (0, 2), 5)
        hat, near0 = chain((hat, near0))
        near0 = tokens_of(near0)
        came0 = far_first(near0)
        up_part = outer_dot(hat, grad_hidden)
        up_sum = scatter(up_part)
        came0, left = chain((came0, grad_packed), up_part)
        onward, left = chain((far_onward(near0, came0), left))
        parts0 = far_second(near0, came0, onward)
        near1 = pair_matmul(lay, left, fold_qkv, grad_hidden, fold_up, batch, (1, 2), 6)
        near1 = tokens_of(near1)
        came1 = far_first(near1)

        own_sums = [
            jnp.sum(grad_packed.astype(F32), 0),
            jnp.sum(grad_hidden.astype(F32), 0),
            jnp.sum(cotangent.astype(F32), (0, 1)),
        ]
        out_parts, vec, down_sum, out_w_sum = chain((out_parts, laid(own_sums), down_sum, out_w_sum), near1)
        output = (tokens.astype(F32) + add_all(out_parts) + b_out_all + b_down_all).astype(BF16)
        came1, vec = chain((came1, vec), output)
        onward, vec = chain((far_onward(near1, came1), vec))
        parts1 = far_second(near1, came1, onward)
        everyone, down_raw, out_raw, qkv_raw = exchange(
            lay, [plans["down"], plans["out"], plans["qkv"]], vec, [down_sum, out_w_sum, qkv_sum], 2, 40
        )
        (parts1,) = chain((parts1,), everyone)

        inputs = tokens.astype(F32)
        center = inputs - jnp.mean(inputs, -1, keepdims=True)
        inv_std = lax.rsqrt(jnp.mean(center * center, -1, keepdims=True) + EPSILON)
        normal = center * inv_std
        grad_normal = jnp.concatenate([add_all(parts0), add_all(parts1)], -1)
        token_grad = cotangent.astype(F32) + inv_std * (
            grad_normal
            - jnp.mean(grad_normal, -1, keepdims=True)
            - normal * jnp.mean(grad_normal * normal, -1, keepdims=True)
        )

        rank = lax.axis_index("zo") * group + me
        (up_raw,) = deal_exchange(lay, [plans["up"]], [up_sum], True, 3)
        sums = jnp.sum(everyone.reshape(lay.outer, group, -1), 0)
        sum_qkv = jnp.transpose(sums[:, : 3 * cols].reshape(group, 3, cols), (1, 0, 2)).reshape(-1)
        sum_up = sums[:, 3 * cols : 3 * cols + ff_cols].reshape(-1)
        sum_dy = jnp.sum(sums[:, 3 * cols + ff_cols : 3 * cols + ff_cols + width], 0)

        def own_part(vector):
            return lax.dynamic_index_in_dim(vector.reshape(lay.count, -1), rank, 0, keepdims=False)

        up_raw, qkv_raw = up_raw.astype(F32), qkv_raw.astype(F32)
        column = lambda v: v.astype(F32)[:, None]
        return (
            output,
            token_grad,
            jnp.sum(w_qkv.astype(F32) * qkv_raw, 1),
            jnp.sum(w_qkv.astype(F32) * sum_qkv, 1),
            jnp.sum(w_up.astype(F32) * up_raw, 1),
            jnp.sum(w_up.astype(F32) * sum_up, 1),
            column(gain1) * qkv_raw + column(bias1) * sum_qkv,
            own_part(sum_qkv),
            out_raw.astype(F32),
            own_part(sum_dy),
            column(gain2) * up_raw + column(bias2) * sum_up,
            own_part(sum_up),
            down_raw.astype(F32),
            own_part(sum_dy),
        )

    return step


def solution(mesh):
    outer, sub, seq = split_axes(mesh)
    inner = Mesh(mesh.devices.reshape(outer, sub, seq), ALL)
    act = P(None, ALL, None)
    vec = P(ALL)
    mat = P(ALL, None)
    return jax.shard_map(
        make_body(Layout(outer, sub, seq)),
        mesh=inner,
        in_specs=(
            act, P(None, ("zo", "yi")), act, vec, vec, vec, vec,
            mat, vec, mat, vec, mat, vec, mat, vec,
        ),
        out_specs=(act, act, vec, vec, vec, vec, mat, vec, mat, vec, mat, vec, mat, vec),
        check_vma=False,
    )
```

```python
import functools
import math

import jax
import jax.numpy as jnp
from jax import lax
from jax.experimental import pallas as pl
from jax.experimental.pallas import tpu as pltpu
from jax.sharding import Mesh, PartitionSpec as P


HEADS = 8
HEAD_DIM = 256
ROTARY = 64
EPSILON = 1e-05
NEGATIVE = -1e30
F32 = jnp.float32
BF16 = jnp.bfloat16
ALL = ("zo", "yi", "seq")
GROUP = ("yi", "seq")
MESH = pl.DeviceIdType.MESH
ANY = pl.BlockSpec(memory_space=pl.ANY)


def dot(left, right, dims):
    return lax.dot_general(left, right, (dims, ((), ())), preferred_element_type=F32)


def split_axes(mesh):
    dp, seq = mesh.shape["dp"], mesh.shape["seq"]
    sub = 1
    while seq * sub * 2 <= HEADS and dp % (sub * 2) == 0:
        sub *= 2
    return dp // sub, sub, seq


def remote(source, target, send, recv, device):
    return pltpu.make_async_remote_copy(
        src_ref=source, dst_ref=target, send_sem=send, recv_sem=recv,
        device_id=device, device_id_type=MESH,
    )


class Layout:
    def __init__(self, outer, sub, seq):
        self.outer, self.sub, self.seq = outer, sub, seq
        self.chips_x = seq // 2
        self.group = sub * seq
        self.count = outer * self.group
        self.heads = HEADS // self.group
        self.offsets = [(ry, rx) for ry in range(sub) for rx in range(self.chips_x)]
        self.square = sub == 2 and self.chips_x == 2
        self.near = [o for o in self.offsets if not (self.square and o == (1, 1))]
        self.far = sorted(self.offsets[1:], key=lambda o: (o[0] > 0) + (o[1] > 0))

    def shift(self, ry, rx):
        pairs = []
        for y in range(self.sub):
            for x in range(self.chips_x):
                for c in range(2):
                    there = ((y + ry) % self.sub, (x + rx) % self.chips_x)
                    pairs.append((y * self.seq + x * 2 + c, there[0] * self.seq + there[1] * 2 + c))
        return pairs

    def flip(self):
        return [(i, i ^ 1) for i in range(self.seq)]


def swap_copies(lay, plan, me, sources, targets, send, recv, back):
    zo = lax.axis_index("zo")
    copies = []
    for k in range(1, lay.group):
        peer = lax.rem(me + k, lay.group)
        device = (zo, peer // lay.seq, lax.rem(peer, lay.seq))
        j = 0
        for (parts, rows, cols), source, target in zip(plan, sources, targets, strict=True):
            for part in range(parts):
                wide = lambda who: pl.ds(pl.multiple_of((part * lay.group + who) * cols, 128), cols)
                thin = pl.ds(part * cols, cols)
                block = lambda who: pl.ds(pl.multiple_of(who * rows, rows), rows)
                if back:
                    copies.append(remote(source.at[block(peer), thin], target.at[:, wide(me)], send.at[k - 1, j], recv.at[k - 1, j], device))
                else:
                    copies.append(remote(source.at[:, wide(peer)], target.at[block(me), thin], send.at[k - 1, j], recv.at[k - 1, j], device))
                j += 1
    return copies


def swap_own(lay, plan, me, sources, targets, sems, back):
    copies = []
    j = 0
    for (parts, rows, cols), source, target in zip(plan, sources, targets, strict=True):
        for part in range(parts):
            wide = pl.ds(pl.multiple_of((part * lay.group + me) * cols, 128), cols)
            thin = pl.ds(part * cols, cols)
            block = pl.ds(pl.multiple_of(me * rows, rows), rows)
            if back:
                copies.append(pltpu.make_async_copy(source.at[block, thin], target.at[:, wide], sems.at[j]))
            else:
                copies.append(pltpu.make_async_copy(source.at[:, wide], target.at[block, thin], sems.at[j]))
            j += 1
    return copies


def group_barrier(lay, me):
    zo = lax.axis_index("zo")
    barrier = pltpu.get_barrier_semaphore()
    for k in range(1, lay.group):
        peer = lax.rem(me + k, lay.group)
        pl.semaphore_signal(
            barrier, inc=1, device_id=(zo, peer // lay.seq, lax.rem(peer, lay.seq)), device_id_type=MESH
        )
    pl.semaphore_wait(barrier, lay.group - 1)


def swap_shapes(lay, plan, back):
    if back:
        return [jax.ShapeDtypeStruct((rows, parts * lay.group * cols), BF16) for parts, rows, cols in plan]
    return [jax.ShapeDtypeStruct((lay.group * rows, parts * cols), BF16) for parts, rows, cols in plan]


def device_after(lay, rank, k):
    peer = lax.rem(rank + k, lay.count)
    inner = lax.rem(peer, lay.group)
    return (peer // lay.group, inner // lay.seq, lax.rem(inner, lay.seq))


def barrier_all(lay, device_of):
    barrier = pltpu.get_barrier_semaphore()

    def greet(k, carry):
        pl.semaphore_signal(barrier, inc=1, device_id=device_of(k), device_id_type=MESH)
        return carry

    lax.fori_loop(1, lay.count, greet, 0)
    pl.semaphore_wait(barrier, lay.count - 1)


def busy(microseconds):
    return pl.CostEstimate(flops=int(7e8 * microseconds), bytes_accessed=1 << 20, transcendentals=0)


def norm_kernel(lay, plan, *refs):
    n = len(plan)
    x_ref, vec_ref, sources = refs[0], refs[1], refs[2 : 2 + n]
    one_ref, two_ref, hat_ref, all_ref, targets = *refs[2 + n : 6 + n], refs[6 + n : 6 + 2 * n]
    (held, stage, vectors, gain_buf, send, recv, core_send, core_recv, w_send, w_recv, w_own, own_sem, out_sem,
     vec_send, vec_recv, vec_own) = refs[6 + 2 * n :]
    batch, length, width = x_ref.shape
    zo, yi, s = lax.axis_index("zo"), lax.axis_index("yi"), lax.axis_index("seq")
    me = yi * lay.seq + s
    x, core = s // 2, lax.rem(s, 2)
    partner = (zo, yi, x * 2 + 1 - core)

    def chip(ry, rx):
        return (zo, lax.rem(yi + ry, lay.sub), lax.rem(x + rx, lay.chips_x) * 2 + core)

    rank = zo * lay.group + me
    device_of = functools.partial(device_after, lay, rank)
    barrier_all(lay, device_of)

    def vec_copy(k):
        return remote(vec_ref, vectors.at[rank], vec_send.at[k - 1], vec_recv.at[k - 1], device_of(k))

    def vec_start(k, carry):
        vec_copy(k).start()
        return carry

    def vec_finish(k, carry):
        vec_copy(k).wait()
        return carry

    lax.fori_loop(1, lay.count, vec_start, 0)
    vec_mine = pltpu.make_async_copy(vec_ref, vectors.at[rank], vec_own.at[0])
    vec_mine.start()
    slot = {offset: i for i, offset in enumerate(lay.offsets)}
    own_copy = pltpu.make_async_copy(x_ref, held.at[0, 0], own_sem)
    own_copy.start()
    straight = [o for o in lay.far if not (o[0] and o[1])]
    diagonal = [o for o in lay.far if o[0] and o[1]]
    copies = {}
    for o in straight:
        copies[o] = [remote(x_ref, held.at[0, slot[o]], send.at[slot[o], 0], recv.at[slot[o], 0], chip(*o))]
    half = batch // 2
    for ry, rx in diagonal:
        j = slot[(ry, rx)]
        copies[(ry, rx)] = [
            remote(held.at[0, slot[(0, rx)], :half], held.at[0, j, :half], send.at[j, 0], recv.at[j, 0], chip(ry, 0)),
            remote(held.at[0, slot[(ry, 0)], half:], held.at[0, j, half:], send.at[j, 1], recv.at[j, 1], chip(0, rx)),
        ]
    to_partner = {
        o: remote(x_ref if o == (0, 0) else held.at[0, slot[o]], held.at[1, slot[o]],
                  core_send.at[slot[o]], core_recv.at[slot[o]], partner)
        for o in lay.offsets
    }
    for o in straight:
        copies[o][0].start()
    to_partner[(0, 0)].start()
    swaps = swap_copies(lay, plan, me, sources, targets, w_send, w_recv, False)
    swaps += swap_own(lay, plan, me, sources, targets, w_own, False)
    lax.fori_loop(1, lay.count, vec_finish, 0)
    vec_mine.wait()
    vec_out = pltpu.make_async_copy(vectors, all_ref, vec_own.at[1])
    vec_out.start()
    size = width // lay.count
    lane = lax.broadcasted_iota(jnp.int32, (1, 128), 1)
    for v in range(4):
        row, low = (v * size) // 128, (v * size) % 128
        for k in range(width // 128):
            line = None
            for j in range(128 // size):
                piece = vectors[k * (128 // size) + j, row : row + 1, :]
                turn = (j * size - low) % 128
                piece = pltpu.roll(piece, turn, 1) if turn else piece
                line = piece if line is None else jnp.where(lane >= j * size, piece, line)
            gain_buf[v : v + 1, k * 128 : (k + 1) * 128] = line
    gains = [gain_buf[i : i + 1, :] for i in range(4)]
    rows = 16
    pending = [[], []]
    turn = [0]

    def norm(c, j):
        for m in range(batch):
            k = turn[0] % 2
            turn[0] += 1
            for copy in pending[k]:
                copy.wait()

            def chunk(i, carry):
                at = pl.ds(pl.multiple_of(i * rows, rows), rows)
                value = held[c, j, m, at, :].astype(F32)
                center = value - jnp.mean(value, -1, keepdims=True)
                hat = center * lax.rsqrt(jnp.mean(center * center, -1, keepdims=True) + EPSILON)
                stage[k, 0, at, :] = (hat * gains[2] + gains[0]).astype(BF16)
                stage[k, 1, at, :] = (hat * gains[3] + gains[1]).astype(BF16)
                stage[k, 2, at, :] = hat.astype(BF16)
                return carry

            lax.fori_loop(0, length // rows, chunk, 0, unroll=2)
            pending[k] = [
                pltpu.make_async_copy(stage.at[k, i], ref.at[c, j, m], out_sem.at[k, i])
                for i, ref in enumerate((one_ref, two_ref, hat_ref))
            ]
            for copy in pending[k]:
                copy.start()

    own_copy.wait()
    norm(0, 0)
    to_partner[(0, 0)].wait_recv()
    norm(1, 0)
    for o in straight:
        copies[o][0].wait_recv()
        to_partner[o].start()
        for ry, rx in diagonal:
            if o == (0, rx):
                copies[(ry, rx)][0].start()
            if o == (ry, 0):
                copies[(ry, rx)][1].start()
        if o == straight[-1]:
            for copy in swaps:
                copy.start()
        norm(0, slot[o])
    for o in straight:
        to_partner[o].wait_recv()
        norm(1, slot[o])
    for o in diagonal:
        for copy in copies[o]:
            copy.wait_recv()
        to_partner[o].start()
        norm(0, slot[o])
    for o in diagonal:
        to_partner[o].wait_recv()
        norm(1, slot[o])
    for side in pending:
        for copy in side:
            copy.wait()
    for o in lay.far:
        for copy in copies[o]:
            copy.wait_send()
    for o in lay.offsets:
        to_partner[o].wait_send()
    for copy in swaps:
        copy.wait()
    vec_out.wait()


def norm_exchange(lay, plan, tokens, vec, weights):
    count = sum(parts for parts, _, _ in plan)
    chips = lay.group // 2
    whole = jax.ShapeDtypeStruct((2, chips, *tokens.shape), BF16)
    return pl.pallas_call(
        functools.partial(norm_kernel, lay, plan),
        out_shape=[whole] * 3 + [jax.ShapeDtypeStruct((lay.count, *vec.shape), F32)] + swap_shapes(lay, plan, False),
        in_specs=[ANY] * (2 + len(plan)),
        out_specs=[ANY] * (4 + len(plan)),
        scratch_shapes=[
            pltpu.VMEM((2, chips, *tokens.shape), BF16),
            pltpu.VMEM((2, 3, *tokens.shape[1:]), BF16),
            pltpu.VMEM((lay.count, *vec.shape), F32),
            pltpu.VMEM((4, tokens.shape[2]), F32),
            pltpu.SemaphoreType.DMA((chips, 2)),
            pltpu.SemaphoreType.DMA((chips, 2)),
            pltpu.SemaphoreType.DMA((chips,)),
            pltpu.SemaphoreType.DMA((chips,)),
            pltpu.SemaphoreType.DMA((lay.group - 1, count)),
            pltpu.SemaphoreType.DMA((lay.group - 1, count)),
            pltpu.SemaphoreType.DMA((count,)),
            pltpu.SemaphoreType.DMA,
            pltpu.SemaphoreType.DMA((2, 3)),
            pltpu.SemaphoreType.DMA((lay.count - 1,)),
            pltpu.SemaphoreType.DMA((lay.count - 1,)),
            pltpu.SemaphoreType.DMA((2,)),
        ],
        compiler_params=pltpu.CompilerParams(
            collective_id=1, has_side_effects=True, vmem_limit_bytes=48 << 20
        ),
        cost_estimate=busy(100),
        name="norm_exchange",
    )(tokens, vec, *weights)


def deal_kernel(lay, plan, back, *refs):
    n = len(plan)
    sources, targets = refs[:n], refs[n : 2 * n]
    send, recv, own = refs[2 * n :]
    me = lax.axis_index("yi") * lay.seq + lax.axis_index("seq")
    group_barrier(lay, me)
    copies = swap_copies(lay, plan, me, sources, targets, send, recv, back)
    copies += swap_own(lay, plan, me, sources, targets, own, back)
    for copy in copies:
        copy.start()
    for copy in copies:
        copy.wait()


def deal_exchange(lay, plan, arrays, back, number):
    count = sum(parts for parts, _, _ in plan)
    return pl.pallas_call(
        functools.partial(deal_kernel, lay, plan, back),
        out_shape=swap_shapes(lay, plan, back),
        in_specs=[ANY] * len(plan),
        out_specs=[ANY] * len(plan),
        scratch_shapes=[
            pltpu.SemaphoreType.DMA((lay.group - 1, count)),
            pltpu.SemaphoreType.DMA((lay.group - 1, count)),
            pltpu.SemaphoreType.DMA((count,)),
        ],
        compiler_params=pltpu.CompilerParams(collective_id=number, has_side_effects=True),
        cost_estimate=busy(17),
    )(*arrays)


def pair_kernel(lay, plan, with_vec, scaled, batch, *refs):
    refs = list(refs)
    take = lambda k: [refs.pop(0) for _ in range(k)]
    step = pl.program_id(0)
    chips = lay.group // 2
    first_ref, first_w, second_ref, second_w = take(4)
    scales = take(2) if scaled else []
    sources, vec_ref = take(len(plan)), take(int(with_vec))
    outs, targets, all_ref = take(chips * batch), take(len(plan)), take(int(with_vec))
    given, came, send, recv, out_sem = take(5)
    zo, yi, s = lax.axis_index("zo"), lax.axis_index("yi"), lax.axis_index("seq")
    me = yi * lay.seq + s
    rank = zo * lay.group + me
    device_of = functools.partial(device_after, lay, rank)
    partner = (zo, yi, (s // 2) * 2 + 1 - lax.rem(s, 2))
    swap_sems = take(3) if plan else []
    vec_sems = take(3) if with_vec else []

    def copy(j):
        return remote(given.at[j], came.at[j], send.at[j], recv.at[j], partner)

    def stores(j):
        length = came.shape[1] // batch
        return [
            pltpu.make_async_copy(
                came.at[j, pl.ds(m * length, length)], outs[(j + 1) % chips * batch + m], out_sem.at[j, m]
            )
            for m in range(batch)
        ]

    def riders():
        if not plan:
            return []
        copies = swap_copies(lay, plan, me, sources, targets, swap_sems[0], swap_sems[1], True)
        return copies + swap_own(lay, plan, me, sources, targets, swap_sems[2], True)

    def vec_copy(k):
        return remote(vec_ref[0], all_ref[0].at[rank], vec_sems[0].at[k - 1], vec_sems[1].at[k - 1], device_of(k))

    def vec_start(k, carry):
        vec_copy(k).start()
        return carry

    def vec_finish(k, carry):
        vec_copy(k).wait()
        return carry

    def vec_mine():
        return pltpu.make_async_copy(vec_ref[0], all_ref[0].at[rank], vec_sems[2])

    @pl.when(step == 0)
    def _():
        if with_vec:
            barrier_all(lay, device_of)
            vec_mine().start()
            lax.fori_loop(1, lay.count, vec_start, 0)
        elif plan:
            group_barrier(lay, me)
        else:
            barrier = pltpu.get_barrier_semaphore()
            pl.semaphore_signal(barrier, inc=1, device_id=partner, device_id_type=MESH)
            pl.semaphore_wait(barrier, 1)
        for rider in riders():
            rider.start()

    for j in range(chips):

        @pl.when(step == j + 1)
        def _():
            copy(j).start()

    total = dot(first_ref[0, 0], first_w[...], ((1,), (1,)))
    other = dot(second_ref[0, 0], second_w[...], ((1,), (1,)))
    total = total * scales[0][...] + other * scales[1][...] if scaled else total + other
    for j in range(chips):

        @pl.when(step == j)
        def _():
            given[j] = total.astype(BF16)

        @pl.when(step == chips + j)
        def _():
            copy(j).wait_recv()
            came[j] = (total + came[j].astype(F32)).astype(BF16)

    for j in range(chips - 1):

        @pl.when(step == chips + j + 1)
        def _():
            for piece in stores(j):
                piece.start()

    @pl.when(step == 2 * chips - 1)
    def _():
        for piece in stores(chips - 1):
            piece.start()
        for j in range(chips):
            copy(j).wait_send()
            for piece in stores(j):
                piece.wait()
        for rider in riders():
            rider.wait()
        if with_vec:
            vec_mine().wait()
            lax.fori_loop(1, lay.count, vec_finish, 0)


def pair_matmul(lay, acts, weights, batch, cut, number, scales=(), plan=(), arrays=(), vec=None):
    chips = lay.group // 2
    rows = acts[0].shape[0] // lay.group
    width = weights[0].shape[0] // cut[1]
    count = sum(parts for parts, _, _ in plan)
    with_vec = vec is not None

    def act(depth):
        return pl.BlockSpec((1, 1, rows, depth), lambda i: (1 - i // chips, (i + 1) % chips, 0, 0))

    def weight(depth):
        return pl.BlockSpec((width, depth), lambda i: (cut[0], 0), pipeline_mode=pl.Buffered(1))

    specs, args = [], []
    for a, w in zip(acts, weights, strict=True):
        specs += [act(a.shape[1]), weight(a.shape[1])]
        args += [a.reshape(2, chips, rows, a.shape[1]), w]
    for scale in scales:
        specs.append(pl.BlockSpec((1, width), lambda i: (0, cut[0])))
        args.append(scale.reshape(1, -1))
    args += [*arrays, *([vec] if with_vec else [])]
    specs += [ANY] * (len(args) - len(specs))
    shapes = [jax.ShapeDtypeStruct((rows // batch, width), BF16)] * (chips * batch) + swap_shapes(lay, plan, True)
    scratch = [
        pltpu.VMEM((chips, rows, width), BF16),
        pltpu.VMEM((chips, rows, width), BF16),
        pltpu.SemaphoreType.DMA((chips,)),
        pltpu.SemaphoreType.DMA((chips,)),
        pltpu.SemaphoreType.DMA((chips, batch)),
    ]
    if plan:
        scratch += [pltpu.SemaphoreType.DMA((lay.group - 1, count))] * 2 + [pltpu.SemaphoreType.DMA((count,))]
    if with_vec:
        shapes.append(jax.ShapeDtypeStruct((lay.count, *vec.shape), F32))
        scratch += [pltpu.SemaphoreType.DMA((lay.count - 1,))] * 2 + [pltpu.SemaphoreType.DMA]
    depth = sum(a.shape[1] for a in acts)
    return pl.pallas_call(
        functools.partial(pair_kernel, lay, plan, with_vec, bool(scales), batch),
        grid=(2 * chips,),
        in_specs=specs,
        out_specs=[ANY] * len(shapes),
        out_shape=shapes,
        scratch_shapes=scratch,
        compiler_params=pltpu.CompilerParams(
            collective_id=number, has_side_effects=True, vmem_limit_bytes=60 << 20
        ),
        cost_estimate=pl.CostEstimate(
            flops=2 * acts[0].shape[0] * depth * width, bytes_accessed=32 << 20, transcendentals=0
        ),
    )(*args)


def turn_pairs(field, cosine, sine):
    halves = ROTARY // 2
    front = field[:, :128]
    lane = lax.broadcasted_iota(jnp.int32, front.shape, 1)
    other = jnp.where(lane < halves, pltpu.roll(front, 128 - halves, 1), pltpu.roll(front, halves, 1))
    return jnp.concatenate([front * cosine + other * sine, field[:, 128:]], -1)


QUERY_BLOCK = 256


def wide_angles(ref):
    part = ref[0]
    return jnp.transpose(jnp.concatenate([part, part, part, part], 0), (1, 0))


def wide_pair(cos_ref, sin_ref):
    cosine, sine = wide_angles(cos_ref), wide_angles(sin_ref)
    lane = lax.broadcasted_iota(jnp.int32, cosine.shape, 1)
    cosine = jnp.where(lane < ROTARY, cosine, 1.0)
    sine = jnp.where(lane < ROTARY // 2, -sine, jnp.where(lane < ROTARY, sine, 0.0))
    return cosine, sine


def attend_kernel(lay, scaling, *refs):
    refs = list(refs)
    take = lambda k: [refs.pop(0) for _ in range(k)]
    near_count = len(lay.near)
    packed_ref, cos_ref, sin_ref, col_ref, row_ref = take(5)
    near = take(near_count)
    q_ref, k_ref, v_ref, ctx_ref, lse_ref, dy_ref = take(6)
    q_buf, k_buf, v_buf, ctx_buf, cos_buf, sin_buf, bounce = take(7)
    load_sem, store_sem, core_send, core_recv, on_send, on_recv = take(6)
    step, last = pl.program_id(0), pl.num_programs(0) - 1
    zo, yi, s = lax.axis_index("zo"), lax.axis_index("yi"), lax.axis_index("seq")
    x, core = s // 2, lax.rem(s, 2)
    partner = (zo, yi, x * 2 + 1 - core)
    chips = lay.group // 2
    half = near[0].shape[0] // 2

    def load(i):
        return pltpu.make_async_copy(near[i], bounce.at[i], load_sem.at[i])

    def store(i):
        return pltpu.make_async_copy(bounce.at[i], dy_ref.at[0, i], store_sem.at[i])

    def to_partner(i):
        source = near[i] if i < near_count else dy_ref.at[0, i]
        return remote(source, dy_ref.at[1, i], core_send.at[i], core_recv.at[i], partner)

    def onward():
        if not lay.square:
            return []
        over_y = (zo, lax.rem(yi + 1, lay.sub), s)
        over_x = (zo, yi, lax.rem(x + 1, lay.chips_x) * 2 + core)
        return [
            remote(near[1].at[:half], dy_ref.at[0, 3, :half], on_send.at[0], on_recv.at[0], over_y),
            remote(near[2].at[half:], dy_ref.at[0, 3, half:], on_send.at[1], on_recv.at[1], over_x),
        ]

    @pl.when(step == 0)
    def _():
        group_barrier(lay, yi * lay.seq + s)
        for copy in onward():
            copy.start()
        for i in range(near_count):
            load(i).start()
            to_partner(i).start()

    @pl.when(step == 1)
    def _():
        for i in range(near_count):
            load(i).wait()
            store(i).start()

    attend_one(scaling, packed_ref, cos_ref, sin_ref, col_ref, row_ref, q_ref, k_ref, v_ref, ctx_ref, lse_ref,
               q_buf, k_buf, v_buf, ctx_buf, cos_buf, sin_buf)

    @pl.when(step == last)
    def _():
        for copy in onward():
            copy.wait_recv()
        for i in range(near_count, chips):
            to_partner(i).start()
        for i in range(near_count):
            store(i).wait()
        for i in range(chips):
            to_partner(i).wait()
        for copy in onward():
            copy.wait_send()


def attend_one(scaling, packed_ref, cos_ref, sin_ref, col_ref, row_ref, q_ref, k_ref, v_ref, ctx_ref, lse_ref,
               q_buf, k_buf, v_buf, ctx_buf, cos_buf, sin_buf):
    cores, _, chips, _, length, _ = packed_ref.shape
    cos_all, sin_all = wide_pair(cos_ref, sin_ref)
    cos_buf[...] = cos_all
    sin_buf[...] = sin_all
    for c in range(cores):
        for i in range(chips):
            at = pl.ds((c * chips + i) * length, length)
            block = packed_ref[c, 0, i, 0]
            cosine, sine = cos_buf[at, :], sin_buf[at, :]
            q_buf[at, :] = turn_pairs(block[:, :HEAD_DIM], cosine, sine).astype(BF16)
            k_buf[at, :] = turn_pairs(block[:, HEAD_DIM : 2 * HEAD_DIM], cosine, sine).astype(BF16)
            v_buf[at, :] = block[:, 2 * HEAD_DIM :].astype(BF16)
    q_ref[0] = q_buf[...]
    k_ref[0] = k_buf[...]
    v_ref[0] = v_buf[...]
    total = cores * chips * length

    def one(j, carry):
        at = pl.ds(pl.multiple_of(j * QUERY_BLOCK, QUERY_BLOCK), QUERY_BLOCK)
        scores = dot(k_buf[...], q_buf[at, :], ((1,), (1,))) * scaling
        allowed = col_ref[0] <= row_ref[0, :, at]
        scores = jnp.where(allowed, scores, NEGATIVE)
        top = jnp.max(scores, 0, keepdims=True)
        weights = jnp.where(allowed, jnp.exp(scores - top), 0.0)
        total_row = jnp.sum(weights, 0, keepdims=True)
        probs = (weights * (1.0 / total_row)).astype(BF16)
        ctx_buf[at, :] = dot(probs, v_buf[...], ((0,), (0,))).astype(BF16)
        lse_ref[0, :, at] = top + jnp.log(total_row)
        return carry

    lax.fori_loop(0, total // QUERY_BLOCK, one, 0)
    for c in range(cores):
        for i in range(chips):
            ctx_ref[c, 0, i, 0] = ctx_buf[pl.ds((c * chips + i) * length, length), :]


def attend_back_kernel(scaling, q_ref, k_ref, v_ref, g_ref, cos_ref, sin_ref, col_ref, row_ref, lse_ref, out_ref,
                       g_buf, dq_buf, dk_buf, dv_buf, cos_buf, sin_buf):
    cores, _, chips, _, length, _ = out_ref.shape
    total = q_ref.shape[1]
    cos_all, sin_all = wide_pair(cos_ref, sin_ref)
    cos_buf[...] = cos_all
    sin_buf[...] = sin_all
    for c in range(cores):
        for i in range(chips):
            g_buf[pl.ds((c * chips + i) * length, length), :] = g_ref[c, 0, i, 0]
    dk_buf[...] = jnp.zeros_like(dk_buf)
    dv_buf[...] = jnp.zeros_like(dv_buf)

    def one(j, carry):
        at = pl.ds(pl.multiple_of(j * QUERY_BLOCK, QUERY_BLOCK), QUERY_BLOCK)
        queries = q_ref[0, at, :]
        grads = g_buf[at, :]
        scores = dot(k_ref[0], queries, ((1,), (1,))) * scaling
        allowed = col_ref[0] <= row_ref[0, :, at]
        scores = jnp.where(allowed, scores, NEGATIVE)
        probs = jnp.where(allowed, jnp.exp(scores - lse_ref[0, :, at]), 0.0)
        grad_probs = dot(v_ref[0], grads, ((1,), (1,)))
        delta = jnp.sum(probs * grad_probs, 0, keepdims=True)
        grad_scores = (probs * (grad_probs - delta)).astype(BF16)
        dv_buf[...] += dot(probs.astype(BF16), grads, ((1,), (0,)))
        dk_buf[...] += dot(grad_scores, queries, ((1,), (0,)))
        dq_buf[at, :] = dot(grad_scores, k_ref[0], ((0,), (0,)))
        return carry

    lax.fori_loop(0, total // QUERY_BLOCK, one, 0)
    for c in range(cores):
        for i in range(chips):
            at = pl.ds((c * chips + i) * length, length)
            cosine, sine = cos_buf[at, :], sin_buf[at, :]
            out_ref[c, 0, i, 0, :, :HEAD_DIM] = turn_pairs(dq_buf[at, :] * scaling, cosine, -sine).astype(BF16)
            out_ref[c, 0, i, 0, :, HEAD_DIM : 2 * HEAD_DIM] = turn_pairs(dk_buf[at, :] * scaling, cosine, -sine).astype(BF16)
            out_ref[c, 0, i, 0, :, 2 * HEAD_DIM :] = dv_buf[at, :].astype(BF16)


def make_body(lay):
    sub, seq, group, chips_x = lay.sub, lay.seq, lay.group, lay.chips_x

    square = lay.square

    def across(value, o):
        return lax.ppermute(value, GROUP, lay.shift(*o))

    def add(*pieces):
        total = pieces[0].astype(F32)
        for piece in pieces[1:]:
            total = total + piece.astype(F32)
        return total

    def far_first(pieces):
        if square:
            return [
                [across(pieces[2][0], (1, 0)), across(pieces[3][0], (1, 0))],
                [across(pieces[1][1], (0, 1)), across(pieces[3][1], (0, 1))],
            ]
        batch = len(pieces[0])
        return [
            [across(pieces[i][m], ((-o[0]) % sub, (-o[1]) % chips_x)) for i, o in enumerate(lay.offsets) if i]
            for m in range(batch)
        ]

    def far_onward(pieces, came):
        if square:
            return [add(pieces[1][0], came[0][1]).astype(BF16), add(pieces[2][1], came[1][1]).astype(BF16)]
        return []

    def far_second(pieces, came, onward):
        if square:
            last = [across(onward[0], (0, 1)), across(onward[1], (1, 0))]
            return [[pieces[0][m], came[m][0], last[m]] for m in range(2)]
        return [[pieces[0][m], *came[m]] for m in range(len(came))]

    def add_all(parts):
        return jnp.stack([add(*pieces) for pieces in parts])

    def after(value, *tokens):
        return lax.optimization_barrier((value, *tokens))[0]

    def step(
        tokens, positions, cotangent, gain1, bias1, gain2, bias2,
        w_qkv, b_qkv, w_out, b_out, w_up, b_up, w_down, b_down,
    ):
        batch, length, width = tokens.shape
        rows = w_qkv.shape[0]
        ff = w_up.shape[1]
        count = seq * length
        total = group * batch * length
        my_seq = lax.axis_index("seq")
        me = lax.axis_index("yi") * seq + my_seq
        scaling = HEAD_DIM ** (-0.5)
        cols = lay.heads * HEAD_DIM
        ff_cols = ff // group
        out_cols = width // group
        plans = {"up": (1, rows, ff_cols), "down": (1, rows, ff_cols), "qkv": (3, rows, cols), "out": (1, rows, out_cols)}

        def gather_rows(mine):
            return lax.all_gather(mine, "zo", axis=0, tiled=True)

        x, core = my_seq // 2, my_seq % 2
        places = []
        for ry in range(sub):
            from_there = positions
            if ry:
                from_there = lax.ppermute(positions, "yi", [(i, (i + ry) % sub) for i in range(sub)])
            blocks = from_there.reshape(batch, seq, length)
            order = [((x - rx) % chips_x) * 2 + (core + rc) % 2 for rc in range(2) for rx in range(chips_x)]
            places.append(jnp.concatenate([lax.dynamic_slice_in_dim(blocks, o, 1, 1) for o in order], 1))
        places = jnp.stack(places).reshape(sub * batch, count)

        def laid(values):
            size = -(-sum(v.size for v in values) // 1024) * 1024
            whole, at = 0.0, 0
            for v in values:
                whole = whole + jnp.pad(v.astype(F32), (at, size - at - v.size))
                at += v.size
            return whole.reshape(-1, 128)

        names = (bias1, bias2, gain1, gain2, b_qkv, b_up, b_out, b_down)
        (qkv_own,) = deal_exchange(lay, [plans["qkv"]], [w_qkv], False, 0)
        qkv_w = gather_rows(qkv_own)
        w_up_late, _ = lax.optimization_barrier((w_up, qkv_own))
        (up_own,) = deal_exchange(lay, [plans["up"]], [w_up_late], False, 7)
        up_w = gather_rows(up_own)
        tokens_late, _ = lax.optimization_barrier((tokens, up_own))
        one, two, hat, vectors, out_own, down_own = norm_exchange(
            lay, [plans["out"], plans["down"]], tokens_late, laid(names), [w_out, w_down]
        )
        out_w = gather_rows(out_own)
        down_w = gather_rows(down_own)
        vectors = vectors.reshape(lay.count, -1)
        cuts = []
        at = 0
        for piece in names:
            cuts.append(vectors[:, at : at + piece.shape[0]].reshape(-1))
            at += piece.shape[0]
        _, _, gain1_all, gain2_all, b_qkv_all, b_up_all, b_out_all, b_down_all = cuts
        b_qkv_mine = lax.dynamic_index_in_dim(b_qkv_all.reshape(3, group, cols), me, 1, keepdims=False).reshape(-1)
        b_up_mine = lax.dynamic_index_in_dim(b_up_all.reshape(group, ff_cols), me, 0, keepdims=False)
        one, two, hat = [v.reshape(total, width) for v in (one, two, hat)]
        cotangent, hat, places = lax.optimization_barrier((cotangent, hat, places))
        near_dy = [cotangent] + [across(cotangent, o) for o in lay.near[1:]]

        halves = ROTARY // 2
        frequency = jnp.exp(jnp.arange(halves, dtype=F32) * (-2.0 * math.log(10000.0) / ROTARY))
        phases = places.astype(F32)[:, None, :] * frequency[None, :, None]
        cosine, sine = jnp.cos(phases), jnp.sin(phases)
        place_col = places[:, :, None]
        place_row = places[:, None, :]

        seqs = sub * batch
        one = after(one, cosine, sine)
        packed = dot(one, qkv_w, ((1,), (0,))) + b_qkv_mine
        two = after(two, packed)

        hidden = dot(two, up_w, ((1,), (0,))) + b_up_mine
        phi_cdf = 0.5 * (1.0 + lax.erf(hidden * math.sqrt(0.5)))
        density = jnp.exp(-0.5 * hidden * hidden) * (1.0 / math.sqrt(2.0 * math.pi))
        activated = (hidden * phi_cdf).astype(BF16)
        slope = (phi_cdf + hidden * density).astype(BF16)
        activated, slope = lax.optimization_barrier((activated, slope))
        packed = after(packed, activated)
        wide = (2, 1, chips_x, 1, length, 3 * cols)
        wide_spec = pl.BlockSpec(wide, lambda i: (0, i // batch, 0, i % batch, 0, 0))
        full = (2, sub, chips_x, batch, length, 3 * cols)
        head_spec = pl.BlockSpec((1, count, HEAD_DIM), lambda i: (i, 0, 0))
        turn_spec = pl.BlockSpec((1, ROTARY // 2, count), lambda i: (i, 0, 0))
        tokens_spec = pl.BlockSpec((2, 1, chips_x, 1, length, cols), lambda i: (0, i // batch, 0, i % batch, 0, 0))
        by_token = (2, sub, chips_x, batch, length, cols)
        turn_bufs = [pltpu.VMEM((count, 128), F32)] * 2
        col_spec = pl.BlockSpec((1, count, 1), lambda i: (i, 0, 0))
        row_spec = pl.BlockSpec((1, 1, count), lambda i: (i, 0, 0))
        head_shape = jax.ShapeDtypeStruct((seqs, count, HEAD_DIM), BF16)
        work = 2 * seqs * count * count * HEAD_DIM
        params = pltpu.CompilerParams(vmem_limit_bytes=56 << 20)
        near_count, chips = len(near_dy), group // 2
        queries, keys, values, context, lse, upstream = pl.pallas_call(
            functools.partial(attend_kernel, lay, scaling),
            grid=(seqs,),
            in_specs=[wide_spec, turn_spec, turn_spec, col_spec, row_spec] + [ANY] * near_count,
            out_specs=[head_spec] * 3 + [tokens_spec, row_spec, ANY],
            out_shape=[head_shape] * 3
            + [
                jax.ShapeDtypeStruct(by_token, BF16),
                jax.ShapeDtypeStruct((seqs, 1, count), F32),
                jax.ShapeDtypeStruct((2, chips, *cotangent.shape), BF16),
            ],
            scratch_shapes=[pltpu.VMEM((count, HEAD_DIM), BF16)] * 4
            + turn_bufs
            + [pltpu.VMEM((near_count, *cotangent.shape), BF16)]
            + [pltpu.SemaphoreType.DMA((near_count,))] * 2
            + [pltpu.SemaphoreType.DMA((chips,))] * 2
            + [pltpu.SemaphoreType.DMA((2,))] * 2,
            compiler_params=pltpu.CompilerParams(collective_id=8, has_side_effects=True, vmem_limit_bytes=58 << 20),
            cost_estimate=pl.CostEstimate(flops=2 * work, bytes_accessed=30 << 20, transcendentals=seqs * count * count),
            name="attend",
        )(packed.reshape(full), cosine, sine, place_col, place_row, *near_dy)
        upstream = upstream.reshape(total, width)

        context = context.reshape(total, cols)

        def scatter(grad):
            return lax.psum_scatter(grad, "zo", scatter_dimension=0, tiled=True)

        def outer_dot(left, right):
            return dot(left, right, ((0,), (0,))).astype(BF16)

        def chain(values, *tokens):
            return lax.optimization_barrier((*values, *tokens))[: len(values)]

        def tokens_of(pieces):
            return [pieces[i * batch : (i + 1) * batch] for i in range(group // 2)]

        down_part = outer_dot(upstream, activated)
        upstream, down_part = chain((upstream, down_part))
        down_sum = scatter(down_part)
        grad_context = dot(upstream, out_w, ((1,), (0,))).astype(BF16)

        grad_packed = pl.pallas_call(
            functools.partial(attend_back_kernel, scaling),
            grid=(seqs,),
            in_specs=[head_spec] * 3 + [tokens_spec, turn_spec, turn_spec, col_spec, row_spec, row_spec],
            out_specs=wide_spec,
            out_shape=jax.ShapeDtypeStruct(full, BF16),
            scratch_shapes=[pltpu.VMEM((count, HEAD_DIM), BF16)] + [pltpu.VMEM((count, HEAD_DIM), F32)] * 3 + turn_bufs,
            compiler_params=params,
            cost_estimate=pl.CostEstimate(flops=5 * work, bytes_accessed=24 << 20, transcendentals=seqs * count * count),
            name="attend_back",
        )(queries, keys, values, grad_context.reshape(by_token), cosine, sine, place_col, place_row, lse)
        grad_packed = grad_packed.reshape(total, 3 * cols)

        qkv_part = outer_dot(hat, grad_packed)
        qkv_sum = scatter(qkv_part)
        acts = chain((context, activated), qkv_part)
        out_near = tokens_of(pair_matmul(lay, acts, (out_w, down_w), batch, (0, 1), 4))
        out_came = far_first(out_near)
        (upstream,) = chain((upstream,), out_near)
        out_part = outer_dot(upstream, context)
        out_part, upstream = chain((out_part, upstream))
        grad_hidden = (dot(upstream, down_w, ((1,), (0,))) * slope.astype(F32)).astype(BF16)
        up_part = outer_dot(hat, grad_hidden)
        up_sum = scatter(up_part)
        (out_part,) = chain((out_part,), up_part)
        out_w_sum = scatter(out_part)
        out_came, left = chain((out_came, grad_packed), up_part)
        onward, left = chain((far_onward(out_near, out_came), left))
        out_parts = far_second(out_near, out_came, onward)

        folded = (qkv_w, up_w)
        scales = (gain1_all, gain2_all)
        left, down_sum = chain((left, down_sum))
        *near0, down_raw = pair_matmul(
            lay, (left, grad_hidden), folded, batch, (0, 2), 5, scales, [plans["down"]], [down_sum]
        )
        near0 = tokens_of(near0)
        came0 = far_first(near0)
        own_sums = [
            jnp.sum(grad_packed.astype(F32), 0),
            jnp.sum(grad_hidden.astype(F32), 0),
            jnp.sum(cotangent.astype(F32), (0, 1)),
        ]
        left, vec, qkv_sum = chain((left, laid(own_sums), qkv_sum), near0)
        *near1, qkv_raw, everyone = pair_matmul(
            lay, (left, grad_hidden), folded, batch, (1, 2), 6, scales, [plans["qkv"]], [qkv_sum], vec
        )
        near1 = tokens_of(near1)
        came1 = far_first(near1)
        (came0,) = chain((came0,), near1)
        onward0 = far_onward(near0, came0)
        parts0 = far_second(near0, came0, onward0)
        (out_parts,) = chain((out_parts,), onward0)
        output = (tokens.astype(F32) + add_all(out_parts) + b_out_all + b_down_all).astype(BF16)
        sums = jnp.sum(everyone.reshape(lay.outer, group, -1), 0)
        sum_qkv = jnp.transpose(sums[:, : 3 * cols].reshape(group, 3, cols), (1, 0, 2)).reshape(-1)
        sum_up = sums[:, 3 * cols : 3 * cols + ff_cols].reshape(-1)
        sum_dy = jnp.sum(sums[:, 3 * cols + ff_cols : 3 * cols + ff_cols + width], 0)
        rank = lax.axis_index("zo") * group + me

        def own_part(vector):
            return lax.dynamic_index_in_dim(vector.reshape(lay.count, -1), rank, 0, keepdims=False)

        column = lambda v: v.astype(F32)[:, None]
        qkv_raw = qkv_raw.astype(F32)
        bias_grads = (own_part(sum_qkv), own_part(sum_up), own_part(sum_dy))
        qkv_grads = (
            jnp.sum(w_qkv.astype(F32) * qkv_raw, 1),
            jnp.sum(w_qkv.astype(F32) * sum_qkv, 1),
            column(gain1) * qkv_raw + column(bias1) * sum_qkv,
        )
        down_grad = down_raw.astype(F32)
        came1, *early = chain((came1, output, down_grad, *bias_grads, *qkv_grads))
        output, down_grad, bias_grads, qkv_grads = early[0], early[1], early[2:5], early[5:8]
        onward1 = far_onward(near1, came1)
        parts1 = far_second(near1, came1, onward1)

        inputs = tokens.astype(F32)
        center = inputs - jnp.mean(inputs, -1, keepdims=True)
        inv_std = lax.rsqrt(jnp.mean(center * center, -1, keepdims=True) + EPSILON)
        normal = center * inv_std
        grad_normal = jnp.concatenate([add_all(parts0), add_all(parts1)], -1)
        token_grad = cotangent.astype(F32) + inv_std * (
            grad_normal
            - jnp.mean(grad_normal, -1, keepdims=True)
            - normal * jnp.mean(grad_normal * normal, -1, keepdims=True)
        )

        up_sum, token_grad = chain((up_sum, token_grad))
        (up_raw,) = deal_exchange(lay, [plans["up"]], [up_sum], True, 3)
        up_raw = up_raw.astype(F32)
        up_grads = (
            jnp.sum(w_up.astype(F32) * up_raw, 1),
            jnp.sum(w_up.astype(F32) * sum_up, 1),
            column(gain2) * up_raw + column(bias2) * sum_up,
        )
        out_w_sum, *up_grads = chain((out_w_sum, *up_grads))
        (out_raw,) = deal_exchange(lay, [plans["out"]], [out_w_sum], True, 2)
        return (
            output,
            token_grad,
            qkv_grads[0],
            qkv_grads[1],
            up_grads[0],
            up_grads[1],
            qkv_grads[2],
            bias_grads[0],
            out_raw.astype(F32),
            bias_grads[2],
            up_grads[2],
            bias_grads[1],
            down_grad,
            bias_grads[2],
        )

    return step


def solution(mesh):
    outer, sub, seq = split_axes(mesh)
    inner = Mesh(mesh.devices.reshape(outer, sub, seq), ALL)
    act = P(None, ALL, None)
    vec = P(ALL)
    mat = P(ALL, None)
    return jax.shard_map(
        make_body(Layout(outer, sub, seq)),
        mesh=inner,
        in_specs=(
            act, P(None, ("zo", "yi")), act, vec, vec, vec, vec,
            mat, vec, mat, vec, mat, vec, mat, vec,
        ),
        out_specs=(act, act, vec, vec, vec, vec, mat, vec, mat, vec, mat, vec, mat, vec),
        check_vma=False,
    )
```

```python
import functools
import math

import jax
import jax.numpy as jnp
from jax import lax
from jax.experimental import pallas as pl
from jax.experimental.pallas import tpu as pltpu
from jax.sharding import Mesh, PartitionSpec as P


HEADS = 8
HEAD_DIM = 256
ROTARY = 64
EPSILON = 1e-05
NEGATIVE = -1e30
F32 = jnp.float32
BF16 = jnp.bfloat16
ALL = ("zo", "yi", "seq")
GROUP = ("yi", "seq")
MESH = pl.DeviceIdType.MESH
ANY = pl.BlockSpec(memory_space=pl.ANY)


def dot(left, right, dims):
    return lax.dot_general(left, right, (dims, ((), ())), preferred_element_type=F32)


def split_axes(mesh):
    dp, seq = mesh.shape["dp"], mesh.shape["seq"]
    sub = 1
    while seq * sub * 2 <= HEADS and dp % (sub * 2) == 0:
        sub *= 2
    return dp // sub, sub, seq


def remote(source, target, send, recv, device):
    return pltpu.make_async_remote_copy(
        src_ref=source, dst_ref=target, send_sem=send, recv_sem=recv,
        device_id=device, device_id_type=MESH,
    )


class Layout:
    def __init__(self, outer, sub, seq):
        self.outer, self.sub, self.seq = outer, sub, seq
        self.chips_x = seq // 2
        self.group = sub * seq
        self.count = outer * self.group
        self.heads = HEADS // self.group
        self.offsets = [(ry, rx) for ry in range(sub) for rx in range(self.chips_x)]
        self.square = sub == 2 and self.chips_x == 2
        self.near = [o for o in self.offsets if not (self.square and o == (1, 1))]
        self.far = sorted(self.offsets[1:], key=lambda o: (o[0] > 0) + (o[1] > 0))

    def shift(self, ry, rx):
        pairs = []
        for y in range(self.sub):
            for x in range(self.chips_x):
                for c in range(2):
                    there = ((y + ry) % self.sub, (x + rx) % self.chips_x)
                    pairs.append((y * self.seq + x * 2 + c, there[0] * self.seq + there[1] * 2 + c))
        return pairs

    def flip(self):
        return [(i, i ^ 1) for i in range(self.seq)]


def swap_copies(lay, plan, me, sources, targets, send, recv, back):
    zo = lax.axis_index("zo")
    copies = []
    for k in range(1, lay.group):
        peer = lax.rem(me + k, lay.group)
        device = (zo, peer // lay.seq, lax.rem(peer, lay.seq))
        j = 0
        for (parts, rows, cols), source, target in zip(plan, sources, targets, strict=True):
            for part in range(parts):
                wide = lambda who: pl.ds(pl.multiple_of((part * lay.group + who) * cols, 128), cols)
                thin = pl.ds(part * cols, cols)
                block = lambda who: pl.ds(pl.multiple_of(who * rows, rows), rows)
                if back:
                    copies.append(remote(source.at[block(peer), thin], target.at[:, wide(me)], send.at[k - 1, j], recv.at[k - 1, j], device))
                else:
                    copies.append(remote(source.at[:, wide(peer)], target.at[block(me), thin], send.at[k - 1, j], recv.at[k - 1, j], device))
                j += 1
    return copies


def swap_own(lay, plan, me, sources, targets, sems, back):
    copies = []
    j = 0
    for (parts, rows, cols), source, target in zip(plan, sources, targets, strict=True):
        for part in range(parts):
            wide = pl.ds(pl.multiple_of((part * lay.group + me) * cols, 128), cols)
            thin = pl.ds(part * cols, cols)
            block = pl.ds(pl.multiple_of(me * rows, rows), rows)
            if back:
                copies.append(pltpu.make_async_copy(source.at[block, thin], target.at[:, wide], sems.at[j]))
            else:
                copies.append(pltpu.make_async_copy(source.at[:, wide], target.at[block, thin], sems.at[j]))
            j += 1
    return copies


def group_barrier(lay, me):
    zo = lax.axis_index("zo")
    barrier = pltpu.get_barrier_semaphore()
    for k in range(1, lay.group):
        peer = lax.rem(me + k, lay.group)
        pl.semaphore_signal(
            barrier, inc=1, device_id=(zo, peer // lay.seq, lax.rem(peer, lay.seq)), device_id_type=MESH
        )
    pl.semaphore_wait(barrier, lay.group - 1)


def swap_shapes(lay, plan, back):
    if back:
        return [jax.ShapeDtypeStruct((rows, parts * lay.group * cols), BF16) for parts, rows, cols in plan]
    return [jax.ShapeDtypeStruct((lay.group * rows, parts * cols), BF16) for parts, rows, cols in plan]


def device_after(lay, rank, k):
    peer = lax.rem(rank + k, lay.count)
    inner = lax.rem(peer, lay.group)
    return (peer // lay.group, inner // lay.seq, lax.rem(inner, lay.seq))


def barrier_all(lay, device_of):
    barrier = pltpu.get_barrier_semaphore()

    def greet(k, carry):
        pl.semaphore_signal(barrier, inc=1, device_id=device_of(k), device_id_type=MESH)
        return carry

    lax.fori_loop(1, lay.count, greet, 0)
    pl.semaphore_wait(barrier, lay.count - 1)


def busy(microseconds):
    return pl.CostEstimate(flops=int(7e8 * microseconds), bytes_accessed=1 << 20, transcendentals=0)


def norm_kernel(lay, plan, *refs):
    n = len(plan)
    x_ref, vec_ref, sources = refs[0], refs[1], refs[2 : 2 + n]
    one_ref, two_ref, hat_ref, all_ref, targets = *refs[2 + n : 6 + n], refs[6 + n : 6 + 2 * n]
    (held, stage, vectors, gain_buf, send, recv, core_send, core_recv, w_send, w_recv, w_own, own_sem, out_sem,
     vec_send, vec_recv, vec_own) = refs[6 + 2 * n :]
    batch, length, width = x_ref.shape
    zo, yi, s = lax.axis_index("zo"), lax.axis_index("yi"), lax.axis_index("seq")
    me = yi * lay.seq + s
    x, core = s // 2, lax.rem(s, 2)
    partner = (zo, yi, x * 2 + 1 - core)

    def chip(ry, rx):
        return (zo, lax.rem(yi + ry, lay.sub), lax.rem(x + rx, lay.chips_x) * 2 + core)

    rank = zo * lay.group + me
    device_of = functools.partial(device_after, lay, rank)
    barrier_all(lay, device_of)

    def vec_copy(k):
        return remote(vec_ref, vectors.at[rank], vec_send.at[k - 1], vec_recv.at[k - 1], device_of(k))

    def vec_start(k, carry):
        vec_copy(k).start()
        return carry

    def vec_finish(k, carry):
        vec_copy(k).wait()
        return carry

    lax.fori_loop(1, lay.count, vec_start, 0)
    vec_mine = pltpu.make_async_copy(vec_ref, vectors.at[rank], vec_own.at[0])
    vec_mine.start()
    slot = {offset: i for i, offset in enumerate(lay.offsets)}
    own_copy = pltpu.make_async_copy(x_ref, held.at[0, 0], own_sem)
    own_copy.start()
    straight = [o for o in lay.far if not (o[0] and o[1])]
    diagonal = [o for o in lay.far if o[0] and o[1]]
    copies = {}
    for o in straight:
        copies[o] = [remote(x_ref, held.at[0, slot[o]], send.at[slot[o], 0], recv.at[slot[o], 0], chip(*o))]
    half = batch // 2
    for ry, rx in diagonal:
        j = slot[(ry, rx)]
        copies[(ry, rx)] = [
            remote(held.at[0, slot[(0, rx)], :half], held.at[0, j, :half], send.at[j, 0], recv.at[j, 0], chip(ry, 0)),
            remote(held.at[0, slot[(ry, 0)], half:], held.at[0, j, half:], send.at[j, 1], recv.at[j, 1], chip(0, rx)),
        ]
    to_partner = {
        o: remote(x_ref if o == (0, 0) else held.at[0, slot[o]], held.at[1, slot[o]],
                  core_send.at[slot[o]], core_recv.at[slot[o]], partner)
        for o in lay.offsets
    }
    for o in straight:
        copies[o][0].start()
    to_partner[(0, 0)].start()
    swaps = swap_copies(lay, plan, me, sources, targets, w_send, w_recv, False)
    swaps += swap_own(lay, plan, me, sources, targets, w_own, False)
    lax.fori_loop(1, lay.count, vec_finish, 0)
    vec_mine.wait()
    vec_out = pltpu.make_async_copy(vectors, all_ref, vec_own.at[1])
    vec_out.start()
    size = width // lay.count
    lane = lax.broadcasted_iota(jnp.int32, (1, 128), 1)
    for v in range(4):
        row, low = (v * size) // 128, (v * size) % 128
        for k in range(width // 128):
            line = None
            for j in range(128 // size):
                piece = vectors[k * (128 // size) + j, row : row + 1, :]
                turn = (j * size - low) % 128
                piece = pltpu.roll(piece, turn, 1) if turn else piece
                line = piece if line is None else jnp.where(lane >= j * size, piece, line)
            gain_buf[v : v + 1, k * 128 : (k + 1) * 128] = line
    gains = [gain_buf[i : i + 1, :] for i in range(4)]
    rows = 16
    pending = [[], []]
    turn = [0]

    def norm(c, j):
        for m in range(batch):
            k = turn[0] % 2
            turn[0] += 1
            for copy in pending[k]:
                copy.wait()

            def chunk(i, carry):
                at = pl.ds(pl.multiple_of(i * rows, rows), rows)
                value = held[c, j, m, at, :].astype(F32)
                center = value - jnp.mean(value, -1, keepdims=True)
                hat = center * lax.rsqrt(jnp.mean(center * center, -1, keepdims=True) + EPSILON)
                stage[k, 0, at, :] = (hat * gains[2] + gains[0]).astype(BF16)
                stage[k, 1, at, :] = (hat * gains[3] + gains[1]).astype(BF16)
                stage[k, 2, at, :] = hat.astype(BF16)
                return carry

            lax.fori_loop(0, length // rows, chunk, 0, unroll=2)
            pending[k] = [
                pltpu.make_async_copy(stage.at[k, i], ref.at[c, j, m], out_sem.at[k, i])
                for i, ref in enumerate((one_ref, two_ref, hat_ref))
            ]
            for copy in pending[k]:
                copy.start()

    own_copy.wait()
    norm(0, 0)
    to_partner[(0, 0)].wait_recv()
    norm(1, 0)
    for o in straight:
        copies[o][0].wait_recv()
        to_partner[o].start()
        for ry, rx in diagonal:
            if o == (0, rx):
                copies[(ry, rx)][0].start()
            if o == (ry, 0):
                copies[(ry, rx)][1].start()
        if o == straight[-1]:
            for copy in swaps:
                copy.start()
        norm(0, slot[o])
    for o in straight:
        to_partner[o].wait_recv()
        norm(1, slot[o])
    for o in diagonal:
        for copy in copies[o]:
            copy.wait_recv()
        to_partner[o].start()
        norm(0, slot[o])
    for o in diagonal:
        to_partner[o].wait_recv()
        norm(1, slot[o])
    for side in pending:
        for copy in side:
            copy.wait()
    for o in lay.far:
        for copy in copies[o]:
            copy.wait_send()
    for o in lay.offsets:
        to_partner[o].wait_send()
    for copy in swaps:
        copy.wait()
    vec_out.wait()


def norm_exchange(lay, plan, tokens, vec, weights):
    count = sum(parts for parts, _, _ in plan)
    chips = lay.group // 2
    whole = jax.ShapeDtypeStruct((2, chips, *tokens.shape), BF16)
    return pl.pallas_call(
        functools.partial(norm_kernel, lay, plan),
        out_shape=[whole] * 3 + [jax.ShapeDtypeStruct((lay.count, *vec.shape), F32)] + swap_shapes(lay, plan, False),
        in_specs=[ANY] * (2 + len(plan)),
        out_specs=[ANY] * (4 + len(plan)),
        scratch_shapes=[
            pltpu.VMEM((2, chips, *tokens.shape), BF16),
            pltpu.VMEM((2, 3, *tokens.shape[1:]), BF16),
            pltpu.VMEM((lay.count, *vec.shape), F32),
            pltpu.VMEM((4, tokens.shape[2]), F32),
            pltpu.SemaphoreType.DMA((chips, 2)),
            pltpu.SemaphoreType.DMA((chips, 2)),
            pltpu.SemaphoreType.DMA((chips,)),
            pltpu.SemaphoreType.DMA((chips,)),
            pltpu.SemaphoreType.DMA((lay.group - 1, count)),
            pltpu.SemaphoreType.DMA((lay.group - 1, count)),
            pltpu.SemaphoreType.DMA((count,)),
            pltpu.SemaphoreType.DMA,
            pltpu.SemaphoreType.DMA((2, 3)),
            pltpu.SemaphoreType.DMA((lay.count - 1,)),
            pltpu.SemaphoreType.DMA((lay.count - 1,)),
            pltpu.SemaphoreType.DMA((2,)),
        ],
        compiler_params=pltpu.CompilerParams(
            collective_id=1, has_side_effects=True, vmem_limit_bytes=48 << 20
        ),
        cost_estimate=busy(100),
        name="norm_exchange",
    )(tokens, vec, *weights)


def deal_kernel(lay, plan, back, *refs):
    n = len(plan)
    sources, targets = refs[:n], refs[n : 2 * n]
    send, recv, own = refs[2 * n :]
    me = lax.axis_index("yi") * lay.seq + lax.axis_index("seq")
    group_barrier(lay, me)
    copies = swap_copies(lay, plan, me, sources, targets, send, recv, back)
    copies += swap_own(lay, plan, me, sources, targets, own, back)
    for copy in copies:
        copy.start()
    for copy in copies:
        copy.wait()


def deal_exchange(lay, plan, arrays, back, number):
    count = sum(parts for parts, _, _ in plan)
    return pl.pallas_call(
        functools.partial(deal_kernel, lay, plan, back),
        out_shape=swap_shapes(lay, plan, back),
        in_specs=[ANY] * len(plan),
        out_specs=[ANY] * len(plan),
        scratch_shapes=[
            pltpu.SemaphoreType.DMA((lay.group - 1, count)),
            pltpu.SemaphoreType.DMA((lay.group - 1, count)),
            pltpu.SemaphoreType.DMA((count,)),
        ],
        compiler_params=pltpu.CompilerParams(collective_id=number, has_side_effects=True),
        cost_estimate=busy(17),
    )(*arrays)


def pair_kernel(lay, plan, with_vec, scaled, batch, *refs):
    refs = list(refs)
    take = lambda k: [refs.pop(0) for _ in range(k)]
    step = pl.program_id(0)
    chips = lay.group // 2
    first_ref, first_w, second_ref, second_w = take(4)
    scales = take(2) if scaled else []
    sources, vec_ref = take(len(plan)), take(int(with_vec))
    outs, targets, all_ref = take(chips * batch), take(len(plan)), take(int(with_vec))
    given, came, send, recv, out_sem = take(5)
    zo, yi, s = lax.axis_index("zo"), lax.axis_index("yi"), lax.axis_index("seq")
    me = yi * lay.seq + s
    rank = zo * lay.group + me
    device_of = functools.partial(device_after, lay, rank)
    partner = (zo, yi, (s // 2) * 2 + 1 - lax.rem(s, 2))
    swap_sems = take(3) if plan else []
    vec_sems = take(3) if with_vec else []

    def copy(j):
        return remote(given.at[j], came.at[j], send.at[j], recv.at[j], partner)

    def stores(j):
        length = came.shape[1] // batch
        return [
            pltpu.make_async_copy(
                came.at[j, pl.ds(m * length, length)], outs[(j + 1) % chips * batch + m], out_sem.at[j, m]
            )
            for m in range(batch)
        ]

    def riders():
        if not plan:
            return []
        copies = swap_copies(lay, plan, me, sources, targets, swap_sems[0], swap_sems[1], True)
        return copies + swap_own(lay, plan, me, sources, targets, swap_sems[2], True)

    def vec_copy(k):
        return remote(vec_ref[0], all_ref[0].at[rank], vec_sems[0].at[k - 1], vec_sems[1].at[k - 1], device_of(k))

    def vec_start(k, carry):
        vec_copy(k).start()
        return carry

    def vec_finish(k, carry):
        vec_copy(k).wait()
        return carry

    def vec_mine():
        return pltpu.make_async_copy(vec_ref[0], all_ref[0].at[rank], vec_sems[2])

    @pl.when(step == 0)
    def _():
        if with_vec:
            barrier_all(lay, device_of)
            vec_mine().start()
            lax.fori_loop(1, lay.count, vec_start, 0)
        elif plan:
            group_barrier(lay, me)
        else:
            barrier = pltpu.get_barrier_semaphore()
            pl.semaphore_signal(barrier, inc=1, device_id=partner, device_id_type=MESH)
            pl.semaphore_wait(barrier, 1)
        for rider in riders():
            rider.start()

    for j in range(chips):

        @pl.when(step == j + 1)
        def _():
            copy(j).start()

    total = dot(first_ref[0, 0], first_w[...], ((1,), (1,)))
    other = dot(second_ref[0, 0], second_w[...], ((1,), (1,)))
    total = total * scales[0][...] + other * scales[1][...] if scaled else total + other
    for j in range(chips):

        @pl.when(step == j)
        def _():
            given[j] = total.astype(BF16)

        @pl.when(step == chips + j)
        def _():
            copy(j).wait_recv()
            came[j] = (total + came[j].astype(F32)).astype(BF16)

    for j in range(chips - 1):

        @pl.when(step == chips + j + 1)
        def _():
            for piece in stores(j):
                piece.start()

    @pl.when(step == 2 * chips - 1)
    def _():
        for piece in stores(chips - 1):
            piece.start()
        for j in range(chips):
            copy(j).wait_send()
            for piece in stores(j):
                piece.wait()
        for rider in riders():
            rider.wait()
        if with_vec:
            vec_mine().wait()
            lax.fori_loop(1, lay.count, vec_finish, 0)


def pair_matmul(lay, acts, weights, batch, cut, number, scales=(), plan=(), arrays=(), vec=None):
    chips = lay.group // 2
    rows = acts[0].shape[0] // lay.group
    width = weights[0].shape[0] // cut[1]
    count = sum(parts for parts, _, _ in plan)
    with_vec = vec is not None

    def act(depth):
        return pl.BlockSpec((1, 1, rows, depth), lambda i: (1 - i // chips, (i + 1) % chips, 0, 0))

    def weight(depth):
        return pl.BlockSpec((width, depth), lambda i: (cut[0], 0), pipeline_mode=pl.Buffered(1))

    specs, args = [], []
    for a, w in zip(acts, weights, strict=True):
        specs += [act(a.shape[1]), weight(a.shape[1])]
        args += [a.reshape(2, chips, rows, a.shape[1]), w]
    for scale in scales:
        specs.append(pl.BlockSpec((1, width), lambda i: (0, cut[0])))
        args.append(scale.reshape(1, -1))
    args += [*arrays, *([vec] if with_vec else [])]
    specs += [ANY] * (len(args) - len(specs))
    shapes = [jax.ShapeDtypeStruct((rows // batch, width), BF16)] * (chips * batch) + swap_shapes(lay, plan, True)
    scratch = [
        pltpu.VMEM((chips, rows, width), BF16),
        pltpu.VMEM((chips, rows, width), BF16),
        pltpu.SemaphoreType.DMA((chips,)),
        pltpu.SemaphoreType.DMA((chips,)),
        pltpu.SemaphoreType.DMA((chips, batch)),
    ]
    if plan:
        scratch += [pltpu.SemaphoreType.DMA((lay.group - 1, count))] * 2 + [pltpu.SemaphoreType.DMA((count,))]
    if with_vec:
        shapes.append(jax.ShapeDtypeStruct((lay.count, *vec.shape), vec.dtype))
        scratch += [pltpu.SemaphoreType.DMA((lay.count - 1,))] * 2 + [pltpu.SemaphoreType.DMA]
    depth = sum(a.shape[1] for a in acts)
    return pl.pallas_call(
        functools.partial(pair_kernel, lay, plan, with_vec, bool(scales), batch),
        grid=(2 * chips,),
        in_specs=specs,
        out_specs=[ANY] * len(shapes),
        out_shape=shapes,
        scratch_shapes=scratch,
        compiler_params=pltpu.CompilerParams(
            collective_id=number, has_side_effects=True, vmem_limit_bytes=60 << 20
        ),
        cost_estimate=pl.CostEstimate(
            flops=2 * acts[0].shape[0] * depth * width, bytes_accessed=32 << 20, transcendentals=0
        ),
    )(*args)


def turn_pairs(field, cosine, sine):
    halves = ROTARY // 2
    front = field[:, :128]
    lane = lax.broadcasted_iota(jnp.int32, front.shape, 1)
    other = jnp.where(lane < halves, pltpu.roll(front, 128 - halves, 1), pltpu.roll(front, halves, 1))
    return jnp.concatenate([front * cosine + other * sine, field[:, 128:]], -1)


QUERY_BLOCK = 256


def wide_angles(ref):
    part = ref[0]
    return jnp.transpose(jnp.concatenate([part, part, part, part], 0), (1, 0))


def wide_pair(cos_ref, sin_ref):
    cosine, sine = wide_angles(cos_ref), wide_angles(sin_ref)
    lane = lax.broadcasted_iota(jnp.int32, cosine.shape, 1)
    cosine = jnp.where(lane < ROTARY, cosine, 1.0)
    sine = jnp.where(lane < ROTARY // 2, -sine, jnp.where(lane < ROTARY, sine, 0.0))
    return cosine, sine


def attend_kernel(lay, scaling, *refs):
    refs = list(refs)
    take = lambda k: [refs.pop(0) for _ in range(k)]
    near_count = len(lay.near)
    packed_ref, cos_ref, sin_ref, col_ref, row_ref = take(5)
    near = take(near_count)
    q_ref, k_ref, v_ref, ctx_ref, lse_ref, dy_ref = take(6)
    q_buf, k_buf, v_buf, ctx_buf, cos_buf, sin_buf, bounce = take(7)
    load_sem, store_sem, core_send, core_recv, on_send, on_recv = take(6)
    step, last = pl.program_id(0), pl.num_programs(0) - 1
    zo, yi, s = lax.axis_index("zo"), lax.axis_index("yi"), lax.axis_index("seq")
    x, core = s // 2, lax.rem(s, 2)
    partner = (zo, yi, x * 2 + 1 - core)
    chips = lay.group // 2
    half = near[0].shape[0] // 2

    def load(i):
        return pltpu.make_async_copy(near[i], bounce.at[i], load_sem.at[i])

    def store(i):
        return pltpu.make_async_copy(bounce.at[i], dy_ref.at[0, i], store_sem.at[i])

    def to_partner(i):
        source = near[i] if i < near_count else dy_ref.at[0, i]
        return remote(source, dy_ref.at[1, i], core_send.at[i], core_recv.at[i], partner)

    def onward():
        if not lay.square:
            return []
        over_y = (zo, lax.rem(yi + 1, lay.sub), s)
        over_x = (zo, yi, lax.rem(x + 1, lay.chips_x) * 2 + core)
        return [
            remote(near[1].at[:half], dy_ref.at[0, 3, :half], on_send.at[0], on_recv.at[0], over_y),
            remote(near[2].at[half:], dy_ref.at[0, 3, half:], on_send.at[1], on_recv.at[1], over_x),
        ]

    @pl.when(step == 0)
    def _():
        group_barrier(lay, yi * lay.seq + s)
        for copy in onward():
            copy.start()
        for i in range(near_count):
            load(i).start()
            to_partner(i).start()

    @pl.when(step == 1)
    def _():
        for i in range(near_count):
            load(i).wait()
            store(i).start()

    attend_one(scaling, packed_ref, cos_ref, sin_ref, col_ref, row_ref, q_ref, k_ref, v_ref, ctx_ref, lse_ref,
               q_buf, k_buf, v_buf, ctx_buf, cos_buf, sin_buf)

    @pl.when(step == last)
    def _():
        for copy in onward():
            copy.wait_recv()
        for i in range(near_count, chips):
            to_partner(i).start()
        for i in range(near_count):
            store(i).wait()
        for i in range(chips):
            to_partner(i).wait()
        for copy in onward():
            copy.wait_send()


def attend_one(scaling, packed_ref, cos_ref, sin_ref, col_ref, row_ref, q_ref, k_ref, v_ref, ctx_ref, lse_ref,
               q_buf, k_buf, v_buf, ctx_buf, cos_buf, sin_buf):
    cores, _, chips, _, length, _ = packed_ref.shape
    cos_all, sin_all = wide_pair(cos_ref, sin_ref)
    cos_buf[...] = cos_all
    sin_buf[...] = sin_all
    for c in range(cores):
        for i in range(chips):
            at = pl.ds((c * chips + i) * length, length)
            block = packed_ref[c, 0, i, 0]
            cosine, sine = cos_buf[at, :], sin_buf[at, :]
            q_buf[at, :] = turn_pairs(block[:, :HEAD_DIM], cosine, sine).astype(BF16)
            k_buf[at, :] = turn_pairs(block[:, HEAD_DIM : 2 * HEAD_DIM], cosine, sine).astype(BF16)
            v_buf[at, :] = block[:, 2 * HEAD_DIM :].astype(BF16)
    q_ref[0] = q_buf[...]
    k_ref[0] = k_buf[...]
    v_ref[0] = v_buf[...]
    total = cores * chips * length

    def one(j, carry):
        at = pl.ds(pl.multiple_of(j * QUERY_BLOCK, QUERY_BLOCK), QUERY_BLOCK)
        scores = dot(k_buf[...], q_buf[at, :], ((1,), (1,))) * scaling
        allowed = col_ref[0] <= row_ref[0, :, at]
        scores = jnp.where(allowed, scores, NEGATIVE)
        top = jnp.max(scores, 0, keepdims=True)
        weights = jnp.where(allowed, jnp.exp(scores - top), 0.0)
        total_row = jnp.sum(weights, 0, keepdims=True)
        probs = (weights * (1.0 / total_row)).astype(BF16)
        ctx_buf[at, :] = dot(probs, v_buf[...], ((0,), (0,))).astype(BF16)
        lse_ref[0, :, at] = top + jnp.log(total_row)
        return carry

    lax.fori_loop(0, total // QUERY_BLOCK, one, 0)
    for c in range(cores):
        for i in range(chips):
            ctx_ref[c, 0, i, 0] = ctx_buf[pl.ds((c * chips + i) * length, length), :]


def attend_back_kernel(scaling, q_ref, k_ref, v_ref, g_ref, cos_ref, sin_ref, col_ref, row_ref, lse_ref, out_ref, sum_ref,
                       g_buf, dq_buf, dk_buf, dv_buf, cos_buf, sin_buf):
    cores, _, chips, _, length, _ = out_ref.shape
    total = q_ref.shape[1]
    cos_all, sin_all = wide_pair(cos_ref, sin_ref)
    cos_buf[...] = cos_all
    sin_buf[...] = sin_all
    for c in range(cores):
        for i in range(chips):
            g_buf[pl.ds((c * chips + i) * length, length), :] = g_ref[c, 0, i, 0]
    dk_buf[...] = jnp.zeros_like(dk_buf)
    dv_buf[...] = jnp.zeros_like(dv_buf)

    def one(j, carry):
        at = pl.ds(pl.multiple_of(j * QUERY_BLOCK, QUERY_BLOCK), QUERY_BLOCK)
        queries = q_ref[0, at, :]
        grads = g_buf[at, :]
        scores = dot(k_ref[0], queries, ((1,), (1,))) * scaling
        allowed = col_ref[0] <= row_ref[0, :, at]
        scores = jnp.where(allowed, scores, NEGATIVE)
        probs = jnp.where(allowed, jnp.exp(scores - lse_ref[0, :, at]), 0.0)
        grad_probs = dot(v_ref[0], grads, ((1,), (1,)))
        delta = jnp.sum(probs * grad_probs, 0, keepdims=True)
        grad_scores = (probs * (grad_probs - delta)).astype(BF16)
        dv_buf[...] += dot(probs.astype(BF16), grads, ((1,), (0,)))
        dk_buf[...] += dot(grad_scores, queries, ((1,), (0,)))
        dq_buf[at, :] = dot(grad_scores, k_ref[0], ((0,), (0,)))
        return carry

    lax.fori_loop(0, total // QUERY_BLOCK, one, 0)
    for c in range(cores):
        for i in range(chips):
            at = pl.ds((c * chips + i) * length, length)
            cosine, sine = cos_buf[at, :], sin_buf[at, :]
            pieces = (
                turn_pairs(dq_buf[at, :] * scaling, cosine, -sine),
                turn_pairs(dk_buf[at, :] * scaling, cosine, -sine),
                dv_buf[at, :],
            )
            for k, piece in enumerate(pieces):
                columns = slice(k * HEAD_DIM, (k + 1) * HEAD_DIM)
                low = piece.astype(BF16)
                out_ref[c, 0, i, 0, :, columns] = low
                part = jnp.sum(low.astype(F32), 0, keepdims=True)
                sum_ref[0, :, columns] = part if c + i == 0 else sum_ref[0, :, columns] + part


def make_body(lay):
    sub, seq, group, chips_x = lay.sub, lay.seq, lay.group, lay.chips_x

    square = lay.square

    def across(value, o):
        return lax.ppermute(value, GROUP, lay.shift(*o))

    def add(*pieces):
        total = pieces[0].astype(F32)
        for piece in pieces[1:]:
            total = total + piece.astype(F32)
        return total

    def far_first(pieces):
        if square:
            return [
                [across(pieces[2][0], (1, 0)), across(pieces[3][0], (1, 0))],
                [across(pieces[1][1], (0, 1)), across(pieces[3][1], (0, 1))],
            ]
        batch = len(pieces[0])
        return [
            [across(pieces[i][m], ((-o[0]) % sub, (-o[1]) % chips_x)) for i, o in enumerate(lay.offsets) if i]
            for m in range(batch)
        ]

    def far_onward(pieces, came):
        if square:
            return [add(pieces[1][0], came[0][1]).astype(BF16), add(pieces[2][1], came[1][1]).astype(BF16)]
        return []

    def far_second(pieces, came, onward):
        if square:
            last = [across(onward[0], (0, 1)), across(onward[1], (1, 0))]
            return [[pieces[0][m], came[m][0], last[m]] for m in range(2)]
        return [[pieces[0][m], *came[m]] for m in range(len(came))]

    def add_all(parts):
        return jnp.stack([add(*pieces) for pieces in parts])

    def after(value, *tokens):
        return lax.optimization_barrier((value, *tokens))[0]

    def step(
        tokens, positions, cotangent, gain1, bias1, gain2, bias2,
        w_qkv, b_qkv, w_out, b_out, w_up, b_up, w_down, b_down,
    ):
        batch, length, width = tokens.shape
        rows = w_qkv.shape[0]
        ff = w_up.shape[1]
        count = seq * length
        total = group * batch * length
        my_seq = lax.axis_index("seq")
        me = lax.axis_index("yi") * seq + my_seq
        scaling = HEAD_DIM ** (-0.5)
        cols = lay.heads * HEAD_DIM
        ff_cols = ff // group
        out_cols = width // group
        plans = {"up": (1, rows, ff_cols), "down": (1, rows, ff_cols), "qkv": (3, rows, cols), "out": (1, rows, out_cols)}

        def gather_rows(mine):
            return lax.all_gather(mine, "zo", axis=0, tiled=True)

        x, core = my_seq // 2, my_seq % 2
        places = []
        for ry in range(sub):
            from_there = positions
            if ry:
                from_there = lax.ppermute(positions, "yi", [(i, (i + ry) % sub) for i in range(sub)])
            blocks = from_there.reshape(batch, seq, length)
            order = [((x - rx) % chips_x) * 2 + (core + rc) % 2 for rc in range(2) for rx in range(chips_x)]
            places.append(jnp.concatenate([lax.dynamic_slice_in_dim(blocks, o, 1, 1) for o in order], 1))
        places = jnp.stack(places).reshape(sub * batch, count)

        def laid(values):
            size = -(-sum(v.size for v in values) // 1024) * 1024
            whole, at = 0.0, 0
            for v in values:
                whole = whole + jnp.pad(v.astype(F32), (at, size - at - v.size))
                at += v.size
            return whole.reshape(-1, 128)

        names = (bias1, bias2, gain1, gain2, b_qkv, b_up, b_out, b_down)
        (up_own,) = deal_exchange(lay, [plans["up"]], [w_up], False, 0)
        up_w = gather_rows(up_own)
        w_qkv_late, _ = lax.optimization_barrier((w_qkv, up_own))
        (qkv_own,) = deal_exchange(lay, [plans["qkv"]], [w_qkv_late], False, 7)
        qkv_w = gather_rows(qkv_own)
        tokens_late, _ = lax.optimization_barrier((tokens, qkv_own))
        one, two, hat, vectors, out_own, down_own = norm_exchange(
            lay, [plans["out"], plans["down"]], tokens_late, laid(names), [w_out, w_down]
        )
        out_w = gather_rows(out_own)
        down_w = gather_rows(down_own)
        vectors = vectors.reshape(lay.count, -1)
        cuts = []
        at = 0
        for piece in names:
            cuts.append(vectors[:, at : at + piece.shape[0]].reshape(-1))
            at += piece.shape[0]
        _, _, gain1_all, gain2_all, b_qkv_all, b_up_all, b_out_all, b_down_all = cuts
        b_qkv_mine = lax.dynamic_index_in_dim(b_qkv_all.reshape(3, group, cols), me, 1, keepdims=False).reshape(-1)
        b_up_mine = lax.dynamic_index_in_dim(b_up_all.reshape(group, ff_cols), me, 0, keepdims=False)
        one, two, hat = [v.reshape(total, width) for v in (one, two, hat)]
        cotangent, hat, places = lax.optimization_barrier((cotangent, hat, places))
        near_dy = [cotangent] + [across(cotangent, o) for o in lay.near[1:]]

        hidden = dot(two, up_w, ((1,), (0,))) + b_up_mine
        phi_cdf = 0.5 * (1.0 + lax.erf(hidden * math.sqrt(0.5)))
        density = jnp.exp(-0.5 * hidden * hidden) * (1.0 / math.sqrt(2.0 * math.pi))
        activated = (hidden * phi_cdf).astype(BF16)
        slope = (phi_cdf + hidden * density).astype(BF16)
        activated, slope = lax.optimization_barrier((activated, slope))

        halves = ROTARY // 2
        frequency = jnp.exp(jnp.arange(halves, dtype=F32) * (-2.0 * math.log(10000.0) / ROTARY))
        places = after(places, activated)
        phases = places.astype(F32)[:, None, :] * frequency[None, :, None]
        cosine, sine = jnp.cos(phases), jnp.sin(phases)
        place_col = places[:, :, None]
        place_row = places[:, None, :]

        seqs = sub * batch
        one = after(one, cosine, sine)
        packed = dot(one, qkv_w, ((1,), (0,))) + b_qkv_mine

        wide = (2, 1, chips_x, 1, length, 3 * cols)
        wide_spec = pl.BlockSpec(wide, lambda i: (0, i // batch, 0, i % batch, 0, 0))
        full = (2, sub, chips_x, batch, length, 3 * cols)
        head_spec = pl.BlockSpec((1, count, HEAD_DIM), lambda i: (i, 0, 0))
        turn_spec = pl.BlockSpec((1, ROTARY // 2, count), lambda i: (i, 0, 0))
        tokens_spec = pl.BlockSpec((2, 1, chips_x, 1, length, cols), lambda i: (0, i // batch, 0, i % batch, 0, 0))
        by_token = (2, sub, chips_x, batch, length, cols)
        turn_bufs = [pltpu.VMEM((count, 128), F32)] * 2
        col_spec = pl.BlockSpec((1, count, 1), lambda i: (i, 0, 0))
        row_spec = pl.BlockSpec((1, 1, count), lambda i: (i, 0, 0))
        head_shape = jax.ShapeDtypeStruct((seqs, count, HEAD_DIM), BF16)
        work = 2 * seqs * count * count * HEAD_DIM
        params = pltpu.CompilerParams(vmem_limit_bytes=56 << 20)
        near_count, chips = len(near_dy), group // 2
        queries, keys, values, context, lse, upstream = pl.pallas_call(
            functools.partial(attend_kernel, lay, scaling),
            grid=(seqs,),
            in_specs=[wide_spec, turn_spec, turn_spec, col_spec, row_spec] + [ANY] * near_count,
            out_specs=[head_spec] * 3 + [tokens_spec, row_spec, ANY],
            out_shape=[head_shape] * 3
            + [
                jax.ShapeDtypeStruct(by_token, BF16),
                jax.ShapeDtypeStruct((seqs, 1, count), F32),
                jax.ShapeDtypeStruct((2, chips, *cotangent.shape), BF16),
            ],
            scratch_shapes=[pltpu.VMEM((count, HEAD_DIM), BF16)] * 4
            + turn_bufs
            + [pltpu.VMEM((near_count, *cotangent.shape), BF16)]
            + [pltpu.SemaphoreType.DMA((near_count,))] * 2
            + [pltpu.SemaphoreType.DMA((chips,))] * 2
            + [pltpu.SemaphoreType.DMA((2,))] * 2,
            compiler_params=pltpu.CompilerParams(collective_id=8, has_side_effects=True, vmem_limit_bytes=58 << 20),
            cost_estimate=pl.CostEstimate(flops=2 * work, bytes_accessed=30 << 20, transcendentals=seqs * count * count),
            name="attend",
        )(packed.reshape(full), cosine, sine, place_col, place_row, *near_dy)
        upstream = upstream.reshape(total, width)

        context = context.reshape(total, cols)

        def scatter(grad):
            return lax.psum_scatter(grad, "zo", scatter_dimension=0, tiled=True)

        def outer_dot(left, right):
            return dot(left, right, ((0,), (0,))).astype(BF16)

        def chain(values, *tokens):
            return lax.optimization_barrier((*values, *tokens))[: len(values)]

        def tokens_of(pieces):
            return [pieces[i * batch : (i + 1) * batch] for i in range(group // 2)]

        down_part = outer_dot(upstream, activated)
        upstream, down_part = chain((upstream, down_part))
        down_sum = scatter(down_part)
        grad_context = dot(upstream, out_w, ((1,), (0,))).astype(BF16)

        grad_packed, sum_packed = pl.pallas_call(
            functools.partial(attend_back_kernel, scaling),
            grid=(seqs,),
            in_specs=[head_spec] * 3 + [tokens_spec, turn_spec, turn_spec, col_spec, row_spec, row_spec],
            out_specs=[wide_spec, pl.BlockSpec((1, 1, 3 * cols), lambda i: (i, 0, 0))],
            out_shape=[jax.ShapeDtypeStruct(full, BF16), jax.ShapeDtypeStruct((seqs, 1, 3 * cols), F32)],
            scratch_shapes=[pltpu.VMEM((count, HEAD_DIM), BF16)] + [pltpu.VMEM((count, HEAD_DIM), F32)] * 3 + turn_bufs,
            compiler_params=params,
            cost_estimate=pl.CostEstimate(flops=5 * work, bytes_accessed=24 << 20, transcendentals=seqs * count * count),
            name="attend_back",
        )(queries, keys, values, grad_context.reshape(by_token), cosine, sine, place_col, place_row, lse)
        grad_packed = grad_packed.reshape(total, 3 * cols)

        acts = chain((context, activated), grad_packed)
        out_near = tokens_of(pair_matmul(lay, acts, (out_w, down_w), batch, (0, 1), 4))
        out_came = far_first(out_near)
        hat, out_near = chain((hat, out_near))
        qkv_part = outer_dot(hat, grad_packed)
        qkv_sum = scatter(qkv_part)
        (upstream,) = chain((upstream,), qkv_part)
        grad_hidden = (dot(upstream, down_w, ((1,), (0,))) * slope.astype(F32)).astype(BF16)
        sum_hidden = jnp.sum(grad_hidden.astype(F32), 0)
        out_came, grad_hidden = chain((out_came, grad_hidden))
        onward, grad_hidden = chain((far_onward(out_near, out_came), grad_hidden))
        out_parts = far_second(out_near, out_came, onward)
        up_part = outer_dot(hat, grad_hidden)
        up_sum = scatter(up_part)
        (left,) = chain((grad_packed,), up_part)

        folded = (qkv_w, up_w)
        scales = (gain1_all, gain2_all)
        left, down_sum = chain((left, down_sum))
        *near0, down_raw = pair_matmul(
            lay, (left, grad_hidden), folded, batch, (0, 2), 5, scales, [plans["down"]], [down_sum]
        )
        near0 = tokens_of(near0)
        came0 = far_first(near0)
        own_sums = [
            jnp.sum(sum_packed, (0, 1)),
            sum_hidden,
            jnp.sum(cotangent.astype(F32), (0, 1)),
        ]
        left, vec, qkv_sum = chain((left, laid(own_sums).astype(BF16), qkv_sum), near0)
        *near1, qkv_raw, everyone = pair_matmul(
            lay, (left, grad_hidden), folded, batch, (1, 2), 6, scales, [plans["qkv"]], [qkv_sum], vec
        )
        near1 = tokens_of(near1)
        came1 = far_first(near1)
        (came0,) = chain((came0,), near1)
        onward0 = far_onward(near0, came0)
        onward0, upstream = chain((onward0, upstream))
        parts0 = far_second(near0, came0, onward0)
        out_part = outer_dot(upstream, context)
        out_w_sum = scatter(out_part)
        (out_parts,) = chain((out_parts,), out_part)
        output = (tokens.astype(F32) + add_all(out_parts) + b_out_all + b_down_all).astype(BF16)
        sums = jnp.sum(everyone.astype(F32).reshape(lay.outer, group, -1), 0)
        sum_qkv = jnp.transpose(sums[:, : 3 * cols].reshape(group, 3, cols), (1, 0, 2)).reshape(-1)
        sum_up = sums[:, 3 * cols : 3 * cols + ff_cols].reshape(-1)
        sum_dy = jnp.sum(sums[:, 3 * cols + ff_cols : 3 * cols + ff_cols + width], 0)
        rank = lax.axis_index("zo") * group + me

        def own_part(vector):
            return lax.dynamic_index_in_dim(vector.reshape(lay.count, -1), rank, 0, keepdims=False)

        column = lambda v: v.astype(F32)[:, None]
        qkv_raw = qkv_raw.astype(F32)
        bias_grads = (own_part(sum_qkv), own_part(sum_up), own_part(sum_dy))
        qkv_grads = (
            jnp.sum(w_qkv.astype(F32) * qkv_raw, 1),
            jnp.sum(w_qkv.astype(F32) * sum_qkv, 1),
            column(gain1) * qkv_raw + column(bias1) * sum_qkv,
        )
        down_grad = down_raw.astype(F32)
        came1, *early = chain((came1, output, down_grad, *bias_grads, *qkv_grads))
        output, down_grad, bias_grads, qkv_grads = early[0], early[1], early[2:5], early[5:8]
        onward1 = far_onward(near1, came1)
        parts1 = far_second(near1, came1, onward1)

        inputs = tokens.astype(F32)
        center = inputs - jnp.mean(inputs, -1, keepdims=True)
        inv_std = lax.rsqrt(jnp.mean(center * center, -1, keepdims=True) + EPSILON)
        normal = center * inv_std
        grad_normal = jnp.concatenate([add_all(parts0), add_all(parts1)], -1)
        token_grad = cotangent.astype(F32) + inv_std * (
            grad_normal
            - jnp.mean(grad_normal, -1, keepdims=True)
            - normal * jnp.mean(grad_normal * normal, -1, keepdims=True)
        )

        up_sum, token_grad = chain((up_sum, token_grad))
        up_raw, out_raw = deal_exchange(lay, [plans["up"], plans["out"]], [up_sum, out_w_sum], True, 3)
        up_raw = up_raw.astype(F32)
        up_grads = (
            jnp.sum(w_up.astype(F32) * up_raw, 1),
            jnp.sum(w_up.astype(F32) * sum_up, 1),
            column(gain2) * up_raw + column(bias2) * sum_up,
        )
        return (
            output,
            token_grad,
            qkv_grads[0],
            qkv_grads[1],
            up_grads[0],
            up_grads[1],
            qkv_grads[2],
            bias_grads[0],
            out_raw.astype(F32),
            bias_grads[2],
            up_grads[2],
            bias_grads[1],
            down_grad,
            bias_grads[2],
        )

    return step


def solution(mesh):
    outer, sub, seq = split_axes(mesh)
    inner = Mesh(mesh.devices.reshape(outer, sub, seq), ALL)
    act = P(None, ALL, None)
    vec = P(ALL)
    mat = P(ALL, None)
    return jax.shard_map(
        make_body(Layout(outer, sub, seq)),
        mesh=inner,
        in_specs=(
            act, P(None, ("zo", "yi")), act, vec, vec, vec, vec,
            mat, vec, mat, vec, mat, vec, mat, vec,
        ),
        out_specs=(act, act, vec, vec, vec, vec, mat, vec, mat, vec, mat, vec, mat, vec),
        check_vma=False,
    )
```

```python
import functools
import math

import jax
import jax.numpy as jnp
from jax import lax
from jax.experimental import pallas as pl
from jax.experimental.pallas import tpu as pltpu
from jax.sharding import Mesh, PartitionSpec as P


HEADS = 8
HEAD_DIM = 256
ROTARY = 64
EPSILON = 1e-05
NEGATIVE = -1e30
F32 = jnp.float32
BF16 = jnp.bfloat16
ALL = ("zo", "yi", "seq")
GROUP = ("yi", "seq")
MESH = pl.DeviceIdType.MESH
ANY = pl.BlockSpec(memory_space=pl.ANY)


def dot(left, right, dims):
    return lax.dot_general(left, right, (dims, ((), ())), preferred_element_type=F32)


def split_axes(mesh):
    dp, seq = mesh.shape["dp"], mesh.shape["seq"]
    sub = 1
    while seq * sub * 2 <= HEADS and dp % (sub * 2) == 0:
        sub *= 2
    return dp // sub, sub, seq


def remote(source, target, send, recv, device):
    return pltpu.make_async_remote_copy(
        src_ref=source, dst_ref=target, send_sem=send, recv_sem=recv,
        device_id=device, device_id_type=MESH,
    )


class Layout:
    def __init__(self, outer, sub, seq):
        self.outer, self.sub, self.seq = outer, sub, seq
        self.chips_x = seq // 2
        self.group = sub * seq
        self.count = outer * self.group
        self.heads = HEADS // self.group
        self.offsets = [(ry, rx) for ry in range(sub) for rx in range(self.chips_x)]
        self.square = sub == 2 and self.chips_x == 2
        self.near = [o for o in self.offsets if not (self.square and o == (1, 1))]
        self.far = sorted(self.offsets[1:], key=lambda o: (o[0] > 0) + (o[1] > 0))

    def shift(self, ry, rx):
        pairs = []
        for y in range(self.sub):
            for x in range(self.chips_x):
                for c in range(2):
                    there = ((y + ry) % self.sub, (x + rx) % self.chips_x)
                    pairs.append((y * self.seq + x * 2 + c, there[0] * self.seq + there[1] * 2 + c))
        return pairs

    def flip(self):
        return [(i, i ^ 1) for i in range(self.seq)]


def swap_copies(lay, plan, me, sources, targets, send, recv, back):
    zo = lax.axis_index("zo")
    copies = []
    for k in range(1, lay.group):
        peer = lax.rem(me + k, lay.group)
        device = (zo, peer // lay.seq, lax.rem(peer, lay.seq))
        j = 0
        for (parts, rows, cols, first), source, target in zip(plan, sources, targets, strict=True):
            for part in range(parts):
                wide = lambda who: pl.ds(pl.multiple_of((part * lay.group + who) * cols, 128), cols)
                thin = pl.ds(first + part * cols, cols)
                block = lambda who: pl.ds(pl.multiple_of(who * rows, rows), rows)
                if back:
                    copies.append(remote(source.at[block(peer), thin], target.at[:, wide(me)], send.at[k - 1, j], recv.at[k - 1, j], device))
                else:
                    copies.append(remote(source.at[:, wide(peer)], target.at[block(me), thin], send.at[k - 1, j], recv.at[k - 1, j], device))
                j += 1
    return copies


def swap_own(lay, plan, me, sources, targets, sems, back):
    copies = []
    j = 0
    for (parts, rows, cols, first), source, target in zip(plan, sources, targets, strict=True):
        for part in range(parts):
            wide = pl.ds(pl.multiple_of((part * lay.group + me) * cols, 128), cols)
            thin = pl.ds(first + part * cols, cols)
            block = pl.ds(pl.multiple_of(me * rows, rows), rows)
            if back:
                copies.append(pltpu.make_async_copy(source.at[block, thin], target.at[:, wide], sems.at[j]))
            else:
                copies.append(pltpu.make_async_copy(source.at[:, wide], target.at[block, thin], sems.at[j]))
            j += 1
    return copies


def group_barrier(lay, me):
    zo = lax.axis_index("zo")
    barrier = pltpu.get_barrier_semaphore()
    for k in range(1, lay.group):
        peer = lax.rem(me + k, lay.group)
        pl.semaphore_signal(
            barrier, inc=1, device_id=(zo, peer // lay.seq, lax.rem(peer, lay.seq)), device_id_type=MESH
        )
    pl.semaphore_wait(barrier, lay.group - 1)


def swap_shapes(lay, plan, back):
    if back:
        return [jax.ShapeDtypeStruct((rows, parts * lay.group * cols), BF16) for parts, rows, cols, _ in plan]
    return [jax.ShapeDtypeStruct((lay.group * rows, parts * cols), BF16) for parts, rows, cols, _ in plan]


def device_after(lay, rank, k):
    peer = lax.rem(rank + k, lay.count)
    inner = lax.rem(peer, lay.group)
    return (peer // lay.group, inner // lay.seq, lax.rem(inner, lay.seq))


def barrier_all(lay, device_of):
    barrier = pltpu.get_barrier_semaphore()

    def greet(k, carry):
        pl.semaphore_signal(barrier, inc=1, device_id=device_of(k), device_id_type=MESH)
        return carry

    lax.fori_loop(1, lay.count, greet, 0)
    pl.semaphore_wait(barrier, lay.count - 1)


def busy(microseconds):
    return pl.CostEstimate(flops=int(7e8 * microseconds), bytes_accessed=1 << 20, transcendentals=0)


def norm_kernel(lay, plan, *refs):
    n = len(plan)
    x_ref, vec_ref, sources = refs[0], refs[1], refs[2 : 2 + n]
    one_ref, two_ref, hat_ref, all_ref, targets = *refs[2 + n : 6 + n], refs[6 + n : 6 + 2 * n]
    (held, stage, vectors, gain_buf, send, recv, core_send, core_recv, w_send, w_recv, w_own, own_sem, out_sem,
     vec_send, vec_recv, vec_own) = refs[6 + 2 * n :]
    batch, length, width = x_ref.shape
    zo, yi, s = lax.axis_index("zo"), lax.axis_index("yi"), lax.axis_index("seq")
    me = yi * lay.seq + s
    x, core = s // 2, lax.rem(s, 2)
    partner = (zo, yi, x * 2 + 1 - core)

    def chip(ry, rx):
        return (zo, lax.rem(yi + ry, lay.sub), lax.rem(x + rx, lay.chips_x) * 2 + core)

    rank = zo * lay.group + me
    device_of = functools.partial(device_after, lay, rank)
    barrier_all(lay, device_of)

    def vec_copy(k):
        return remote(vec_ref, vectors.at[rank], vec_send.at[k - 1], vec_recv.at[k - 1], device_of(k))

    def vec_start(k, carry):
        vec_copy(k).start()
        return carry

    def vec_finish(k, carry):
        vec_copy(k).wait()
        return carry

    lax.fori_loop(1, lay.count, vec_start, 0)
    vec_mine = pltpu.make_async_copy(vec_ref, vectors.at[rank], vec_own.at[0])
    vec_mine.start()
    slot = {offset: i for i, offset in enumerate(lay.offsets)}
    own_copy = pltpu.make_async_copy(x_ref, held.at[0, 0], own_sem)
    own_copy.start()
    straight = [o for o in lay.far if not (o[0] and o[1])]
    diagonal = [o for o in lay.far if o[0] and o[1]]
    copies = {}
    for o in straight:
        copies[o] = [remote(x_ref, held.at[0, slot[o]], send.at[slot[o], 0], recv.at[slot[o], 0], chip(*o))]
    half = batch // 2
    for ry, rx in diagonal:
        j = slot[(ry, rx)]
        copies[(ry, rx)] = [
            remote(held.at[0, slot[(0, rx)], :half], held.at[0, j, :half], send.at[j, 0], recv.at[j, 0], chip(ry, 0)),
            remote(held.at[0, slot[(ry, 0)], half:], held.at[0, j, half:], send.at[j, 1], recv.at[j, 1], chip(0, rx)),
        ]
    to_partner = {
        o: remote(x_ref if o == (0, 0) else held.at[0, slot[o]], held.at[1, slot[o]],
                  core_send.at[slot[o]], core_recv.at[slot[o]], partner)
        for o in lay.offsets
    }
    for o in straight:
        copies[o][0].start()
    to_partner[(0, 0)].start()
    swaps = swap_copies(lay, plan, me, sources, targets, w_send, w_recv, False)
    swaps += swap_own(lay, plan, me, sources, targets, w_own, False)
    lax.fori_loop(1, lay.count, vec_finish, 0)
    vec_mine.wait()
    vec_out = pltpu.make_async_copy(vectors, all_ref, vec_own.at[1])
    vec_out.start()
    size = width // lay.count
    lane = lax.broadcasted_iota(jnp.int32, (1, 128), 1)
    for v in range(4):
        row, low = (v * size) // 128, (v * size) % 128
        for k in range(width // 128):
            line = None
            for j in range(128 // size):
                piece = vectors[k * (128 // size) + j, row : row + 1, :]
                turn = (j * size - low) % 128
                piece = pltpu.roll(piece, turn, 1) if turn else piece
                line = piece if line is None else jnp.where(lane >= j * size, piece, line)
            gain_buf[v : v + 1, k * 128 : (k + 1) * 128] = line
    gains = [gain_buf[i : i + 1, :] for i in range(4)]
    rows = 16
    pending = [[], []]
    turn = [0]

    def norm(c, j):
        for m in range(batch):
            k = turn[0] % 2
            turn[0] += 1
            for copy in pending[k]:
                copy.wait()

            def chunk(i, carry):
                at = pl.ds(pl.multiple_of(i * rows, rows), rows)
                value = held[c, j, m, at, :].astype(F32)
                center = value - jnp.mean(value, -1, keepdims=True)
                hat = center * lax.rsqrt(jnp.mean(center * center, -1, keepdims=True) + EPSILON)
                stage[k, 0, at, :] = (hat * gains[2] + gains[0]).astype(BF16)
                stage[k, 1, at, :] = (hat * gains[3] + gains[1]).astype(BF16)
                stage[k, 2, at, :] = hat.astype(BF16)
                return carry

            lax.fori_loop(0, length // rows, chunk, 0, unroll=2)
            pending[k] = [
                pltpu.make_async_copy(stage.at[k, i], ref.at[c, j, m], out_sem.at[k, i])
                for i, ref in enumerate((one_ref, two_ref, hat_ref))
            ]
            for copy in pending[k]:
                copy.start()

    own_copy.wait()
    norm(0, 0)
    to_partner[(0, 0)].wait_recv()
    norm(1, 0)
    for o in straight:
        copies[o][0].wait_recv()
        to_partner[o].start()
        for ry, rx in diagonal:
            if o == (0, rx):
                copies[(ry, rx)][0].start()
            if o == (ry, 0):
                copies[(ry, rx)][1].start()
        if o == straight[-1]:
            for copy in swaps:
                copy.start()
        norm(0, slot[o])
    for o in straight:
        to_partner[o].wait_recv()
        norm(1, slot[o])
    for o in diagonal:
        for copy in copies[o]:
            copy.wait_recv()
        to_partner[o].start()
        norm(0, slot[o])
    for o in diagonal:
        to_partner[o].wait_recv()
        norm(1, slot[o])
    for side in pending:
        for copy in side:
            copy.wait()
    for o in lay.far:
        for copy in copies[o]:
            copy.wait_send()
    for o in lay.offsets:
        to_partner[o].wait_send()
    for copy in swaps:
        copy.wait()
    vec_out.wait()


def norm_exchange(lay, plan, tokens, vec, weights):
    count = sum(parts for parts, _, _, _ in plan)
    chips = lay.group // 2
    whole = jax.ShapeDtypeStruct((2, chips, *tokens.shape), BF16)
    return pl.pallas_call(
        functools.partial(norm_kernel, lay, plan),
        out_shape=[whole] * 3 + [jax.ShapeDtypeStruct((lay.count, *vec.shape), F32)] + swap_shapes(lay, plan, False),
        in_specs=[ANY] * (2 + len(plan)),
        out_specs=[ANY] * (4 + len(plan)),
        scratch_shapes=[
            pltpu.VMEM((2, chips, *tokens.shape), BF16),
            pltpu.VMEM((2, 3, *tokens.shape[1:]), BF16),
            pltpu.VMEM((lay.count, *vec.shape), F32),
            pltpu.VMEM((4, tokens.shape[2]), F32),
            pltpu.SemaphoreType.DMA((chips, 2)),
            pltpu.SemaphoreType.DMA((chips, 2)),
            pltpu.SemaphoreType.DMA((chips,)),
            pltpu.SemaphoreType.DMA((chips,)),
            pltpu.SemaphoreType.DMA((lay.group - 1, count)),
            pltpu.SemaphoreType.DMA((lay.group - 1, count)),
            pltpu.SemaphoreType.DMA((count,)),
            pltpu.SemaphoreType.DMA,
            pltpu.SemaphoreType.DMA((2, 3)),
            pltpu.SemaphoreType.DMA((lay.count - 1,)),
            pltpu.SemaphoreType.DMA((lay.count - 1,)),
            pltpu.SemaphoreType.DMA((2,)),
        ],
        compiler_params=pltpu.CompilerParams(
            collective_id=1, has_side_effects=True, vmem_limit_bytes=48 << 20
        ),
        cost_estimate=busy(100),
        name="norm_exchange",
    )(tokens, vec, *weights)


def deal_kernel(lay, plan, back, *refs):
    n = len(plan)
    sources, targets = refs[:n], refs[n : 2 * n]
    send, recv, own = refs[2 * n :]
    me = lax.axis_index("yi") * lay.seq + lax.axis_index("seq")
    group_barrier(lay, me)
    copies = swap_copies(lay, plan, me, sources, targets, send, recv, back)
    copies += swap_own(lay, plan, me, sources, targets, own, back)
    for copy in copies:
        copy.start()
    for copy in copies:
        copy.wait()


def deal_exchange(lay, plan, arrays, back, number):
    count = sum(parts for parts, _, _, _ in plan)
    return pl.pallas_call(
        functools.partial(deal_kernel, lay, plan, back),
        out_shape=swap_shapes(lay, plan, back),
        in_specs=[ANY] * len(plan),
        out_specs=[ANY] * len(plan),
        scratch_shapes=[
            pltpu.SemaphoreType.DMA((lay.group - 1, count)),
            pltpu.SemaphoreType.DMA((lay.group - 1, count)),
            pltpu.SemaphoreType.DMA((count,)),
        ],
        compiler_params=pltpu.CompilerParams(collective_id=number, has_side_effects=True),
        cost_estimate=busy(17),
    )(*arrays)


def pair_kernel(lay, plan, with_vec, scaled, batch, *refs):
    refs = list(refs)
    take = lambda k: [refs.pop(0) for _ in range(k)]
    step = pl.program_id(0)
    chips = lay.group // 2
    first_ref, first_w, second_ref, second_w = take(4)
    scales = take(2) if scaled else []
    sources, vec_ref = take(len(plan)), take(int(with_vec))
    outs, targets, all_ref = take(chips * batch), take(len(plan)), take(int(with_vec))
    given, came, act_buf, w_buf, send, recv, out_sem = take(7)
    zo, yi, s = lax.axis_index("zo"), lax.axis_index("yi"), lax.axis_index("seq")
    me = yi * lay.seq + s
    rank = zo * lay.group + me
    device_of = functools.partial(device_after, lay, rank)
    partner = (zo, yi, (s // 2) * 2 + 1 - lax.rem(s, 2))
    swap_sems = take(3) if plan else []
    vec_sems = take(3) if with_vec else []

    def copy(j):
        return remote(given.at[j], came.at[j], send.at[j], recv.at[j], partner)

    def stores(j):
        length = came.shape[1] // batch
        return [
            pltpu.make_async_copy(
                came.at[j, pl.ds(m * length, length)], outs[(j + 1) % chips * batch + m], out_sem.at[j, m]
            )
            for m in range(batch)
        ]

    def riders():
        if not plan:
            return []
        copies = swap_copies(lay, plan, me, sources, targets, swap_sems[0], swap_sems[1], True)
        return copies + swap_own(lay, plan, me, sources, targets, swap_sems[2], True)

    def vec_copy(k):
        return remote(vec_ref[0], all_ref[0].at[rank], vec_sems[0].at[k - 1], vec_sems[1].at[k - 1], device_of(k))

    def vec_start(k, carry):
        vec_copy(k).start()
        return carry

    def vec_finish(k, carry):
        vec_copy(k).wait()
        return carry

    def vec_mine():
        return pltpu.make_async_copy(vec_ref[0], all_ref[0].at[rank], vec_sems[2])

    @pl.when(step == 0)
    def _():
        if with_vec:
            barrier_all(lay, device_of)
            vec_mine().start()
            lax.fori_loop(1, lay.count, vec_start, 0)
        elif plan:
            group_barrier(lay, me)
        else:
            barrier = pltpu.get_barrier_semaphore()
            pl.semaphore_signal(barrier, inc=1, device_id=partner, device_id_type=MESH)
            pl.semaphore_wait(barrier, 1)
        for rider in riders():
            rider.start()
        at = 0
        for k, weight in enumerate((first_w, second_w)):
            depth = weight.shape[1]
            if scaled:
                line = scales[k][...]
                gain = jnp.transpose(jnp.broadcast_to(line, (128, line.shape[1])), (1, 0))
                for c in range(0, depth, 128):
                    w_buf[:, at + c : at + c + 128] = (weight[:, c : c + 128].astype(F32) * gain).astype(BF16)
            else:
                w_buf[:, at : at + depth] = weight[...]
            at += depth

    for j in range(chips):

        @pl.when(step == j + 1)
        def _():
            copy(j).start()

    cut = first_ref.shape[3]
    act_buf[:, :cut] = first_ref[0, 0]
    act_buf[:, cut:] = second_ref[0, 0]
    total = dot(act_buf[...], w_buf[...], ((1,), (1,)))
    for j in range(chips):

        @pl.when(step == j)
        def _():
            given[j] = total.astype(BF16)

        @pl.when(step == chips + j)
        def _():
            copy(j).wait_recv()
            came[j] = (total + came[j].astype(F32)).astype(BF16)

    for j in range(chips - 1):

        @pl.when(step == chips + j + 1)
        def _():
            for piece in stores(j):
                piece.start()

    @pl.when(step == 2 * chips - 1)
    def _():
        for piece in stores(chips - 1):
            piece.start()
        for j in range(chips):
            copy(j).wait_send()
            for piece in stores(j):
                piece.wait()
        for rider in riders():
            rider.wait()
        if with_vec:
            vec_mine().wait()
            lax.fori_loop(1, lay.count, vec_finish, 0)


def pair_matmul(lay, acts, weights, batch, cut, number, scales=(), plan=(), arrays=(), vec=None):
    chips = lay.group // 2
    rows = acts[0].shape[0] // lay.group
    width = weights[0].shape[0] // cut[1]
    count = sum(parts for parts, _, _, _ in plan)
    with_vec = vec is not None

    def act(depth):
        return pl.BlockSpec((1, 1, rows, depth), lambda i: (1 - i // chips, (i + 1) % chips, 0, 0))

    def weight(depth):
        return pl.BlockSpec((width, depth), lambda i: (cut[0], 0), pipeline_mode=pl.Buffered(1))

    specs, args = [], []
    for a, w in zip(acts, weights, strict=True):
        specs += [act(a.shape[1]), weight(a.shape[1])]
        args += [a.reshape(2, chips, rows, a.shape[1]), w]
    for scale in scales:
        specs.append(pl.BlockSpec((1, width), lambda i: (0, cut[0])))
        args.append(scale.reshape(1, -1))
    args += [*arrays, *([vec] if with_vec else [])]
    specs += [ANY] * (len(args) - len(specs))
    shapes = [jax.ShapeDtypeStruct((rows // batch, width), BF16)] * (chips * batch) + swap_shapes(lay, plan, True)
    depth = sum(a.shape[1] for a in acts)
    scratch = [
        pltpu.VMEM((chips, rows, width), BF16),
        pltpu.VMEM((chips, rows, width), BF16),
        pltpu.VMEM((rows, depth), BF16),
        pltpu.VMEM((width, depth), BF16),
        pltpu.SemaphoreType.DMA((chips,)),
        pltpu.SemaphoreType.DMA((chips,)),
        pltpu.SemaphoreType.DMA((chips, batch)),
    ]
    if plan:
        scratch += [pltpu.SemaphoreType.DMA((lay.group - 1, count))] * 2 + [pltpu.SemaphoreType.DMA((count,))]
    if with_vec:
        shapes.append(jax.ShapeDtypeStruct((lay.count, *vec.shape), vec.dtype))
        scratch += [pltpu.SemaphoreType.DMA((lay.count - 1,))] * 2 + [pltpu.SemaphoreType.DMA]
    return pl.pallas_call(
        functools.partial(pair_kernel, lay, plan, with_vec, bool(scales), batch),
        grid=(2 * chips,),
        in_specs=specs,
        out_specs=[ANY] * len(shapes),
        out_shape=shapes,
        scratch_shapes=scratch,
        compiler_params=pltpu.CompilerParams(
            collective_id=number, has_side_effects=True, vmem_limit_bytes=60 << 20
        ),
        cost_estimate=pl.CostEstimate(
            flops=2 * acts[0].shape[0] * depth * width, bytes_accessed=32 << 20, transcendentals=0
        ),
    )(*args)


def turn_pairs(field, cosine, sine):
    halves = ROTARY // 2
    front = field[:, :128]
    lane = lax.broadcasted_iota(jnp.int32, front.shape, 1)
    other = jnp.where(lane < halves, pltpu.roll(front, 128 - halves, 1), pltpu.roll(front, halves, 1))
    return jnp.concatenate([front * cosine + other * sine, field[:, 128:]], -1)


QUERY_BLOCK = 256


def wide_angles(ref):
    part = ref[0]
    return jnp.transpose(jnp.concatenate([part, part, part, part], 0), (1, 0))


def wide_pair(cos_ref, sin_ref):
    cosine, sine = wide_angles(cos_ref), wide_angles(sin_ref)
    lane = lax.broadcasted_iota(jnp.int32, cosine.shape, 1)
    cosine = jnp.where(lane < ROTARY, cosine, 1.0)
    sine = jnp.where(lane < ROTARY // 2, -sine, jnp.where(lane < ROTARY, sine, 0.0))
    return cosine, sine


def attend_kernel(lay, scaling, *refs):
    refs = list(refs)
    take = lambda k: [refs.pop(0) for _ in range(k)]
    near_count = len(lay.near)
    packed_ref, cos_ref, sin_ref, col_ref, row_ref = take(5)
    near = take(near_count)
    q_ref, k_ref, v_ref, ctx_ref, lse_ref, dy_ref = take(6)
    q_buf, k_buf, v_buf, ctx_buf, cos_buf, sin_buf, bounce = take(7)
    load_sem, store_sem, core_send, core_recv, on_send, on_recv = take(6)
    step, last = pl.program_id(0), pl.num_programs(0) - 1
    zo, yi, s = lax.axis_index("zo"), lax.axis_index("yi"), lax.axis_index("seq")
    x, core = s // 2, lax.rem(s, 2)
    partner = (zo, yi, x * 2 + 1 - core)
    chips = lay.group // 2
    half = near[0].shape[0] // 2

    def load(i):
        return pltpu.make_async_copy(near[i], bounce.at[i], load_sem.at[i])

    def store(i):
        return pltpu.make_async_copy(bounce.at[i], dy_ref.at[0, i], store_sem.at[i])

    def to_partner(i):
        source = near[i] if i < near_count else dy_ref.at[0, i]
        return remote(source, dy_ref.at[1, i], core_send.at[i], core_recv.at[i], partner)

    def onward():
        if not lay.square:
            return []
        over_y = (zo, lax.rem(yi + 1, lay.sub), s)
        over_x = (zo, yi, lax.rem(x + 1, lay.chips_x) * 2 + core)
        return [
            remote(near[1].at[:half], dy_ref.at[0, 3, :half], on_send.at[0], on_recv.at[0], over_y),
            remote(near[2].at[half:], dy_ref.at[0, 3, half:], on_send.at[1], on_recv.at[1], over_x),
        ]

    @pl.when(step == 0)
    def _():
        group_barrier(lay, yi * lay.seq + s)
        for copy in onward():
            copy.start()
        for i in range(near_count):
            load(i).start()
            to_partner(i).start()

    @pl.when(step == 1)
    def _():
        for i in range(near_count):
            load(i).wait()
            store(i).start()

    attend_one(scaling, packed_ref, cos_ref, sin_ref, col_ref, row_ref, q_ref, k_ref, v_ref, ctx_ref, lse_ref,
               q_buf, k_buf, v_buf, ctx_buf, cos_buf, sin_buf)

    @pl.when(step == last)
    def _():
        for copy in onward():
            copy.wait_recv()
        for i in range(near_count, chips):
            to_partner(i).start()
        for i in range(near_count):
            store(i).wait()
        for i in range(chips):
            to_partner(i).wait()
        for copy in onward():
            copy.wait_send()


def attend_one(scaling, packed_ref, cos_ref, sin_ref, col_ref, row_ref, q_ref, k_ref, v_ref, ctx_ref, lse_ref,
               q_buf, k_buf, v_buf, ctx_buf, cos_buf, sin_buf):
    cores, _, chips, _, length, _ = packed_ref.shape
    cos_all, sin_all = wide_pair(cos_ref, sin_ref)
    cos_buf[...] = cos_all
    sin_buf[...] = sin_all
    for c in range(cores):
        for i in range(chips):
            at = pl.ds((c * chips + i) * length, length)
            block = packed_ref[c, 0, i, 0]
            cosine, sine = cos_buf[at, :], sin_buf[at, :]
            q_buf[at, :] = turn_pairs(block[:, :HEAD_DIM], cosine, sine).astype(BF16)
            k_buf[at, :] = turn_pairs(block[:, HEAD_DIM : 2 * HEAD_DIM], cosine, sine).astype(BF16)
            v_buf[at, :] = block[:, 2 * HEAD_DIM :].astype(BF16)
    q_ref[0] = q_buf[...]
    k_ref[0] = k_buf[...]
    v_ref[0] = v_buf[...]
    total = cores * chips * length

    def one(j, carry):
        at = pl.ds(pl.multiple_of(j * QUERY_BLOCK, QUERY_BLOCK), QUERY_BLOCK)
        scores = dot(k_buf[...], q_buf[at, :], ((1,), (1,))) * scaling
        allowed = col_ref[0] <= row_ref[0, :, at]
        scores = jnp.where(allowed, scores, NEGATIVE)
        top = jnp.max(scores, 0, keepdims=True)
        weights = jnp.where(allowed, jnp.exp(scores - top), 0.0)
        total_row = jnp.sum(weights, 0, keepdims=True)
        probs = (weights * (1.0 / total_row)).astype(BF16)
        ctx_buf[at, :] = dot(probs, v_buf[...], ((0,), (0,))).astype(BF16)
        lse_ref[0, :, at] = top + jnp.log(total_row)
        return carry

    lax.fori_loop(0, total // QUERY_BLOCK, one, 0)
    for c in range(cores):
        for i in range(chips):
            ctx_ref[c, 0, i, 0] = ctx_buf[pl.ds((c * chips + i) * length, length), :]


def attend_back_kernel(scaling, q_ref, k_ref, v_ref, dy_ref, w_ref, cos_ref, sin_ref, col_ref, row_ref, lse_ref, out_ref, sum_ref,
                       g_buf, dq_buf, dk_buf, dv_buf, cos_buf, sin_buf):
    cores, _, chips, _, length, _ = out_ref.shape
    total = q_ref.shape[1]
    cos_all, sin_all = wide_pair(cos_ref, sin_ref)
    cos_buf[...] = cos_all
    sin_buf[...] = sin_all
    for c in range(cores):
        for i in range(chips):
            g_buf[pl.ds((c * chips + i) * length, length), :] = dot(dy_ref[c, 0, i, 0], w_ref[...], ((1,), (0,))).astype(BF16)
    dk_buf[...] = jnp.zeros_like(dk_buf)
    dv_buf[...] = jnp.zeros_like(dv_buf)

    def one(j, carry):
        at = pl.ds(pl.multiple_of(j * QUERY_BLOCK, QUERY_BLOCK), QUERY_BLOCK)
        queries = q_ref[0, at, :]
        grads = g_buf[at, :]
        scores = dot(k_ref[0], queries, ((1,), (1,))) * scaling
        allowed = col_ref[0] <= row_ref[0, :, at]
        scores = jnp.where(allowed, scores, NEGATIVE)
        probs = jnp.where(allowed, jnp.exp(scores - lse_ref[0, :, at]), 0.0)
        grad_probs = dot(v_ref[0], grads, ((1,), (1,)))
        delta = jnp.sum(probs * grad_probs, 0, keepdims=True)
        grad_scores = (probs * (grad_probs - delta)).astype(BF16)
        dv_buf[...] += dot(probs.astype(BF16), grads, ((1,), (0,)))
        dk_buf[...] += dot(grad_scores, queries, ((1,), (0,)))
        dq_buf[at, :] = dot(grad_scores, k_ref[0], ((0,), (0,)))
        return carry

    lax.fori_loop(0, total // QUERY_BLOCK, one, 0)
    for c in range(cores):
        for i in range(chips):
            at = pl.ds((c * chips + i) * length, length)
            cosine, sine = cos_buf[at, :], sin_buf[at, :]
            pieces = (
                turn_pairs(dq_buf[at, :] * scaling, cosine, -sine),
                turn_pairs(dk_buf[at, :] * scaling, cosine, -sine),
                dv_buf[at, :],
            )
            for k, piece in enumerate(pieces):
                columns = slice(k * HEAD_DIM, (k + 1) * HEAD_DIM)
                low = piece.astype(BF16)
                out_ref[c, 0, i, 0, :, columns] = low
                part = jnp.sum(low.astype(F32), 0, keepdims=True)
                sum_ref[0, :, columns] = part if c + i == 0 else sum_ref[0, :, columns] + part


def make_body(lay):
    sub, seq, group, chips_x = lay.sub, lay.seq, lay.group, lay.chips_x

    square = lay.square

    def across(value, o):
        return lax.ppermute(value, GROUP, lay.shift(*o))

    def add(*pieces):
        total = pieces[0].astype(F32)
        for piece in pieces[1:]:
            total = total + piece.astype(F32)
        return total

    def far_first(pieces):
        if square:
            return [
                [across(pieces[2][0], (1, 0)), across(pieces[3][0], (1, 0))],
                [across(pieces[1][1], (0, 1)), across(pieces[3][1], (0, 1))],
            ]
        batch = len(pieces[0])
        return [
            [across(pieces[i][m], ((-o[0]) % sub, (-o[1]) % chips_x)) for i, o in enumerate(lay.offsets) if i]
            for m in range(batch)
        ]

    def far_onward(pieces, came):
        if square:
            return [add(pieces[1][0], came[0][1]).astype(BF16), add(pieces[2][1], came[1][1]).astype(BF16)]
        return []

    def far_second(pieces, came, onward):
        if square:
            last = [across(onward[0], (0, 1)), across(onward[1], (1, 0))]
            return [[pieces[0][m], came[m][0], last[m]] for m in range(2)]
        return [[pieces[0][m], *came[m]] for m in range(len(came))]

    def add_all(parts):
        return jnp.stack([add(*pieces) for pieces in parts])

    def after(value, *tokens):
        return lax.optimization_barrier((value, *tokens))[0]

    def step(
        tokens, positions, cotangent, gain1, bias1, gain2, bias2,
        w_qkv, b_qkv, w_out, b_out, w_up, b_up, w_down, b_down,
    ):
        batch, length, width = tokens.shape
        rows = w_qkv.shape[0]
        ff = w_up.shape[1]
        count = seq * length
        total = group * batch * length
        my_seq = lax.axis_index("seq")
        me = lax.axis_index("yi") * seq + my_seq
        scaling = HEAD_DIM ** (-0.5)
        cols = lay.heads * HEAD_DIM
        ff_cols = ff // group
        out_cols = width // group
        plans = {"up": (1, rows, ff_cols, 0), "down": (1, rows, ff_cols, 0), "qkv": (3, rows, cols, 0), "out": (1, rows, out_cols, 0)}

        def gather_rows(mine):
            return lax.all_gather(mine, "zo", axis=0, tiled=True)

        x, core = my_seq // 2, my_seq % 2
        places = []
        for ry in range(sub):
            from_there = positions
            if ry:
                from_there = lax.ppermute(positions, "yi", [(i, (i + ry) % sub) for i in range(sub)])
            blocks = from_there.reshape(batch, seq, length)
            order = [((x - rx) % chips_x) * 2 + (core + rc) % 2 for rc in range(2) for rx in range(chips_x)]
            places.append(jnp.concatenate([lax.dynamic_slice_in_dim(blocks, o, 1, 1) for o in order], 1))
        places = jnp.stack(places).reshape(sub * batch, count)

        def laid(values):
            size = -(-sum(v.size for v in values) // 1024) * 1024
            whole, at = 0.0, 0
            for v in values:
                whole = whole + jnp.pad(v.astype(F32), (at, size - at - v.size))
                at += v.size
            return whole.reshape(-1, 128)

        names = (bias1, bias2, gain1, gain2, b_qkv, b_up, b_out, b_down)
        (up_own,) = deal_exchange(lay, [plans["up"]], [w_up], False, 0)
        up_w = gather_rows(up_own)
        w_qkv_late, _ = lax.optimization_barrier((w_qkv, up_own))
        (qkv_own,) = deal_exchange(lay, [plans["qkv"]], [w_qkv_late], False, 7)
        qkv_w = gather_rows(qkv_own)
        tokens_late, _ = lax.optimization_barrier((tokens, qkv_own))
        one, two, hat, vectors, out_own, down_own = norm_exchange(
            lay, [plans["out"], plans["down"]], tokens_late, laid(names), [w_out, w_down]
        )
        out_w = gather_rows(out_own)
        down_w = gather_rows(down_own)
        vectors = vectors.reshape(lay.count, -1)
        cuts = []
        at = 0
        for piece in names:
            cuts.append(vectors[:, at : at + piece.shape[0]].reshape(-1))
            at += piece.shape[0]
        _, _, gain1_all, gain2_all, b_qkv_all, b_up_all, b_out_all, b_down_all = cuts
        b_qkv_mine = lax.dynamic_index_in_dim(b_qkv_all.reshape(3, group, cols), me, 1, keepdims=False).reshape(-1)
        b_up_mine = lax.dynamic_index_in_dim(b_up_all.reshape(group, ff_cols), me, 0, keepdims=False)
        one, two, hat = [v.reshape(total, width) for v in (one, two, hat)]
        cotangent, hat, places = lax.optimization_barrier((cotangent, hat, places))
        near_dy = [cotangent] + [across(cotangent, o) for o in lay.near[1:]]

        hidden = dot(two, up_w, ((1,), (0,))) + b_up_mine
        phi_cdf = 0.5 * (1.0 + lax.erf(hidden * math.sqrt(0.5)))
        density = jnp.exp(-0.5 * hidden * hidden) * (1.0 / math.sqrt(2.0 * math.pi))
        activated = (hidden * phi_cdf).astype(BF16)
        slope = (phi_cdf + hidden * density).astype(BF16)
        activated, slope = lax.optimization_barrier((activated, slope))

        halves = ROTARY // 2
        frequency = jnp.exp(jnp.arange(halves, dtype=F32) * (-2.0 * math.log(10000.0) / ROTARY))
        places = after(places, activated)
        phases = places.astype(F32)[:, None, :] * frequency[None, :, None]
        cosine, sine = jnp.cos(phases), jnp.sin(phases)
        place_col = places[:, :, None]
        place_row = places[:, None, :]

        seqs = sub * batch
        one = after(one, cosine, sine)
        packed = dot(one, qkv_w, ((1,), (0,))) + b_qkv_mine

        wide = (2, 1, chips_x, 1, length, 3 * cols)
        wide_spec = pl.BlockSpec(wide, lambda i: (0, i // batch, 0, i % batch, 0, 0))
        full = (2, sub, chips_x, batch, length, 3 * cols)
        head_spec = pl.BlockSpec((1, count, HEAD_DIM), lambda i: (i, 0, 0))
        turn_spec = pl.BlockSpec((1, ROTARY // 2, count), lambda i: (i, 0, 0))
        tokens_spec = pl.BlockSpec((2, 1, chips_x, 1, length, cols), lambda i: (0, i // batch, 0, i % batch, 0, 0))
        by_token = (2, sub, chips_x, batch, length, cols)
        turn_bufs = [pltpu.VMEM((count, 128), F32)] * 2
        col_spec = pl.BlockSpec((1, count, 1), lambda i: (i, 0, 0))
        row_spec = pl.BlockSpec((1, 1, count), lambda i: (i, 0, 0))
        head_shape = jax.ShapeDtypeStruct((seqs, count, HEAD_DIM), BF16)
        work = 2 * seqs * count * count * HEAD_DIM
        params = pltpu.CompilerParams(vmem_limit_bytes=56 << 20)
        near_count, chips = len(near_dy), group // 2
        queries, keys, values, context, lse, upstream = pl.pallas_call(
            functools.partial(attend_kernel, lay, scaling),
            grid=(seqs,),
            in_specs=[wide_spec, turn_spec, turn_spec, col_spec, row_spec] + [ANY] * near_count,
            out_specs=[head_spec] * 3 + [tokens_spec, row_spec, ANY],
            out_shape=[head_shape] * 3
            + [
                jax.ShapeDtypeStruct(by_token, BF16),
                jax.ShapeDtypeStruct((seqs, 1, count), F32),
                jax.ShapeDtypeStruct((2, chips, *cotangent.shape), BF16),
            ],
            scratch_shapes=[pltpu.VMEM((count, HEAD_DIM), BF16)] * 4
            + turn_bufs
            + [pltpu.VMEM((near_count, *cotangent.shape), BF16)]
            + [pltpu.SemaphoreType.DMA((near_count,))] * 2
            + [pltpu.SemaphoreType.DMA((chips,))] * 2
            + [pltpu.SemaphoreType.DMA((2,))] * 2,
            compiler_params=pltpu.CompilerParams(collective_id=8, has_side_effects=True, vmem_limit_bytes=58 << 20),
            cost_estimate=pl.CostEstimate(flops=2 * work, bytes_accessed=30 << 20, transcendentals=seqs * count * count),
            name="attend",
        )(packed.reshape(full), cosine, sine, place_col, place_row, *near_dy)
        upstream = upstream.reshape(total, width)

        context = context.reshape(total, cols)

        def scatter(grad):
            return lax.psum_scatter(grad, "zo", scatter_dimension=0, tiled=True)

        def outer_dot(left, right):
            return dot(left, right, ((0,), (0,))).astype(BF16)

        def chain(values, *tokens):
            return lax.optimization_barrier((*values, *tokens))[: len(values)]

        def tokens_of(pieces):
            return [pieces[i * batch : (i + 1) * batch] for i in range(group // 2)]

        down_part = outer_dot(upstream, activated)
        upstream, down_part = chain((upstream, down_part))
        down_sum = scatter(down_part)
        out_part = outer_dot(upstream, context)
        upstream, out_part = chain((upstream, out_part))

        grad_packed, sum_packed = pl.pallas_call(
            functools.partial(attend_back_kernel, scaling),
            grid=(seqs,),
            in_specs=[head_spec] * 3
            + [
                pl.BlockSpec((2, 1, chips_x, 1, length, width), lambda i: (0, i // batch, 0, i % batch, 0, 0)),
                pl.BlockSpec((width, cols), lambda i: (0, 0), pipeline_mode=pl.Buffered(1)),
            ]
            + [turn_spec, turn_spec, col_spec, row_spec, row_spec],
            out_specs=[wide_spec, pl.BlockSpec((1, 1, 3 * cols), lambda i: (i, 0, 0))],
            out_shape=[jax.ShapeDtypeStruct(full, BF16), jax.ShapeDtypeStruct((seqs, 1, 3 * cols), F32)],
            scratch_shapes=[pltpu.VMEM((count, HEAD_DIM), BF16)] + [pltpu.VMEM((count, HEAD_DIM), F32)] * 3 + turn_bufs,
            compiler_params=params,
            cost_estimate=pl.CostEstimate(flops=7 * work, bytes_accessed=40 << 20, transcendentals=seqs * count * count),
            name="attend_back",
        )(queries, keys, values, upstream.reshape(2, sub, chips_x, batch, length, width), out_w, cosine, sine, place_col, place_row, lse)
        grad_packed = grad_packed.reshape(total, 3 * cols)

        acts = chain((context, activated), grad_packed)
        out_near = tokens_of(pair_matmul(lay, acts, (out_w, down_w), batch, (0, 1), 4))
        out_came = far_first(out_near)
        hat, out_near = chain((hat, out_near))
        qkv_part = outer_dot(hat, grad_packed)
        qkv_sum = scatter(qkv_part)
        (upstream,) = chain((upstream,), qkv_part)
        grad_hidden = (dot(upstream, down_w, ((1,), (0,))) * slope.astype(F32)).astype(BF16)
        sum_hidden = jnp.sum(grad_hidden.astype(F32), 0)
        out_came, grad_hidden = chain((out_came, grad_hidden))
        onward, grad_hidden = chain((far_onward(out_near, out_came), grad_hidden))
        out_parts = far_second(out_near, out_came, onward)
        up_part = outer_dot(hat, grad_hidden)
        last_sum = scatter(jnp.concatenate([up_part, out_part], 1))
        (left,) = chain((grad_packed,), up_part)

        folded = (qkv_w, up_w)
        scales = (gain1_all, gain2_all)
        left, down_sum = chain((left, down_sum))
        *near0, down_raw = pair_matmul(
            lay, (left, grad_hidden), folded, batch, (0, 2), 5, scales, [plans["down"]], [down_sum]
        )
        near0 = tokens_of(near0)
        came0 = far_first(near0)
        own_sums = [
            jnp.sum(sum_packed, (0, 1)),
            sum_hidden,
            jnp.sum(cotangent.astype(F32), (0, 1)),
        ]
        left, vec, qkv_sum = chain((left, laid(own_sums).astype(BF16), qkv_sum), near0)
        *near1, qkv_raw, everyone = pair_matmul(
            lay, (left, grad_hidden), folded, batch, (1, 2), 6, scales, [plans["qkv"]], [qkv_sum], vec
        )
        near1 = tokens_of(near1)
        came1 = far_first(near1)
        (came0,) = chain((came0,), near1)
        onward0 = far_onward(near0, came0)
        parts0 = far_second(near0, came0, onward0)
        (out_parts,) = chain((out_parts,), onward0)
        output = (tokens.astype(F32) + add_all(out_parts) + b_out_all + b_down_all).astype(BF16)
        sums = jnp.sum(everyone.astype(F32).reshape(lay.outer, group, -1), 0)
        sum_qkv = jnp.transpose(sums[:, : 3 * cols].reshape(group, 3, cols), (1, 0, 2)).reshape(-1)
        sum_up = sums[:, 3 * cols : 3 * cols + ff_cols].reshape(-1)
        sum_dy = jnp.sum(sums[:, 3 * cols + ff_cols : 3 * cols + ff_cols + width], 0)
        rank = lax.axis_index("zo") * group + me

        def own_part(vector):
            return lax.dynamic_index_in_dim(vector.reshape(lay.count, -1), rank, 0, keepdims=False)

        column = lambda v: v.astype(F32)[:, None]
        qkv_raw = qkv_raw.astype(F32)
        bias_grads = (own_part(sum_qkv), own_part(sum_up), own_part(sum_dy))
        qkv_grads = (
            jnp.sum(w_qkv.astype(F32) * qkv_raw, 1),
            jnp.sum(w_qkv.astype(F32) * sum_qkv, 1),
            column(gain1) * qkv_raw + column(bias1) * sum_qkv,
        )
        down_grad = down_raw.astype(F32)
        came1, *early = chain((came1, output, down_grad, *bias_grads, *qkv_grads))
        output, down_grad, bias_grads, qkv_grads = early[0], early[1], early[2:5], early[5:8]
        onward1 = far_onward(near1, came1)
        parts1 = far_second(near1, came1, onward1)

        inputs = tokens.astype(F32)
        center = inputs - jnp.mean(inputs, -1, keepdims=True)
        inv_std = lax.rsqrt(jnp.mean(center * center, -1, keepdims=True) + EPSILON)
        normal = center * inv_std
        grad_normal = jnp.concatenate([add_all(parts0), add_all(parts1)], -1)
        token_grad = cotangent.astype(F32) + inv_std * (
            grad_normal
            - jnp.mean(grad_normal, -1, keepdims=True)
            - normal * jnp.mean(grad_normal * normal, -1, keepdims=True)
        )

        last_sum, token_grad = chain((last_sum, token_grad))
        up_raw, out_raw = deal_exchange(
            lay, [plans["up"], (1, rows, out_cols, ff_cols)], [last_sum, last_sum], True, 3
        )
        up_raw = up_raw.astype(F32)
        up_grads = (
            jnp.sum(w_up.astype(F32) * up_raw, 1),
            jnp.sum(w_up.astype(F32) * sum_up, 1),
            column(gain2) * up_raw + column(bias2) * sum_up,
        )
        return (
            output,
            token_grad,
            qkv_grads[0],
            qkv_grads[1],
            up_grads[0],
            up_grads[1],
            qkv_grads[2],
            bias_grads[0],
            out_raw.astype(F32),
            bias_grads[2],
            up_grads[2],
            bias_grads[1],
            down_grad,
            bias_grads[2],
        )

    return step


def solution(mesh):
    outer, sub, seq = split_axes(mesh)
    inner = Mesh(mesh.devices.reshape(outer, sub, seq), ALL)
    act = P(None, ALL, None)
    vec = P(ALL)
    mat = P(ALL, None)
    return jax.shard_map(
        make_body(Layout(outer, sub, seq)),
        mesh=inner,
        in_specs=(
            act, P(None, ("zo", "yi")), act, vec, vec, vec, vec,
            mat, vec, mat, vec, mat, vec, mat, vec,
        ),
        out_specs=(act, act, vec, vec, vec, vec, mat, vec, mat, vec, mat, vec, mat, vec),
        check_vma=False,
    )
```

```python
import functools
import math

import jax
import jax.numpy as jnp
from jax import lax
from jax.experimental import pallas as pl
from jax.experimental.pallas import tpu as pltpu
from jax.sharding import Mesh, PartitionSpec as P


HEADS = 8
HEAD_DIM = 256
ROTARY = 64
EPSILON = 1e-05
NEGATIVE = -1e30
F32 = jnp.float32
BF16 = jnp.bfloat16
ALL = ("zo", "yi", "seq")
GROUP = ("yi", "seq")
MESH = pl.DeviceIdType.MESH
ANY = pl.BlockSpec(memory_space=pl.ANY)


def dot(left, right, dims):
    return lax.dot_general(left, right, (dims, ((), ())), preferred_element_type=F32)


def split_axes(mesh):
    dp, seq = mesh.shape["dp"], mesh.shape["seq"]
    sub = 1
    while seq * sub * 2 <= HEADS and dp % (sub * 2) == 0:
        sub *= 2
    return dp // sub, sub, seq


def remote(source, target, send, recv, device):
    return pltpu.make_async_remote_copy(
        src_ref=source, dst_ref=target, send_sem=send, recv_sem=recv,
        device_id=device, device_id_type=MESH,
    )


def far_places(square, chips, batch):
    if square and batch == 2:
        return {(0, 0): (0, None), (0, 1): (1, None), (1, 0): (2, None), (2, 1): (3, None),
                (2, 0): (4, 0), (3, 0): (4, 1), (1, 1): (5, 0), (3, 1): (5, 1)}
    return {(o, m): (o * batch + m, None) for o in range(chips) for m in range(batch)}


class Layout:
    def __init__(self, outer, sub, seq):
        self.outer, self.sub, self.seq = outer, sub, seq
        self.chips_x = seq // 2
        self.group = sub * seq
        self.count = outer * self.group
        self.heads = HEADS // self.group
        self.offsets = [(ry, rx) for ry in range(sub) for rx in range(self.chips_x)]
        self.square = sub == 2 and self.chips_x == 2
        self.near = [o for o in self.offsets if not (self.square and o == (1, 1))]
        self.far = sorted(self.offsets[1:], key=lambda o: (o[0] > 0) + (o[1] > 0))

    def shift(self, ry, rx):
        pairs = []
        for y in range(self.sub):
            for x in range(self.chips_x):
                for c in range(2):
                    there = ((y + ry) % self.sub, (x + rx) % self.chips_x)
                    pairs.append((y * self.seq + x * 2 + c, there[0] * self.seq + there[1] * 2 + c))
        return pairs

    def flip(self):
        return [(i, i ^ 1) for i in range(self.seq)]


def swap_copies(lay, plan, me, sources, targets, send, recv, back):
    zo = lax.axis_index("zo")
    copies = []
    for k in range(1, lay.group):
        peer = lax.rem(me + k, lay.group)
        device = (zo, peer // lay.seq, lax.rem(peer, lay.seq))
        j = 0
        for (parts, rows, cols, first), source, target in zip(plan, sources, targets, strict=True):
            for part in range(parts):
                wide = lambda who: pl.ds(pl.multiple_of((part * lay.group + who) * cols, 128), cols)
                thin = pl.ds(first + part * cols, cols)
                block = lambda who: pl.ds(pl.multiple_of(who * rows, rows), rows)
                if back:
                    copies.append(remote(source.at[block(peer), thin], target.at[:, wide(me)], send.at[k - 1, j], recv.at[k - 1, j], device))
                else:
                    copies.append(remote(source.at[:, wide(peer)], target.at[block(me), thin], send.at[k - 1, j], recv.at[k - 1, j], device))
                j += 1
    return copies


def swap_own(lay, plan, me, sources, targets, sems, back):
    copies = []
    j = 0
    for (parts, rows, cols, first), source, target in zip(plan, sources, targets, strict=True):
        for part in range(parts):
            wide = pl.ds(pl.multiple_of((part * lay.group + me) * cols, 128), cols)
            thin = pl.ds(first + part * cols, cols)
            block = pl.ds(pl.multiple_of(me * rows, rows), rows)
            if back:
                copies.append(pltpu.make_async_copy(source.at[block, thin], target.at[:, wide], sems.at[j]))
            else:
                copies.append(pltpu.make_async_copy(source.at[:, wide], target.at[block, thin], sems.at[j]))
            j += 1
    return copies


def group_barrier(lay, me):
    zo = lax.axis_index("zo")
    barrier = pltpu.get_barrier_semaphore()
    for k in range(1, lay.group):
        peer = lax.rem(me + k, lay.group)
        pl.semaphore_signal(
            barrier, inc=1, device_id=(zo, peer // lay.seq, lax.rem(peer, lay.seq)), device_id_type=MESH
        )
    pl.semaphore_wait(barrier, lay.group - 1)


def swap_shapes(lay, plan, back):
    if back:
        return [jax.ShapeDtypeStruct((rows, parts * lay.group * cols), BF16) for parts, rows, cols, _ in plan]
    return [jax.ShapeDtypeStruct((lay.group * rows, parts * cols), BF16) for parts, rows, cols, _ in plan]


def device_after(lay, rank, k):
    peer = lax.rem(rank + k, lay.count)
    inner = lax.rem(peer, lay.group)
    return (peer // lay.group, inner // lay.seq, lax.rem(inner, lay.seq))


def barrier_all(lay, device_of):
    barrier = pltpu.get_barrier_semaphore()

    def greet(k, carry):
        pl.semaphore_signal(barrier, inc=1, device_id=device_of(k), device_id_type=MESH)
        return carry

    lax.fori_loop(1, lay.count, greet, 0)
    pl.semaphore_wait(barrier, lay.count - 1)


def busy(microseconds):
    return pl.CostEstimate(flops=int(7e8 * microseconds), bytes_accessed=1 << 20, transcendentals=0)


def norm_kernel(lay, plan, *refs):
    n = len(plan)
    x_ref, vec_ref, sources = refs[0], refs[1], refs[2 : 2 + n]
    one_ref, two_ref, hat_ref, all_ref, targets = *refs[2 + n : 6 + n], refs[6 + n : 6 + 2 * n]
    (held, stage, vectors, gain_buf, send, recv, core_send, core_recv, w_send, w_recv, w_own, own_sem, out_sem,
     vec_send, vec_recv, vec_own) = refs[6 + 2 * n :]
    batch, length, width = x_ref.shape
    zo, yi, s = lax.axis_index("zo"), lax.axis_index("yi"), lax.axis_index("seq")
    me = yi * lay.seq + s
    x, core = s // 2, lax.rem(s, 2)
    partner = (zo, yi, x * 2 + 1 - core)

    def chip(ry, rx):
        return (zo, lax.rem(yi + ry, lay.sub), lax.rem(x + rx, lay.chips_x) * 2 + core)

    rank = zo * lay.group + me
    device_of = functools.partial(device_after, lay, rank)
    barrier_all(lay, device_of)

    def vec_copy(k):
        return remote(vec_ref, vectors.at[rank], vec_send.at[k - 1], vec_recv.at[k - 1], device_of(k))

    def vec_start(k, carry):
        vec_copy(k).start()
        return carry

    def vec_finish(k, carry):
        vec_copy(k).wait()
        return carry

    lax.fori_loop(1, lay.count, vec_start, 0)
    vec_mine = pltpu.make_async_copy(vec_ref, vectors.at[rank], vec_own.at[0])
    vec_mine.start()
    slot = {offset: i for i, offset in enumerate(lay.offsets)}
    own_copy = pltpu.make_async_copy(x_ref, held.at[0, 0], own_sem)
    own_copy.start()
    straight = [o for o in lay.far if not (o[0] and o[1])]
    diagonal = [o for o in lay.far if o[0] and o[1]]
    copies = {}
    for o in straight:
        copies[o] = [remote(x_ref, held.at[0, slot[o]], send.at[slot[o], 0], recv.at[slot[o], 0], chip(*o))]
    half = batch // 2
    for ry, rx in diagonal:
        j = slot[(ry, rx)]
        copies[(ry, rx)] = [
            remote(held.at[0, slot[(0, rx)], :half], held.at[0, j, :half], send.at[j, 0], recv.at[j, 0], chip(ry, 0)),
            remote(held.at[0, slot[(ry, 0)], half:], held.at[0, j, half:], send.at[j, 1], recv.at[j, 1], chip(0, rx)),
        ]
    to_partner = {
        o: remote(x_ref if o == (0, 0) else held.at[0, slot[o]], held.at[1, slot[o]],
                  core_send.at[slot[o]], core_recv.at[slot[o]], partner)
        for o in lay.offsets
    }
    for o in straight:
        copies[o][0].start()
    to_partner[(0, 0)].start()
    swaps = swap_copies(lay, plan, me, sources, targets, w_send, w_recv, False)
    swaps += swap_own(lay, plan, me, sources, targets, w_own, False)
    lax.fori_loop(1, lay.count, vec_finish, 0)
    vec_mine.wait()
    vec_out = pltpu.make_async_copy(vectors, all_ref, vec_own.at[1])
    vec_out.start()
    size = width // lay.count
    lane = lax.broadcasted_iota(jnp.int32, (1, 128), 1)
    for v in range(4):
        row, low = (v * size) // 128, (v * size) % 128
        for k in range(width // 128):
            line = None
            for j in range(128 // size):
                piece = vectors[k * (128 // size) + j, row : row + 1, :]
                turn = (j * size - low) % 128
                piece = pltpu.roll(piece, turn, 1) if turn else piece
                line = piece if line is None else jnp.where(lane >= j * size, piece, line)
            gain_buf[v : v + 1, k * 128 : (k + 1) * 128] = line
    gains = [gain_buf[i : i + 1, :] for i in range(4)]
    rows = 16
    pending = [[], []]
    turn = [0]

    def norm(c, j):
        for m in range(batch):
            k = turn[0] % 2
            turn[0] += 1
            for copy in pending[k]:
                copy.wait()

            def chunk(i, carry):
                at = pl.ds(pl.multiple_of(i * rows, rows), rows)
                value = held[c, j, m, at, :].astype(F32)
                center = value - jnp.mean(value, -1, keepdims=True)
                hat = center * lax.rsqrt(jnp.mean(center * center, -1, keepdims=True) + EPSILON)
                stage[k, 0, at, :] = (hat * gains[2] + gains[0]).astype(BF16)
                stage[k, 1, at, :] = (hat * gains[3] + gains[1]).astype(BF16)
                stage[k, 2, at, :] = hat.astype(BF16)
                return carry

            lax.fori_loop(0, length // rows, chunk, 0, unroll=2)
            pending[k] = [
                pltpu.make_async_copy(stage.at[k, i], ref.at[c, j, m], out_sem.at[k, i])
                for i, ref in enumerate((one_ref, two_ref, hat_ref))
            ]
            for copy in pending[k]:
                copy.start()

    own_copy.wait()
    norm(0, 0)
    to_partner[(0, 0)].wait_recv()
    norm(1, 0)
    for o in straight:
        copies[o][0].wait_recv()
        to_partner[o].start()
        for ry, rx in diagonal:
            if o == (0, rx):
                copies[(ry, rx)][0].start()
            if o == (ry, 0):
                copies[(ry, rx)][1].start()
        if o == straight[-1]:
            for copy in swaps:
                copy.start()
        norm(0, slot[o])
    for o in straight:
        to_partner[o].wait_recv()
        norm(1, slot[o])
    for o in diagonal:
        for copy in copies[o]:
            copy.wait_recv()
        to_partner[o].start()
        norm(0, slot[o])
    for o in diagonal:
        to_partner[o].wait_recv()
        norm(1, slot[o])
    for side in pending:
        for copy in side:
            copy.wait()
    for o in lay.far:
        for copy in copies[o]:
            copy.wait_send()
    for o in lay.offsets:
        to_partner[o].wait_send()
    for copy in swaps:
        copy.wait()
    vec_out.wait()


def norm_exchange(lay, plan, tokens, vec, weights):
    count = sum(parts for parts, _, _, _ in plan)
    chips = lay.group // 2
    whole = jax.ShapeDtypeStruct((2, chips, *tokens.shape), BF16)
    return pl.pallas_call(
        functools.partial(norm_kernel, lay, plan),
        out_shape=[whole] * 3 + [jax.ShapeDtypeStruct((lay.count, *vec.shape), F32)] + swap_shapes(lay, plan, False),
        in_specs=[ANY] * (2 + len(plan)),
        out_specs=[ANY] * (4 + len(plan)),
        scratch_shapes=[
            pltpu.VMEM((2, chips, *tokens.shape), BF16),
            pltpu.VMEM((2, 3, *tokens.shape[1:]), BF16),
            pltpu.VMEM((lay.count, *vec.shape), F32),
            pltpu.VMEM((4, tokens.shape[2]), F32),
            pltpu.SemaphoreType.DMA((chips, 2)),
            pltpu.SemaphoreType.DMA((chips, 2)),
            pltpu.SemaphoreType.DMA((chips,)),
            pltpu.SemaphoreType.DMA((chips,)),
            pltpu.SemaphoreType.DMA((lay.group - 1, count)),
            pltpu.SemaphoreType.DMA((lay.group - 1, count)),
            pltpu.SemaphoreType.DMA((count,)),
            pltpu.SemaphoreType.DMA,
            pltpu.SemaphoreType.DMA((2, 3)),
            pltpu.SemaphoreType.DMA((lay.count - 1,)),
            pltpu.SemaphoreType.DMA((lay.count - 1,)),
            pltpu.SemaphoreType.DMA((2,)),
        ],
        compiler_params=pltpu.CompilerParams(
            collective_id=1, has_side_effects=True, vmem_limit_bytes=48 << 20
        ),
        cost_estimate=busy(100),
        name="norm_exchange",
    )(tokens, vec, *weights)


def deal_kernel(lay, plan, back, *refs):
    n = len(plan)
    sources, targets = refs[:n], refs[n : 2 * n]
    send, recv, own = refs[2 * n :]
    me = lax.axis_index("yi") * lay.seq + lax.axis_index("seq")
    group_barrier(lay, me)
    copies = swap_copies(lay, plan, me, sources, targets, send, recv, back)
    copies += swap_own(lay, plan, me, sources, targets, own, back)
    for copy in copies:
        copy.start()
    for copy in copies:
        copy.wait()


def deal_exchange(lay, plan, arrays, back, number):
    count = sum(parts for parts, _, _, _ in plan)
    return pl.pallas_call(
        functools.partial(deal_kernel, lay, plan, back),
        out_shape=swap_shapes(lay, plan, back),
        in_specs=[ANY] * len(plan),
        out_specs=[ANY] * len(plan),
        scratch_shapes=[
            pltpu.SemaphoreType.DMA((lay.group - 1, count)),
            pltpu.SemaphoreType.DMA((lay.group - 1, count)),
            pltpu.SemaphoreType.DMA((count,)),
        ],
        compiler_params=pltpu.CompilerParams(collective_id=number, has_side_effects=True),
        cost_estimate=busy(17),
    )(*arrays)


def pair_kernel(lay, plan, with_vec, scaled, batch, places, *refs):
    refs = list(refs)
    take = lambda k: [refs.pop(0) for _ in range(k)]
    step = pl.program_id(0)
    chips = lay.group // 2
    first_ref, first_w, second_ref, second_w = take(4)
    scales = take(2) if scaled else []
    sources, vec_ref = take(len(plan)), take(int(with_vec))
    outs, targets, all_ref = take(1 + max(k for k, _ in places.values())), take(len(plan)), take(int(with_vec))
    given, came, act_buf, w_buf, send, recv, out_sem = take(7)
    zo, yi, s = lax.axis_index("zo"), lax.axis_index("yi"), lax.axis_index("seq")
    me = yi * lay.seq + s
    rank = zo * lay.group + me
    device_of = functools.partial(device_after, lay, rank)
    partner = (zo, yi, (s // 2) * 2 + 1 - lax.rem(s, 2))
    swap_sems = take(3) if plan else []
    vec_sems = take(3) if with_vec else []

    def copy(j):
        return remote(given.at[j], came.at[j], send.at[j], recv.at[j], partner)

    def stores(j):
        length = came.shape[1] // batch
        copies = []
        for m in range(batch):
            k, at = places[((j + 1) % chips, m)]
            target = outs[k] if at is None else outs[k].at[at]
            copies.append(pltpu.make_async_copy(came.at[j, pl.ds(m * length, length)], target, out_sem.at[j, m]))
        return copies

    def riders():
        if not plan:
            return []
        copies = swap_copies(lay, plan, me, sources, targets, swap_sems[0], swap_sems[1], True)
        return copies + swap_own(lay, plan, me, sources, targets, swap_sems[2], True)

    def vec_copy(k):
        return remote(vec_ref[0], all_ref[0].at[rank], vec_sems[0].at[k - 1], vec_sems[1].at[k - 1], device_of(k))

    def vec_start(k, carry):
        vec_copy(k).start()
        return carry

    def vec_finish(k, carry):
        vec_copy(k).wait()
        return carry

    def vec_mine():
        return pltpu.make_async_copy(vec_ref[0], all_ref[0].at[rank], vec_sems[2])

    @pl.when(step == 0)
    def _():
        if with_vec:
            barrier_all(lay, device_of)
            vec_mine().start()
            lax.fori_loop(1, lay.count, vec_start, 0)
        elif plan:
            group_barrier(lay, me)
        else:
            barrier = pltpu.get_barrier_semaphore()
            pl.semaphore_signal(barrier, inc=1, device_id=partner, device_id_type=MESH)
            pl.semaphore_wait(barrier, 1)
        for rider in riders():
            rider.start()
        at = 0
        for k, weight in enumerate((first_w, second_w)):
            depth = weight.shape[1]
            if scaled:
                line = scales[k][...]
                gain = jnp.transpose(jnp.broadcast_to(line, (128, line.shape[1])), (1, 0))
                for c in range(0, depth, 128):
                    w_buf[:, at + c : at + c + 128] = (weight[:, c : c + 128].astype(F32) * gain).astype(BF16)
            else:
                w_buf[:, at : at + depth] = weight[...]
            at += depth

    for j in range(chips):

        @pl.when(step == j + 1)
        def _():
            copy(j).start()

    cut = first_ref.shape[3]
    act_buf[:, :cut] = first_ref[0, 0]
    act_buf[:, cut:] = second_ref[0, 0]
    total = dot(act_buf[...], w_buf[...], ((1,), (1,)))
    for j in range(chips):

        @pl.when(step == j)
        def _():
            given[j] = total.astype(BF16)

        @pl.when(step == chips + j)
        def _():
            copy(j).wait_recv()
            came[j] = (total + came[j].astype(F32)).astype(BF16)

    for j in range(chips - 1):

        @pl.when(step == chips + j + 1)
        def _():
            for piece in stores(j):
                piece.start()

    @pl.when(step == 2 * chips - 1)
    def _():
        for piece in stores(chips - 1):
            piece.start()
        for j in range(chips):
            copy(j).wait_send()
            for piece in stores(j):
                piece.wait()
        for rider in riders():
            rider.wait()
        if with_vec:
            vec_mine().wait()
            lax.fori_loop(1, lay.count, vec_finish, 0)


def pair_matmul(lay, acts, weights, batch, cut, number, scales=(), plan=(), arrays=(), vec=None):
    chips = lay.group // 2
    rows = acts[0].shape[0] // lay.group
    width = weights[0].shape[0] // cut[1]
    count = sum(parts for parts, _, _, _ in plan)
    with_vec = vec is not None

    def act(depth):
        return pl.BlockSpec((1, 1, rows, depth), lambda i: (1 - i // chips, (i + 1) % chips, 0, 0))

    def weight(depth):
        return pl.BlockSpec((width, depth), lambda i: (cut[0], 0), pipeline_mode=pl.Buffered(1))

    specs, args = [], []
    for a, w in zip(acts, weights, strict=True):
        specs += [act(a.shape[1]), weight(a.shape[1])]
        args += [a.reshape(2, chips, rows, a.shape[1]), w]
    for scale in scales:
        specs.append(pl.BlockSpec((1, width), lambda i: (0, cut[0])))
        args.append(scale.reshape(1, -1))
    args += [*arrays, *([vec] if with_vec else [])]
    specs += [ANY] * (len(args) - len(specs))
    places = far_places(lay.square, chips, batch)
    piled = [sum(1 for k, _ in places.values() if k == i) for i in range(1 + max(k for k, _ in places.values()))]
    piece = (rows // batch, width)
    shapes = [jax.ShapeDtypeStruct(piece if n == 1 else (n, *piece), BF16) for n in piled] + swap_shapes(lay, plan, True)
    depth = sum(a.shape[1] for a in acts)
    scratch = [
        pltpu.VMEM((chips, rows, width), BF16),
        pltpu.VMEM((chips, rows, width), BF16),
        pltpu.VMEM((rows, depth), BF16),
        pltpu.VMEM((width, depth), BF16),
        pltpu.SemaphoreType.DMA((chips,)),
        pltpu.SemaphoreType.DMA((chips,)),
        pltpu.SemaphoreType.DMA((chips, batch)),
    ]
    if plan:
        scratch += [pltpu.SemaphoreType.DMA((lay.group - 1, count))] * 2 + [pltpu.SemaphoreType.DMA((count,))]
    if with_vec:
        shapes.append(jax.ShapeDtypeStruct((lay.count, *vec.shape), vec.dtype))
        scratch += [pltpu.SemaphoreType.DMA((lay.count - 1,))] * 2 + [pltpu.SemaphoreType.DMA]
    return pl.pallas_call(
        functools.partial(pair_kernel, lay, plan, with_vec, bool(scales), batch, places),
        grid=(2 * chips,),
        in_specs=specs,
        out_specs=[ANY] * len(shapes),
        out_shape=shapes,
        scratch_shapes=scratch,
        compiler_params=pltpu.CompilerParams(
            collective_id=number, has_side_effects=True, vmem_limit_bytes=60 << 20
        ),
        cost_estimate=pl.CostEstimate(
            flops=2 * acts[0].shape[0] * depth * width, bytes_accessed=32 << 20, transcendentals=0
        ),
    )(*args)


def turn_pairs(field, cosine, sine):
    halves = ROTARY // 2
    front = field[:, :128]
    lane = lax.broadcasted_iota(jnp.int32, front.shape, 1)
    other = jnp.where(lane < halves, pltpu.roll(front, 128 - halves, 1), pltpu.roll(front, halves, 1))
    return jnp.concatenate([front * cosine + other * sine, field[:, 128:]], -1)


QUERY_BLOCK = 256


def wide_angles(ref):
    part = ref[0]
    return jnp.transpose(jnp.concatenate([part, part, part, part], 0), (1, 0))


def wide_pair(cos_ref, sin_ref):
    cosine, sine = wide_angles(cos_ref), wide_angles(sin_ref)
    lane = lax.broadcasted_iota(jnp.int32, cosine.shape, 1)
    cosine = jnp.where(lane < ROTARY, cosine, 1.0)
    sine = jnp.where(lane < ROTARY // 2, -sine, jnp.where(lane < ROTARY, sine, 0.0))
    return cosine, sine


def attend_kernel(lay, scaling, *refs):
    refs = list(refs)
    take = lambda k: [refs.pop(0) for _ in range(k)]
    near_count = len(lay.near)
    packed_ref, cos_ref, sin_ref, col_ref, row_ref = take(5)
    near = take(near_count)
    q_ref, k_ref, v_ref, ctx_ref, lse_ref, dy_ref = take(6)
    q_buf, k_buf, v_buf, ctx_buf, cos_buf, sin_buf, bounce = take(7)
    load_sem, store_sem, core_send, core_recv, on_send, on_recv, fwd_send, fwd_recv = take(8)
    step, last = pl.program_id(0), pl.num_programs(0) - 1
    zo, yi, s = lax.axis_index("zo"), lax.axis_index("yi"), lax.axis_index("seq")
    x, core = s // 2, lax.rem(s, 2)
    partner = (zo, yi, x * 2 + 1 - core)
    batch, length = near[0].shape[:2]
    cuts = [(m, pl.ds(q * (length // 2), length // 2)) for m in range(batch) for q in range(2)] if lay.square else []

    def load(i):
        return pltpu.make_async_copy(near[i], bounce.at[i], load_sem.at[i])

    def store(i):
        return pltpu.make_async_copy(bounce.at[i], dy_ref.at[0, i], store_sem.at[i])

    def to_partner(i):
        return remote(near[i], dy_ref.at[1, i], core_send.at[i], core_recv.at[i], partner)

    def onward():
        over_y = (zo, lax.rem(yi + 1, lay.sub), s)
        over_x = (zo, yi, lax.rem(x + 1, lay.chips_x) * 2 + core)
        return [
            remote(near[1 if m < batch // 2 else 2].at[m, rows], dy_ref.at[0, 3, m, rows], on_send.at[k], on_recv.at[k],
                   over_y if m < batch // 2 else over_x)
            for k, (m, rows) in enumerate(cuts)
        ]

    def forward():
        return [
            remote(dy_ref.at[0, 3, m, rows], dy_ref.at[1, 3, m, rows], fwd_send.at[k], fwd_recv.at[k], partner)
            for k, (m, rows) in enumerate(cuts)
        ]

    @pl.when(step == 0)
    def _():
        group_barrier(lay, yi * lay.seq + s)
        for copy in onward():
            copy.start()
        for i in range(near_count):
            load(i).start()
            to_partner(i).start()

    @pl.when(step == 1)
    def _():
        for i in range(near_count):
            load(i).wait()
            store(i).start()

    attend_one(scaling, packed_ref, cos_ref, sin_ref, col_ref, row_ref, q_ref, k_ref, v_ref, ctx_ref, lse_ref,
               q_buf, k_buf, v_buf, ctx_buf, cos_buf, sin_buf)

    @pl.when(step == last)
    def _():
        for came, copy in zip(onward(), forward(), strict=True):
            came.wait_recv()
            copy.start()
        for i in range(near_count):
            store(i).wait()
            to_partner(i).wait()
        for gone, copy in zip(onward(), forward(), strict=True):
            gone.wait_send()
            copy.wait()


def attend_one(scaling, packed_ref, cos_ref, sin_ref, col_ref, row_ref, q_ref, k_ref, v_ref, ctx_ref, lse_ref,
               q_buf, k_buf, v_buf, ctx_buf, cos_buf, sin_buf):
    cores, _, chips, _, length, _ = packed_ref.shape
    cos_all, sin_all = wide_pair(cos_ref, sin_ref)
    cos_buf[...] = cos_all
    sin_buf[...] = sin_all
    for c in range(cores):
        for i in range(chips):
            at = pl.ds((c * chips + i) * length, length)
            block = packed_ref[c, 0, i, 0]
            cosine, sine = cos_buf[at, :], sin_buf[at, :]
            q_buf[at, :] = turn_pairs(block[:, :HEAD_DIM], cosine, sine).astype(BF16)
            k_buf[at, :] = turn_pairs(block[:, HEAD_DIM : 2 * HEAD_DIM], cosine, sine).astype(BF16)
            v_buf[at, :] = block[:, 2 * HEAD_DIM :].astype(BF16)
    q_ref[0] = q_buf[...]
    k_ref[0] = k_buf[...]
    v_ref[0] = v_buf[...]
    total = cores * chips * length

    def one(j, carry):
        at = pl.ds(pl.multiple_of(j * QUERY_BLOCK, QUERY_BLOCK), QUERY_BLOCK)
        scores = dot(k_buf[...], q_buf[at, :], ((1,), (1,))) * scaling
        allowed = col_ref[0] <= row_ref[0, :, at]
        scores = jnp.where(allowed, scores, NEGATIVE)
        top = jnp.max(scores, 0, keepdims=True)
        weights = jnp.where(allowed, jnp.exp(scores - top), 0.0)
        total_row = jnp.sum(weights, 0, keepdims=True)
        probs = (weights * (1.0 / total_row)).astype(BF16)
        ctx_buf[at, :] = dot(probs, v_buf[...], ((0,), (0,))).astype(BF16)
        lse_ref[0, :, at] = top + jnp.log(total_row)
        return carry

    lax.fori_loop(0, total // QUERY_BLOCK, one, 0)
    for c in range(cores):
        for i in range(chips):
            ctx_ref[c, 0, i, 0] = ctx_buf[pl.ds((c * chips + i) * length, length), :]


def attend_back_kernel(scaling, q_ref, k_ref, v_ref, dy_ref, w_ref, ctx_ref, cos_ref, sin_ref, col_ref, row_ref, lse_ref, out_ref, sum_ref, grad_ref,
                       g_buf, acc_buf, dq_buf, dk_buf, dv_buf, cos_buf, sin_buf):
    cores, _, chips, _, length, _ = out_ref.shape
    total = q_ref.shape[1]
    cos_all, sin_all = wide_pair(cos_ref, sin_ref)
    cos_buf[...] = cos_all
    sin_buf[...] = sin_all
    upstream = dy_ref[...].reshape(total, dy_ref.shape[-1])
    g_buf[...] = dot(upstream, w_ref[...], ((1,), (0,))).astype(BF16)
    out_grad = dot(ctx_ref[...].reshape(total, ctx_ref.shape[-1]), upstream, ((0,), (0,)))
    step = pl.program_id(0)

    @pl.when(step == 0)
    def _():
        acc_buf[...] = out_grad

    @pl.when(step > 0)
    def _():
        acc_buf[...] += out_grad

    @pl.when(step == pl.num_programs(0) - 1)
    def _():
        grad_ref[...] = jnp.transpose(acc_buf[...], (1, 0)).astype(BF16)

    dk_buf[...] = jnp.zeros_like(dk_buf)
    dv_buf[...] = jnp.zeros_like(dv_buf)

    def one(j, carry):
        at = pl.ds(pl.multiple_of(j * QUERY_BLOCK, QUERY_BLOCK), QUERY_BLOCK)
        queries = q_ref[0, at, :]
        grads = g_buf[at, :]
        scores = dot(k_ref[0], queries, ((1,), (1,))) * scaling
        allowed = col_ref[0] <= row_ref[0, :, at]
        scores = jnp.where(allowed, scores, NEGATIVE)
        probs = jnp.where(allowed, jnp.exp(scores - lse_ref[0, :, at]), 0.0)
        grad_probs = dot(v_ref[0], grads, ((1,), (1,)))
        delta = jnp.sum(probs * grad_probs, 0, keepdims=True)
        grad_scores = (probs * (grad_probs - delta)).astype(BF16)
        dv_buf[...] += dot(probs.astype(BF16), grads, ((1,), (0,)))
        dk_buf[...] += dot(grad_scores, queries, ((1,), (0,)))
        dq_buf[at, :] = dot(grad_scores, k_ref[0], ((0,), (0,)))
        return carry

    lax.fori_loop(0, total // QUERY_BLOCK, one, 0)
    for c in range(cores):
        for i in range(chips):
            at = pl.ds((c * chips + i) * length, length)
            cosine, sine = cos_buf[at, :], sin_buf[at, :]
            pieces = (
                turn_pairs(dq_buf[at, :] * scaling, cosine, -sine),
                turn_pairs(dk_buf[at, :] * scaling, cosine, -sine),
                dv_buf[at, :],
            )
            for k, piece in enumerate(pieces):
                columns = slice(k * HEAD_DIM, (k + 1) * HEAD_DIM)
                low = piece.astype(BF16)
                out_ref[c, 0, i, 0, :, columns] = low
                part = jnp.sum(low.astype(F32), 0, keepdims=True)
                sum_ref[0, :, columns] = part if c + i == 0 else sum_ref[0, :, columns] + part


def make_body(lay):
    sub, seq, group, chips_x = lay.sub, lay.seq, lay.group, lay.chips_x

    square = lay.square

    def across(value, o):
        return lax.ppermute(value, GROUP, lay.shift(*o))

    def add(*pieces):
        total = pieces[0].astype(F32)
        for piece in pieces[1:]:
            total = total + piece.astype(F32)
        return total

    def far_first(outs):
        if square:
            return [across(outs[4], (1, 0)), across(outs[5], (0, 1))]
        batch = len(outs) // (group // 2)
        return [
            [
                across(outs[i * batch + m], ((-o[0]) % sub, (-o[1]) % chips_x))
                for i, o in enumerate(lay.offsets)
                if i
            ]
            for m in range(batch)
        ]

    def far_onward(outs, came):
        if square:
            return [add(outs[2], came[0][1]).astype(BF16), add(outs[3], came[1][1]).astype(BF16)]
        return []

    def far_second(outs, came, onward):
        if square:
            last = [across(onward[0], (0, 1)), across(onward[1], (1, 0))]
            return [[outs[m], came[m][0], last[m]] for m in range(2)]
        return [[outs[m], *came[m]] for m in range(len(came))]

    def add_all(parts):
        return jnp.stack([add(*pieces) for pieces in parts])

    def after(value, *tokens):
        return lax.optimization_barrier((value, *tokens))[0]

    def step(
        tokens, positions, cotangent, gain1, bias1, gain2, bias2,
        w_qkv, b_qkv, w_out, b_out, w_up, b_up, w_down, b_down,
    ):
        batch, length, width = tokens.shape
        rows = w_qkv.shape[0]
        ff = w_up.shape[1]
        count = seq * length
        total = group * batch * length
        my_seq = lax.axis_index("seq")
        me = lax.axis_index("yi") * seq + my_seq
        scaling = HEAD_DIM ** (-0.5)
        cols = lay.heads * HEAD_DIM
        ff_cols = ff // group
        out_cols = width // group
        plans = {"up": (1, rows, ff_cols, 0), "down": (1, rows, ff_cols, 0), "qkv": (3, rows, cols, 0), "out": (1, rows, out_cols, 0)}

        def gather_rows(mine):
            return lax.all_gather(mine, "zo", axis=0, tiled=True)

        x, core = my_seq // 2, my_seq % 2
        places = []
        for ry in range(sub):
            from_there = positions
            if ry:
                from_there = lax.ppermute(positions, "yi", [(i, (i + ry) % sub) for i in range(sub)])
            blocks = from_there.reshape(batch, seq, length)
            order = [((x - rx) % chips_x) * 2 + (core + rc) % 2 for rc in range(2) for rx in range(chips_x)]
            places.append(jnp.concatenate([lax.dynamic_slice_in_dim(blocks, o, 1, 1) for o in order], 1))
        places = jnp.stack(places).reshape(sub * batch, count)

        def laid(values):
            size = -(-sum(v.size for v in values) // 1024) * 1024
            whole, at = 0.0, 0
            for v in values:
                whole = whole + jnp.pad(v.astype(F32), (at, size - at - v.size))
                at += v.size
            return whole.reshape(-1, 128)

        names = (bias1, bias2, gain1, gain2, b_qkv, b_up, b_out, b_down)
        (up_own,) = deal_exchange(lay, [plans["up"]], [w_up], False, 0)
        up_w = gather_rows(up_own)
        w_qkv_late, _ = lax.optimization_barrier((w_qkv, up_own))
        (qkv_own,) = deal_exchange(lay, [plans["qkv"]], [w_qkv_late], False, 7)
        qkv_w = gather_rows(qkv_own)
        tokens_late, _, places = lax.optimization_barrier((tokens, qkv_own, places))
        one, two, hat, vectors, out_own, down_own = norm_exchange(
            lay, [plans["out"], plans["down"]], tokens_late, laid(names), [w_out, w_down]
        )
        out_w = gather_rows(out_own)
        down_w = gather_rows(down_own)
        vectors = vectors.reshape(lay.count, -1)
        cuts = []
        at = 0
        for piece in names:
            cuts.append(vectors[:, at : at + piece.shape[0]].reshape(-1))
            at += piece.shape[0]
        _, _, gain1_all, gain2_all, b_qkv_all, b_up_all, b_out_all, b_down_all = cuts
        b_qkv_mine = lax.dynamic_index_in_dim(b_qkv_all.reshape(3, group, cols), me, 1, keepdims=False).reshape(-1)
        b_up_mine = lax.dynamic_index_in_dim(b_up_all.reshape(group, ff_cols), me, 0, keepdims=False)
        one, two, hat = [v.reshape(total, width) for v in (one, two, hat)]
        cotangent, hat = lax.optimization_barrier((cotangent, hat))
        near_dy = [cotangent] + [across(cotangent, o) for o in lay.near[1:]]

        hidden = dot(two, up_w, ((1,), (0,))) + b_up_mine
        phi_cdf = 0.5 * (1.0 + lax.erf(hidden * math.sqrt(0.5)))
        density = jnp.exp(-0.5 * hidden * hidden) * (1.0 / math.sqrt(2.0 * math.pi))
        activated = (hidden * phi_cdf).astype(BF16)
        slope = (phi_cdf + hidden * density).astype(BF16)
        activated, slope = lax.optimization_barrier((activated, slope))

        halves = ROTARY // 2
        frequency = jnp.exp(jnp.arange(halves, dtype=F32) * (-2.0 * math.log(10000.0) / ROTARY))
        places = after(places, activated)
        phases = places.astype(F32)[:, None, :] * frequency[None, :, None]
        cosine, sine = jnp.cos(phases), jnp.sin(phases)
        place_col = places[:, :, None]
        place_row = places[:, None, :]

        seqs = sub * batch
        one = after(one, cosine, sine)
        packed = dot(one, qkv_w, ((1,), (0,))) + b_qkv_mine

        wide = (2, 1, chips_x, 1, length, 3 * cols)
        wide_spec = pl.BlockSpec(wide, lambda i: (0, i // batch, 0, i % batch, 0, 0))
        full = (2, sub, chips_x, batch, length, 3 * cols)
        head_spec = pl.BlockSpec((1, count, HEAD_DIM), lambda i: (i, 0, 0))
        turn_spec = pl.BlockSpec((1, ROTARY // 2, count), lambda i: (i, 0, 0))
        tokens_spec = pl.BlockSpec((2, 1, chips_x, 1, length, cols), lambda i: (0, i // batch, 0, i % batch, 0, 0))
        by_token = (2, sub, chips_x, batch, length, cols)
        turn_bufs = [pltpu.VMEM((count, 128), F32)] * 2
        col_spec = pl.BlockSpec((1, count, 1), lambda i: (i, 0, 0))
        row_spec = pl.BlockSpec((1, 1, count), lambda i: (i, 0, 0))
        head_shape = jax.ShapeDtypeStruct((seqs, count, HEAD_DIM), BF16)
        work = 2 * seqs * count * count * HEAD_DIM
        params = pltpu.CompilerParams(vmem_limit_bytes=56 << 20)
        near_count, chips = len(near_dy), group // 2
        queries, keys, values, context, lse, upstream = pl.pallas_call(
            functools.partial(attend_kernel, lay, scaling),
            grid=(seqs,),
            in_specs=[wide_spec, turn_spec, turn_spec, col_spec, row_spec] + [ANY] * near_count,
            out_specs=[head_spec] * 3 + [tokens_spec, row_spec, ANY],
            out_shape=[head_shape] * 3
            + [
                jax.ShapeDtypeStruct(by_token, BF16),
                jax.ShapeDtypeStruct((seqs, 1, count), F32),
                jax.ShapeDtypeStruct((2, chips, *cotangent.shape), BF16),
            ],
            scratch_shapes=[pltpu.VMEM((count, HEAD_DIM), BF16)] * 4
            + turn_bufs
            + [pltpu.VMEM((near_count, *cotangent.shape), BF16)]
            + [pltpu.SemaphoreType.DMA((near_count,))] * 2
            + [pltpu.SemaphoreType.DMA((near_count,))] * 2
            + [pltpu.SemaphoreType.DMA((2 * batch,))] * 4,
            compiler_params=pltpu.CompilerParams(collective_id=8, has_side_effects=True, vmem_limit_bytes=58 << 20),
            cost_estimate=pl.CostEstimate(flops=2 * work, bytes_accessed=30 << 20, transcendentals=seqs * count * count),
            name="attend",
        )(packed.reshape(full), cosine, sine, place_col, place_row, *near_dy)
        upstream = upstream.reshape(total, width)

        context = context.reshape(total, cols)

        def scatter(grad):
            return lax.psum_scatter(grad, "zo", scatter_dimension=0, tiled=True)

        def outer_dot(left, right):
            return dot(left, right, ((0,), (0,))).astype(BF16)

        def chain(values, *tokens):
            return lax.optimization_barrier((*values, *tokens))[: len(values)]

        down_part = outer_dot(upstream, activated)
        upstream, down_part = chain((upstream, down_part))
        down_sum = scatter(down_part)

        grad_packed, sum_packed, out_part = pl.pallas_call(
            functools.partial(attend_back_kernel, scaling),
            grid=(seqs,),
            in_specs=[head_spec] * 3
            + [
                pl.BlockSpec((2, 1, chips_x, 1, length, width), lambda i: (0, i // batch, 0, i % batch, 0, 0)),
                pl.BlockSpec((width, cols), lambda i: (0, 0), pipeline_mode=pl.Buffered(1)),
                tokens_spec,
            ]
            + [turn_spec, turn_spec, col_spec, row_spec, row_spec],
            out_specs=[
                wide_spec,
                pl.BlockSpec((1, 1, 3 * cols), lambda i: (i, 0, 0)),
                pl.BlockSpec((width, cols), lambda i: (0, 0)),
            ],
            out_shape=[
                jax.ShapeDtypeStruct(full, BF16),
                jax.ShapeDtypeStruct((seqs, 1, 3 * cols), F32),
                jax.ShapeDtypeStruct((width, cols), BF16),
            ],
            scratch_shapes=[pltpu.VMEM((count, HEAD_DIM), BF16), pltpu.VMEM((cols, width), F32)] + [pltpu.VMEM((count, HEAD_DIM), F32)] * 3 + turn_bufs,
            compiler_params=params,
            cost_estimate=pl.CostEstimate(flops=9 * work, bytes_accessed=40 << 20, transcendentals=seqs * count * count),
            name="attend_back",
        )(queries, keys, values, upstream.reshape(2, sub, chips_x, batch, length, width), out_w, context.reshape(by_token), cosine, sine, place_col, place_row, lse)
        grad_packed = grad_packed.reshape(total, 3 * cols)

        acts = chain((context, activated), grad_packed)
        out_near = pair_matmul(lay, acts, (out_w, down_w), batch, (0, 1), 4)
        out_came = far_first(out_near)
        hat, out_near = chain((hat, out_near))
        qkv_part = outer_dot(hat, grad_packed)
        qkv_sum = scatter(qkv_part)
        (upstream,) = chain((upstream,), qkv_part)
        grad_hidden = (dot(upstream, down_w, ((1,), (0,))) * slope.astype(F32)).astype(BF16)
        sum_hidden = jnp.sum(grad_hidden.astype(F32), 0)
        out_came, grad_hidden = chain((out_came, grad_hidden))
        onward, grad_hidden = chain((far_onward(out_near, out_came), grad_hidden))
        out_parts = far_second(out_near, out_came, onward)
        up_part = outer_dot(hat, grad_hidden)
        last_sum = scatter(jnp.concatenate([up_part, out_part], 1))
        (left,) = chain((grad_packed,), up_part)

        folded = (qkv_w, up_w)
        scales = (gain1_all, gain2_all)
        own_sums = [
            jnp.sum(sum_packed, (0, 1)),
            sum_hidden,
            jnp.sum(cotangent.astype(F32), (0, 1)),
        ]
        left, vec, down_sum = chain((left, laid(own_sums).astype(BF16), down_sum))
        *near0, down_raw, everyone = pair_matmul(
            lay, (left, grad_hidden), folded, batch, (0, 2), 5, scales, [plans["down"]], [down_sum], vec
        )
        came0 = far_first(near0)
        left, qkv_sum = chain((left, qkv_sum), near0)
        *near1, qkv_raw = pair_matmul(
            lay, (left, grad_hidden), folded, batch, (1, 2), 6, scales, [plans["qkv"]], [qkv_sum]
        )
        came1 = far_first(near1)
        (came0,) = chain((came0,), near1)
        onward0 = far_onward(near0, came0)
        parts0 = far_second(near0, came0, onward0)
        (out_parts,) = chain((out_parts,), onward0)
        output = (tokens.astype(F32) + add_all(out_parts) + b_out_all + b_down_all).astype(BF16)
        sums = jnp.sum(everyone.astype(F32).reshape(lay.outer, group, -1), 0)
        sum_qkv = jnp.transpose(sums[:, : 3 * cols].reshape(group, 3, cols), (1, 0, 2)).reshape(-1)
        sum_up = sums[:, 3 * cols : 3 * cols + ff_cols].reshape(-1)
        sum_dy = jnp.sum(sums[:, 3 * cols + ff_cols : 3 * cols + ff_cols + width], 0)
        rank = lax.axis_index("zo") * group + me

        def own_part(vector):
            return lax.dynamic_index_in_dim(vector.reshape(lay.count, -1), rank, 0, keepdims=False)

        column = lambda v: v.astype(F32)[:, None]
        qkv_raw = qkv_raw.astype(F32)
        bias_grads = (own_part(sum_qkv), own_part(sum_up), own_part(sum_dy))
        qkv_grads = (
            jnp.sum(w_qkv.astype(F32) * qkv_raw, 1),
            jnp.sum(w_qkv.astype(F32) * sum_qkv, 1),
            column(gain1) * qkv_raw + column(bias1) * sum_qkv,
        )
        down_grad = down_raw.astype(F32)
        came1, *early = chain((came1, output, down_grad, *bias_grads, *qkv_grads))
        output, down_grad, bias_grads, qkv_grads = early[0], early[1], early[2:5], early[5:8]
        onward1 = far_onward(near1, came1)
        parts1 = far_second(near1, came1, onward1)

        inputs = tokens.astype(F32)
        center = inputs - jnp.mean(inputs, -1, keepdims=True)
        inv_std = lax.rsqrt(jnp.mean(center * center, -1, keepdims=True) + EPSILON)
        normal = center * inv_std
        grad_normal = jnp.concatenate([add_all(parts0), add_all(parts1)], -1)
        token_grad = cotangent.astype(F32) + inv_std * (
            grad_normal
            - jnp.mean(grad_normal, -1, keepdims=True)
            - normal * jnp.mean(grad_normal * normal, -1, keepdims=True)
        )

        last_sum, token_grad = chain((last_sum, token_grad))
        up_raw, out_raw = deal_exchange(
            lay, [plans["up"], (1, rows, out_cols, ff_cols)], [last_sum, last_sum], True, 3
        )
        up_raw = up_raw.astype(F32)
        up_grads = (
            jnp.sum(w_up.astype(F32) * up_raw, 1),
            jnp.sum(w_up.astype(F32) * sum_up, 1),
            column(gain2) * up_raw + column(bias2) * sum_up,
        )
        return (
            output,
            token_grad,
            qkv_grads[0],
            qkv_grads[1],
            up_grads[0],
            up_grads[1],
            qkv_grads[2],
            bias_grads[0],
            out_raw.astype(F32),
            bias_grads[2],
            up_grads[2],
            bias_grads[1],
            down_grad,
            bias_grads[2],
        )

    return step


def solution(mesh):
    outer, sub, seq = split_axes(mesh)
    inner = Mesh(mesh.devices.reshape(outer, sub, seq), ALL)
    act = P(None, ALL, None)
    vec = P(ALL)
    mat = P(ALL, None)
    return jax.shard_map(
        make_body(Layout(outer, sub, seq)),
        mesh=inner,
        in_specs=(
            act, P(None, ("zo", "yi")), act, vec, vec, vec, vec,
            mat, vec, mat, vec, mat, vec, mat, vec,
        ),
        out_specs=(act, act, vec, vec, vec, vec, mat, vec, mat, vec, mat, vec, mat, vec),
        check_vma=False,
    )
```
